32 devices in a mesh: seq: 8 (over z, y), head: 4 (over x, core).
Axes of the slice: x: 2, y: 2, z: 4, core: 2. Of those that a mesh axis runs over, the one named last changes fastest.
Arguments:
- patches: bfloat16 [2048, 1280], P('seq'), may hold values from -6 to 6
- norm_gain: float32 [1280], replicated, may hold values from 0.5 to 1.5
- w_qkv: bfloat16 [1280, 3, 1280], P('seq', None, 'head'), as said below
- w_out: bfloat16 [1280, 1280], P('head', 'seq'), may hold values from -0.15625 to 0.15625
- window_order: int32 [8, 64], P('seq'), may hold values from 0 to 63, each once within a row
- merge_gain: float32 [1280], replicated, may hold values from 0.5 to 1.5
- w_kv: bfloat16 [5120, 2, 1024], P('seq', None, 'head'), as said below
- queries: bfloat16 [16, 8192], P('seq', 'head'), may hold values from -6 to 6
- suffix_kv: bfloat16 [16, 64, 2, 1024], P('seq', None, None, 'head'), may hold values from -12 to 12
- question_lengths: int32 [16], P('seq'), may hold values from 1 to 64
- frame_range: int32 [16, 2], replicated, may hold values from 0 to 8, as said below
Outputs:
- answers: bfloat16 [16, 8192], P('seq', 'head')
The draws below stay inside these ranges and needn't reach their ends.
Inputs may be any that keep to these rules, and one draw needn't show every extreme that they name: `window_order`: each row is an ordering of a frame's units; positions w * 16 to (w + 1) * 16 - 1 form window w. `frame_range`: the first entry of a row is below the second. `w_qkv`: entries of order one over the square root of 1280. `w_kv`: entries of order one over the square root of 5120.
All inputs are finite; a program needn't handle non-finite values.
Results may differ from the reference program's by a relative error of at most 0.007.
Values may be sent and summed in bfloat16 or wider, within the bound.
A program may use at most 64 MiB of HBM per device.

```python
import math
import jax
import jax.numpy as jnp
from jax import lax

VD = 1280
VH = 16
QH = 64
KVH = 8
HD = 128
FPATCH = 256
WIN = 64
SUF = 64
FRAMES = 8
PATCHES = 2048
QUESTIONS = 16


def draw_frame_range(key, part):
    first_key, second_key = jax.random.split(jax.random.fold_in(key, 11))
    first_pick = jax.random.randint(first_key, (QUESTIONS,), 0, FRAMES)
    second_pick = jax.random.randint(second_key, (QUESTIONS,), 0, FRAMES)
    lower = jnp.minimum(first_pick, second_pick)
    upper = jnp.maximum(first_pick, second_pick) + 1
    return jnp.stack([lower, upper], axis=1).astype(jnp.int32)


def sign_vector(seed_key, count):
    return jnp.where(jax.random.bernoulli(seed_key, 0.5, (count,)), 1.0, -1.0).astype(jnp.float32)


def plant_plan(seed_key):
    subkeys = jax.random.split(jax.random.fold_in(seed_key, 29), 6)
    vision_levels = jnp.linspace(100.0, 400.0, VH)
    prefix_levels = jnp.linspace(100.0, 480.0, KVH)
    head_width = VD // VH
    vision_alpha = jnp.sqrt(jax.random.permutation(subkeys[0], vision_levels) / (VD * math.sqrt(head_width)))
    prefix_alpha = jax.random.permutation(subkeys[1], prefix_levels) / (6.0 * math.sqrt(4 * VD * HD))
    vision_sign = sign_vector(subkeys[2], VD)
    vision_dir = sign_vector(subkeys[3], VD)
    prefix_sign = sign_vector(subkeys[4], 4 * VD)
    prefix_dir = sign_vector(subkeys[5], KVH * HD)
    return (vision_alpha, vision_sign, vision_dir, prefix_alpha, prefix_sign, prefix_dir)


def draw_patches(key, part):
    vision_alpha, vision_sign, vision_dir, prefix_alpha, prefix_sign, prefix_dir = plant_plan(key)
    subkeys = jax.random.split(jax.random.fold_in(key, 37), 9)
    background = jnp.clip(jax.random.normal(subkeys[1], (PATCHES, VD), jnp.float32), -6.0, 6.0)
    unit_count = FPATCH // 4
    frame_keys = jax.random.split(subkeys[2], FRAMES)
    chosen = jax.vmap(lambda frame_key: jax.random.permutation(frame_key, unit_count)[:3])(frame_keys)
    vision_field = jax.random.uniform(subkeys[3], (FRAMES, 1, VD), jnp.float32)
    vision_noise = jnp.clip(jax.random.normal(subkeys[4], (FRAMES, 1, VD), jnp.float32), -6.0, 6.0)
    vision_base = jax.random.uniform(subkeys[5], (FRAMES, 1, 1), jnp.float32, 0.0, 0.2)
    thresholds = vision_base + 0.01 * jnp.arange(4, dtype=jnp.float32).reshape(1, 4, 1)
    vision_unit = jnp.where(vision_field < thresholds, vision_noise, 6.0 * vision_sign.reshape(1, 1, VD))
    prefix_field = jax.random.uniform(subkeys[6], (FRAMES, 4, VD), jnp.float32)
    prefix_noise = jnp.clip(jax.random.normal(subkeys[7], (FRAMES, 4, VD), jnp.float32), -6.0, 6.0)
    prefix_base = jax.random.uniform(subkeys[8], (FRAMES, 1, 1), jnp.float32, 0.0, 0.25)
    pattern = 6.0 * prefix_sign.reshape(1, 4, VD)
    first_unit = jnp.where(prefix_field < prefix_base, prefix_noise, pattern)
    second_unit = jnp.where(prefix_field < prefix_base + 0.01, prefix_noise, pattern)
    frame_ids = jnp.arange(FRAMES)
    layout = background.reshape(FRAMES, unit_count, 4, VD)
    layout = layout.at[frame_ids, chosen[:, 0]].set(vision_unit)
    layout = layout.at[frame_ids, chosen[:, 1]].set(first_unit)
    layout = layout.at[frame_ids, chosen[:, 2]].set(second_unit)
    return layout.reshape(PATCHES, VD).astype(jnp.bfloat16)


def draw_w_qkv(key, part):
    vision_alpha, vision_sign, vision_dir, prefix_alpha, prefix_sign, prefix_dir = plant_plan(key)
    weight_key = jax.random.fold_in(key, 41)
    random_part = jnp.clip(jax.random.normal(weight_key, (VD, 3, VD), jnp.float32), -4.0, 4.0) * VD ** (-0.5)
    column_alpha = jnp.repeat(vision_alpha, VD // VH)
    rank_one = vision_sign[:, None] * (column_alpha * vision_dir)[None, :] * VD ** (-0.5)
    planted = jnp.stack([rank_one, rank_one, jnp.zeros_like(rank_one)], axis=1)
    return (random_part + planted).astype(jnp.bfloat16)


def draw_w_kv(key, part):
    vision_alpha, vision_sign, vision_dir, prefix_alpha, prefix_sign, prefix_dir = plant_plan(key)
    weight_key = jax.random.fold_in(key, 43)
    random_part = jnp.clip(jax.random.normal(weight_key, (4 * VD, 2, KVH * HD), jnp.float32), -4.0, 4.0) * (4 * VD) ** (-0.5)
    column_alpha = jnp.repeat(prefix_alpha, HD)
    rank_one = prefix_sign[:, None] * (column_alpha * prefix_dir)[None, :] * (4 * VD) ** (-0.5)
    planted = jnp.stack([rank_one, jnp.zeros_like(rank_one)], axis=1)
    return (random_part + planted).astype(jnp.bfloat16)


def draw_queries(key, part):
    vision_alpha, vision_sign, vision_dir, prefix_alpha, prefix_sign, prefix_dir = plant_plan(key)
    subkeys = jax.random.split(jax.random.fold_in(key, 47), 3)
    background = jnp.clip(jax.random.normal(subkeys[0], (QUESTIONS, QH, HD), jnp.float32), -6.0, 6.0)
    chosen = jax.random.bernoulli(subkeys[1], 0.25, (QUESTIONS, QH))
    levels = jnp.array([1.5, 3.0, 6.0, 6.0], jnp.float32)
    strength = levels[jax.random.randint(subkeys[2], (QUESTIONS, QH), 0, 4)]
    direction = jnp.broadcast_to(prefix_dir.reshape(KVH, 1, HD), (KVH, QH // KVH, HD)).reshape(QH, HD)
    planted = strength[..., None] * direction[None]
    shaped = jnp.where(chosen[..., None], planted, background)
    return shaped.reshape(QUESTIONS, QH * HD).astype(jnp.bfloat16)


def touch_ends(entries, stream_key, low, largest):
    shape = entries.shape
    place = [jax.random.randint(jax.random.fold_in(stream_key, axis), (), 0, shape[axis]) for axis in range(len(shape))]
    entries = entries.at[tuple(place)].set(low)
    longest = shape.index(max(shape))
    place[longest] = (place[longest] + 1) % shape[longest]
    return entries.at[tuple(place)].set(largest)


def level_of(rng, shape, shards, least, largest):
    level = 1.0
    for axis_at, shards_of in shards:
        heights = jax.random.uniform(jax.random.fold_in(jax.random.fold_in(rng, 6), axis_at), (shards_of,), jnp.float32, least / len(shards), largest / len(shards))
        level = level * jnp.repeat(jnp.exp(heights), shape[axis_at] // shards_of).reshape((-1,) + (1,) * (len(shape) - 1 - axis_at))
    return level


def normal_values(key, dims, deviation, limit, pieces=(), held_as=jnp.bfloat16):
    entries = deviation * jax.random.normal(key, dims, jnp.float32)
    if pieces:
        entries = entries * level_of(key, dims, pieces, -0.22, 0.18)
    return jnp.clip(entries, -limit, limit).astype(held_as)


def setup_inputs(seed: int = 0) -> dict:
    key_list = jax.random.split(jax.random.key(seed), 12)
    patches = draw_patches(jax.random.fold_in(key_list[11], 71), 0)
    norm_gain = jnp.clip(1.0 + 0.1 * jax.random.normal(key_list[1], (VD,), jnp.float32), 0.5, 1.5)
    w_qkv = draw_w_qkv(jax.random.fold_in(key_list[11], 71), 0)
    w_out = normal_values(key_list[3], (VD, VD), VD ** -0.5, 0.15625, ((0, 4), (1, 8)))
    window_order = jax.vmap(lambda own: jax.random.permutation(own, FPATCH // 4))(jax.random.split(key_list[4], FRAMES)).reshape((FRAMES, FPATCH // 4)).astype(jnp.int32)
    merge_gain = jnp.clip(1.0 + 0.1 * jax.random.normal(key_list[5], (VD,), jnp.float32), 0.5, 1.5)
    w_kv = draw_w_kv(jax.random.fold_in(key_list[11], 71), 0)
    queries = draw_queries(jax.random.fold_in(key_list[11], 71), 0)
    suffix_kv = normal_values(key_list[8], (QUESTIONS, SUF, 2, KVH * HD), 2.0, 12.0, ((0, 8), (3, 4)))
    question_lengths = touch_ends(jax.random.randint(key_list[9], (QUESTIONS,), 1, SUF + 1), jax.random.fold_in(key_list[9], 1), 1, SUF).astype(jnp.int32)
    frame_range = draw_frame_range(jax.random.fold_in(key_list[11], 71), 0)
    return {"patches": patches, "norm_gain": norm_gain, "w_qkv": w_qkv, "w_out": w_out, "window_order": window_order, "merge_gain": merge_gain, "w_kv": w_kv, "queries": queries, "suffix_kv": suffix_kv, "question_lengths": question_lengths, "frame_range": frame_range}


def rms_scale(values, gain):
    return values * lax.rsqrt(lax.optimization_barrier(jnp.mean(values * values, axis=-1, keepdims=True)) + 1e-06) * gain

def reference(patches, norm_gain, w_qkv, w_out, window_order, merge_gain, w_kv, queries, suffix_kv, question_lengths, frame_range):
    head_size = VD // VH
    source = patches.astype(jnp.float32)
    normed = rms_scale(source, norm_gain).astype(jnp.bfloat16)
    projected = jnp.dot(normed, w_qkv.reshape(VD, 3 * VD), preferred_element_type=jnp.float32).astype(jnp.bfloat16)
    projected = projected.reshape(FRAMES, FPATCH // 4, 4, 3, VD)

    def frame_window(inputs):
        frame_rows, unit_order = inputs
        grouped = frame_rows[unit_order].reshape(-1, WIN, 3, VH, head_size).astype(jnp.float32)
        scores = jnp.einsum('wqhd,wkhd->whqk', grouped[:, :, 0], grouped[:, :, 1]) * head_size ** (-0.5)
        weights = jax.nn.softmax(scores, axis=-1).astype(jnp.bfloat16)
        weights = lax.optimization_barrier(weights).astype(jnp.float32)
        mixed = jnp.einsum('whqk,wkhd->wqhd', weights, grouped[:, :, 2]).astype(jnp.bfloat16)
        mixed = mixed.reshape(FPATCH // 4, 4, VD)
        return jnp.zeros_like(mixed).at[unit_order].set(mixed)
    attended = lax.map(frame_window, (projected, window_order)).reshape(PATCHES, VD)
    hidden = source + jnp.dot(attended, w_out, preferred_element_type=jnp.float32)
    merged = rms_scale(hidden, merge_gain).astype(jnp.bfloat16).reshape(PATCHES // 4, 4 * VD)
    visual = jnp.dot(merged, w_kv.reshape(4 * VD, 2 * KVH * HD), preferred_element_type=jnp.float32).astype(jnp.bfloat16)
    visual = visual.reshape(PATCHES // 4, 2, KVH, HD).astype(jnp.float32)
    prefix_keys = visual[:, 0]
    prefix_values = visual[:, 1]
    frame_index = jnp.arange(PATCHES // 4) // (FPATCH // 4)
    group = QH // KVH

    def answer(inputs):
        query_row, suffix_rows, length, bounds = inputs
        asking = query_row.reshape(KVH, group, HD).astype(jnp.float32)
        suffix_rows = suffix_rows.reshape(SUF, 2, KVH, HD).astype(jnp.float32)
        keys = jnp.concatenate([prefix_keys, suffix_rows[:, 0]], axis=0)
        values = jnp.concatenate([prefix_values, suffix_rows[:, 1]], axis=0)
        live = jnp.concatenate([(frame_index >= bounds[0]) & (frame_index < bounds[1]), jnp.arange(SUF) < length])
        scores = jnp.einsum('gjd,ngd->gjn', asking, keys) * HD ** (-0.5)
        scores = jnp.where(live[None, None, :], scores, -jnp.inf)
        weights = jnp.exp(scores - lax.optimization_barrier(jnp.max(scores, axis=-1, keepdims=True)))
        totals = lax.optimization_barrier(jnp.sum(weights, axis=-1))
        rounded = lax.optimization_barrier(weights.astype(jnp.bfloat16)).astype(jnp.float32)
        mixed = jnp.einsum('gjn,ngd->gjd', rounded, values) / totals[..., None]
        return mixed.reshape(QH * HD).astype(jnp.bfloat16)
    return lax.map(answer, (queries, suffix_kv, question_lengths, frame_range))
```

```python
import functools

import jax
import jax.numpy as jnp
from jax import lax
from jax.experimental import pallas as pl
from jax.experimental.pallas import tpu as pltpu
from jax.sharding import PartitionSpec as P

VD = 1280
VH = 16
HD = 128
FPATCH = 256
WIN = 64

MESH = pl.DeviceIdType.MESH
VMEM = pl.BlockSpec(memory_space=pltpu.VMEM)


def rms_scale(values, gain):
    return values * lax.rsqrt(jnp.mean(values * values, axis=-1, keepdims=True) + 1e-06) * gain


def exchange_kernel(axis, count, gather, x_ref, out_ref, send_sem, recv_sem, own_sem):
    me = lax.axis_index(axis)
    barrier = pltpu.get_barrier_semaphore()
    for step in range(1, count):
        pl.semaphore_signal(
            barrier, inc=1, device_id={axis: lax.rem(me + step, count)}, device_id_type=MESH
        )
    pl.semaphore_wait(barrier, count - 1)
    copies = []
    for step in range(1, count):
        peer = lax.rem(me + step, count)
        copy = pltpu.make_async_remote_copy(
            src_ref=x_ref if gather else x_ref.at[peer],
            dst_ref=out_ref.at[me],
            send_sem=send_sem.at[step],
            recv_sem=recv_sem.at[step],
            device_id={axis: peer},
            device_id_type=MESH,
        )
        copy.start()
        copies.append(copy)
    own = pltpu.make_async_copy(x_ref if gather else x_ref.at[me], out_ref.at[me], own_sem)
    own.start()
    own.wait()
    for copy in copies:
        copy.wait()


def exchange(x, axis, gather, collective_id):
    count = lax.axis_size(axis)
    shape = ((count,) + x.shape) if gather else x.shape
    return pl.pallas_call(
        functools.partial(exchange_kernel, axis, count, gather),
        out_shape=jax.ShapeDtypeStruct(shape, x.dtype),
        in_specs=[VMEM],
        out_specs=VMEM,
        scratch_shapes=[
            pltpu.SemaphoreType.DMA((count,)),
            pltpu.SemaphoreType.DMA((count,)),
            pltpu.SemaphoreType.DMA,
        ],
        compiler_params=pltpu.CompilerParams(collective_id=collective_id, has_side_effects=True),
        name=f"exchange_{collective_id}",
    )(x)


def ring_kernel(count, qkv_ref, wout_ref, qkv_out, wout_out, send_sem, recv_sem, own_sem):
    me = lax.axis_index("seq")
    odd = lax.rem(me, 2)
    place = (1 - odd) * (me // 2) + odd * (count - 1 - me // 2)

    def index_of(position):
        position = lax.rem(position + count, count)
        late = position // (count // 2)
        return (1 - late) * 2 * position + late * (2 * (count - 1 - position) + 1)

    neighbours = (index_of(place + 1), index_of(place - 1))
    barrier = pltpu.get_barrier_semaphore()
    for neighbour in neighbours:
        pl.semaphore_signal(barrier, inc=1, device_id={"seq": neighbour}, device_id_type=MESH)
    pl.semaphore_wait(barrier, 2)
    far, near = count // 2, count - 1 - count // 2
    pieces = 4

    def slot(piece, source):
        return qkv_out.at[piece, source] if piece < 3 else wout_out.at[source]

    def own(piece):
        return qkv_ref.at[piece] if piece < 3 else wout_ref

    copies = {}
    for step in range(far):
        for piece in range(pieces):
            for way in range(2):
                hops = far if (piece < 2) == (way == 0) else near
                if step >= hops:
                    continue
                source = index_of(place - step if way == 0 else place + step)
                if step > 0:
                    copies[step - 1, piece, way].wait_recv()
                copy = pltpu.make_async_remote_copy(
                    src_ref=own(piece) if step == 0 else slot(piece, source),
                    dst_ref=slot(piece, source),
                    send_sem=send_sem.at[step, piece, way],
                    recv_sem=recv_sem.at[step, piece, way],
                    device_id={"seq": neighbours[way]},
                    device_id_type=MESH,
                )
                copy.start()
                copies[step, piece, way] = copy
    kept = [pltpu.make_async_copy(own(p), slot(p, me), own_sem.at[p]) for p in range(pieces)]
    for copy in kept:
        copy.start()
    for copy in kept:
        copy.wait()
    for (step, piece, way), copy in copies.items():
        if (step + 1, piece, way) not in copies:
            copy.wait_recv()
    for copy in copies.values():
        copy.wait_send()


def ring_weights(w_qkv, w_out):
    count = lax.axis_size("seq")
    far = count // 2
    return pl.pallas_call(
        functools.partial(ring_kernel, count),
        out_shape=(
            jax.ShapeDtypeStruct((3, count) + w_qkv.shape[1:], w_qkv.dtype),
            jax.ShapeDtypeStruct((count,) + w_out.shape, w_out.dtype),
        ),
        in_specs=[VMEM, VMEM],
        out_specs=(VMEM, VMEM),
        scratch_shapes=[
            pltpu.SemaphoreType.DMA((far, 4, 2)),
            pltpu.SemaphoreType.DMA((far, 4, 2)),
            pltpu.SemaphoreType.DMA((4,)),
        ],
        compiler_params=pltpu.CompilerParams(collective_id=0, has_side_effects=True),
        name="ring_weights",
    )(w_qkv, w_out)


def frame_attention(query, key, value, unit_order, head_size):
    unit_count = unit_order.shape[0]
    patch_count = unit_count * 4
    ranks = jnp.sum(
        jnp.where(
            unit_order[None, :] == (jnp.arange(patch_count) // 4)[:, None],
            jnp.arange(unit_count)[None, :] // (WIN // 4),
            0,
        ),
        axis=1,
    )
    same = ranks[:, None] == ranks[None, :]
    scores = jnp.einsum(
        "qhd,khd->hqk", query, key, preferred_element_type=jnp.float32
    ) * head_size ** (-0.5)
    scores = jnp.where(same[None], scores, -jnp.inf)
    weights = jax.nn.softmax(scores, axis=-1).astype(jnp.bfloat16)
    return jnp.einsum(
        "hqk,khd->qhd", weights, value, preferred_element_type=jnp.float32
    ).astype(jnp.bfloat16)


def on_device(
    patches,
    norm_gain,
    w_qkv,
    w_out,
    window_order,
    merge_gain,
    w_kv,
    queries,
    suffix_kv,
    question_lengths,
    frame_range,
):
    head_count = lax.axis_size("head")
    seq_count = lax.axis_size("seq")
    row_count = patches.shape[0]
    frame_count = window_order.shape[0]
    columns = w_qkv.shape[2]
    head_size = VD // VH
    local_heads = columns // head_size
    source = patches.astype(jnp.float32)
    normed = rms_scale(source, norm_gain).astype(jnp.bfloat16)
    qkv_all, w_out_all = ring_weights(w_qkv.transpose(1, 0, 2), w_out)
    qkv_all = qkv_all.reshape(3, -1, columns)
    query, key, value = [
        jnp.dot(normed, qkv_all[part], preferred_element_type=jnp.float32)
        .astype(jnp.bfloat16)
        .reshape(frame_count, -1, local_heads, head_size)
        for part in range(3)
    ]
    attended = jax.vmap(
        lambda q, k, v, order: frame_attention(q, k, v, order, head_size)
    )(query, key, value, window_order).reshape(row_count, columns)
    w_full = w_out_all.transpose(1, 0, 2).reshape(columns, VD)
    share_rows = row_count // head_count
    partial = jnp.dot(attended, w_full, preferred_element_type=jnp.float32).astype(jnp.bfloat16)
    parts = exchange(partial.reshape(head_count, share_rows, VD), "head", False, 1)
    shared = jnp.sum(parts.astype(jnp.float32), axis=0)
    own_rows = lax.dynamic_slice_in_dim(source, lax.axis_index("head") * share_rows, share_rows, 0)
    merged = rms_scale(own_rows + shared, merge_gain).astype(jnp.bfloat16)
    share_tokens = share_rows // 4
    depth = w_kv.shape[0]
    merged = merged.reshape(share_tokens, seq_count, depth).transpose(1, 0, 2)
    merged = exchange(merged, "seq", False, 2)
    merged = exchange(merged, "head", True, 3)
    merged = merged.transpose(1, 0, 2, 3).reshape(-1, depth)
    kv_columns = w_kv.shape[2]
    partial = jnp.dot(
        merged, w_kv.reshape(depth, 2 * kv_columns), preferred_element_type=jnp.float32
    ).astype(jnp.bfloat16)
    parts = exchange(partial.reshape(seq_count, -1, 2 * kv_columns), "seq", False, 4)
    visual = jnp.sum(parts.astype(jnp.float32), axis=0).astype(jnp.bfloat16)
    visual = exchange(visual, "seq", True, 5).reshape(-1, 2 * kv_columns)

    token_count = visual.shape[0]
    quest_count = queries.shape[0]
    span = suffix_kv.shape[1]
    kv_local = kv_columns // HD
    asking = queries.reshape(quest_count, kv_local, -1, HD)
    frame_tokens = FPATCH // 4
    seq_index = lax.axis_index("seq")
    bounds = lax.dynamic_slice_in_dim(frame_range, seq_index * quest_count, quest_count, 0)
    frame_index = jnp.arange(token_count) // frame_tokens
    live = (frame_index[None, :] >= bounds[:, 0:1]) & (frame_index[None, :] < bounds[:, 1:2])
    suffix_live = jnp.arange(span)[None, :] < question_lengths[:, None]
    suffix = suffix_kv.reshape(quest_count, span, 2, kv_local, HD)
    answers = []
    for g in range(kv_local):
        ask = asking[:, g]
        keys = visual[:, g * HD : (g + 1) * HD]
        values = visual[:, kv_columns + g * HD : kv_columns + (g + 1) * HD]
        scores = jnp.einsum(
            "qjd,nd->qjn", ask, keys, preferred_element_type=jnp.float32
        ) * HD ** (-0.5)
        scores = jnp.where(live[:, None, :], scores, -jnp.inf)
        tail = jnp.einsum(
            "qjd,qsd->qjs", ask, suffix[:, :, 0, g], preferred_element_type=jnp.float32
        ) * HD ** (-0.5)
        tail = jnp.where(suffix_live[:, None, :], tail, -jnp.inf)
        highest = jnp.maximum(
            jnp.max(scores, axis=-1, keepdims=True), jnp.max(tail, axis=-1, keepdims=True)
        )
        weights = jnp.exp(scores - highest)
        tail_weights = jnp.exp(tail - highest)
        totals = jnp.sum(weights, axis=-1, keepdims=True) + jnp.sum(
            tail_weights, axis=-1, keepdims=True
        )
        mixed = jnp.einsum(
            "qjn,nd->qjd", weights.astype(jnp.bfloat16), values, preferred_element_type=jnp.float32
        ) + jnp.einsum(
            "qjs,qsd->qjd",
            tail_weights.astype(jnp.bfloat16),
            suffix[:, :, 1, g],
            preferred_element_type=jnp.float32,
        )
        answers.append((mixed / totals).astype(jnp.bfloat16))
    return jnp.stack(answers, axis=1).reshape(quest_count, -1)


def fused_kernel(
    seq_count,
    head_count,
    patches_ref,
    norm_gain_ref,
    merge_gain_ref,
    wq_ref,
    wo_ref,
    order_ref,
    wkv_ref,
    asks_ref,
    suffix_ref,
    lengths_ref,
    range_ref,
    out_ref,
    rows_all,
    order_all,
    normed,
    wq_all,
    wo_all,
    wkv_all,
    asks_all,
    swap_out,
    swap_in,
    core_out,
    core_in,
    side_out,
    side_in,
    merged_out,
    merged_all,
    kv_out,
    kv_in,
    mixed_out,
    mixed_in,
    level_out,
    level_in,
    send_sems,
    recv_sems,
):
    planes = seq_count // 2
    me = lax.axis_index("seq")
    head = lax.axis_index("head")
    z, y = me // 2, lax.rem(me, 2)
    x, c = head // 2, lax.rem(head, 2)
    half = lax.rem(z, 2)
    group = 2 * c + x
    frame_rows, depth = patches_ref.shape
    group_rows = frame_rows // head_count
    share = group_rows // 4
    head_size = VD // VH
    own_width = 2 * head_size

    def at(z_to, y_to, x_to, c_to):
        return {"seq": 2 * z_to + y_to, "head": 2 * x_to + c_to}

    partner = z + 1 - 2 * half
    across = at(z, 1 - y, x, c)
    beside = at(z, y, 1 - x, c)
    twin = at(z, y, x, 1 - c)
    paired = at(partner, y, x, c)

    def plane_at(step):
        return lax.rem(z + step, planes)

    def plane_from(step):
        return lax.rem(z + planes - step, planes)

    barrier = pltpu.get_barrier_semaphore()
    peers = [
        {"seq": lax.rem(me + step, seq_count), "head": head} for step in range(1, seq_count)
    ] + [beside, twin]
    for peer in peers:
        pl.semaphore_signal(barrier, inc=1, device_id=peer, device_id_type=MESH)

    copies = {}

    def send(name, src, dst, device):
        slot = len(copies)
        copy = pltpu.make_async_remote_copy(
            src_ref=src,
            dst_ref=dst,
            send_sem=send_sems.at[slot],
            recv_sem=recv_sems.at[slot],
            device_id=device,
            device_id_type=MESH,
        )
        copy.start()
        copies[name] = copy

    def arrived(name):
        copies[name].wait_recv()

    for part in range(head_count):
        row = lax.broadcasted_iota(jnp.int32, (group_rows, frame_rows), 0)
        place = lax.broadcasted_iota(jnp.int32, (group_rows, frame_rows), 1)
        picked = 4 * (share * part + lax.rem(row, share)) + row // share
        pick = jnp.where(place == picked, 1.0, 0.0).astype(jnp.bfloat16)
        rows_all[half, pl.ds(part * group_rows, group_rows), :] = jnp.dot(
            pick, patches_ref[...], preferred_element_type=jnp.float32
        ).astype(jnp.bfloat16)
    order_all[half] = order_ref[...]
    wq_all[me] = wq_ref[half]
    wo_all[me] = wo_ref[...]
    wkv_all[y] = wkv_ref[...]
    asks_all[me] = asks_ref[...]
    pl.semaphore_wait(barrier, len(peers))

    steps = [1] + ([planes - 1] if planes > 2 else []) + list(range(2, planes - 1))
    quarter = pl.ds(pl.multiple_of(group * group_rows, group_rows), group_rows)
    send("order", order_all.at[half], order_all.at[half], paired)
    send("rows", rows_all.at[half, quarter], rows_all.at[half, quarter], paired)
    send("wq_y0", wq_ref.at[half], wq_all.at[me], across)
    for step in steps:
        to = plane_at(step)
        send(f"wq_z{step}", wq_ref.at[lax.rem(to, 2)], wq_all.at[me], at(to, y, x, c))
    send("wo_y0", wo_ref, wo_all.at[me], across)
    for step in steps:
        send(f"wo_z{step}", wo_ref, wo_all.at[me], at(plane_at(step), y, x, c))
    for step in range(1, seq_count):
        send(
            f"ask{step}",
            asks_ref,
            asks_all.at[me],
            {"seq": lax.rem(me + step, seq_count), "head": head},
        )

    def normalise(slot):
        for part in range(head_count):
            rows = pl.ds(part * group_rows, group_rows)
            source = rows_all[slot, rows, :].astype(jnp.float32)
            normed[slot, rows, :] = rms_scale(source, norm_gain_ref[...]).astype(jnp.bfloat16)

    normalise(half)

    span = suffix_ref.shape[2]
    kv_heads = asks_ref.shape[0]
    asking = asks_ref.shape[1] // suffix_ref.shape[0]
    scale = HD ** (-0.5)
    tails = []
    for g in range(kv_heads):
        columns = slice(g * HD, (g + 1) * HD)
        mixes, levels = [], []
        for q in range(suffix_ref.shape[0]):
            ask = asks_ref[g, q * asking : (q + 1) * asking, :]
            keys = suffix_ref[q, 0, :, columns]
            values = suffix_ref[q, 1, :, columns]
            scores = (
                lax.dot_general(
                    ask, keys, (((1,), (1,)), ((), ())), preferred_element_type=jnp.float32
                )
                * scale
            )
            place = lax.broadcasted_iota(jnp.int32, scores.shape, 1)
            scores = jnp.where(place < lengths_ref[q], scores, -1e30)
            highest = jnp.max(scores, axis=1, keepdims=True)
            weights = jnp.exp(scores - highest)
            total = jnp.sum(weights, axis=1, keepdims=True)
            mix = jnp.dot(
                weights.astype(jnp.bfloat16), values, preferred_element_type=jnp.float32
            )
            mixes.append(mix / total)
            levels.append(highest + jnp.log(total))
        tails.append((jnp.concatenate(mixes, axis=0), jnp.concatenate(levels, axis=0)))

    def forward(name, ref, index, device):
        send(name, ref.at[index], ref.at[index], device)

    other = 1 - half
    arrived("rows")
    send("rows_x", rows_all.at[other, quarter], rows_all.at[other, quarter], beside)
    send("rows_c", rows_all.at[other, quarter], rows_all.at[other, quarter], twin)
    first, second = steps[0], (steps[1] if len(steps) > 1 else None)

    def wq_step(step):
        arrived(f"wq_z{step}")
        forward(f"wq_y{step}", wq_all, 2 * plane_from(step) + y, across)

    wq_step(steps[0])
    arrived("rows_x")
    side_quarter = pl.ds(
        pl.multiple_of((2 * c + 1 - x) * group_rows, group_rows), group_rows
    )
    send("rows_xc", rows_all.at[other, side_quarter], rows_all.at[other, side_quarter], twin)
    for step in steps[1:2]:
        wq_step(step)
    arrived("rows_c")
    arrived("rows_xc")
    arrived("order")
    normalise(other)
    for step in steps[2:]:
        wq_step(step)
    for step in [0] + steps:
        arrived(f"wq_y{step}")

    def wo_step(step):
        arrived(f"wo_z{step}")
        forward(f"wo_y{step}", wo_all, 2 * plane_from(step) + y, across)

    lane = lax.broadcasted_iota(jnp.int32, (frame_rows, 256), 1)

    def attend(slot):
        unit_count = order_ref.shape[1]
        row = lax.broadcasted_iota(jnp.int32, (frame_rows, unit_count), 0)
        unit = row // group_rows * share + lax.rem(row, share)
        place = lax.broadcasted_iota(jnp.int32, (frame_rows, unit_count), 1)
        window = jnp.sum(
            jnp.where(order_all[slot] == unit, place // (WIN // 4), 0).astype(jnp.float32),
            axis=1,
            keepdims=True,
        )
        sort = lax.broadcasted_iota(jnp.int32, (frame_rows, 128), 1).astype(jnp.float32)
        member = jnp.where(window == sort, 1.0, 0.0).astype(jnp.bfloat16)
        same = (
            lax.dot_general(
                member, member, (((1,), (1,)), ((), ())), preferred_element_type=jnp.float32
            )
            > 0.5
        )
        qkv = jnp.dot(
            normed[slot],
            wq_all[...].reshape(depth, wq_ref.shape[2]),
            preferred_element_type=jnp.float32,
        )
        width = qkv.shape[1]
        query = qkv[:, :256].astype(jnp.bfloat16)
        key = pltpu.roll(qkv, width - own_width, 1)[:, :256].astype(jnp.bfloat16)
        value = pltpu.roll(qkv, width - 2 * own_width, 1)[:, :256].astype(jnp.bfloat16)
        mixed = jnp.zeros((frame_rows, 256), jnp.float32)
        for i in range(2):
            inside = (lane >= i * head_size) & (lane < (i + 1) * head_size)
            scores = lax.dot_general(
                jnp.where(inside, query, jnp.zeros_like(query)),
                key,
                (((1,), (1,)), ((), ())),
                preferred_element_type=jnp.float32,
            ) * head_size ** (-0.5)
            scores = jnp.where(same, scores, -1e30)
            weights = jnp.exp(scores - jnp.max(scores, axis=1, keepdims=True))
            weights = weights / jnp.sum(weights, axis=1, keepdims=True)
            product = jnp.dot(
                weights.astype(jnp.bfloat16), value, preferred_element_type=jnp.float32
            )
            mixed = jnp.where(inside, product, mixed)
        shifted = pltpu.roll(mixed, own_width - 128, 1)
        return jnp.where(half == 0, mixed, shifted).astype(jnp.bfloat16)

    swap_out[...] = attend(other)
    send("swap", swap_out, swap_in, paired)
    for step in steps:
        wo_step(step)
    send("wkv", wkv_ref, wkv_all.at[y], across)
    mine = attend(half)
    arrived("swap")
    theirs = swap_in[...]
    low = jnp.where(half == 0, mine, theirs)
    high = jnp.where(half == 0, theirs, mine)
    attended = jnp.concatenate(
        [low[:, :128], low[:, 128:] + high[:, :128], high[:, 128:]], axis=1
    )
    for step in [0] + steps:
        arrived(f"wo_y{step}")
    partial = lax.dot_general(
        attended,
        wo_all[...].reshape(depth, wo_ref.shape[1]),
        (((1,), (1,)), ((), ())),
        preferred_element_type=jnp.float32,
    )
    both = 2 * group_rows
    top, bottom = partial[:both], partial[both:]
    core_out[...] = jnp.where(c == 0, bottom, top).astype(jnp.bfloat16)
    send("core", core_out, core_in, twin)
    kept = jnp.where(c == 0, top, bottom)
    arrived("core")
    kept = kept + core_in[...].astype(jnp.float32)
    top, bottom = kept[:group_rows], kept[group_rows:]
    side_out[...] = jnp.where(x == 0, bottom, top).astype(jnp.bfloat16)
    send("side", side_out, side_in, beside)
    kept = jnp.where(x == 0, top, bottom) + rows_all[half, quarter, :].astype(jnp.float32)
    arrived("side")
    hidden = kept + side_in[...].astype(jnp.float32)
    merged = rms_scale(hidden, merge_gain_ref[...]).astype(jnp.bfloat16)
    merged_out[...] = merged.reshape(planes, share, depth)

    merged_all[z, group] = merged_out[z]
    send("mx0", merged_out.at[z], merged_all.at[z, group], beside)
    send("mc0", merged_out.at[z], merged_all.at[z, group], twin)
    for step in steps:
        to = plane_at(step)
        send(f"mz{step}", merged_out.at[to], merged_all.at[z, group], at(to, y, x, c))
    side_group = 2 * c + 1 - x
    for step in steps:
        arrived(f"mz{step}")
        source = merged_all.at[plane_from(step), group]
        send(f"mx{step}", source, source, beside)
        send(f"mc{step}", source, source, twin)
    for step in [0] + steps:
        arrived(f"mx{step}")
        source = merged_all.at[plane_from(step), side_group]
        send(f"mxc{step}", source, source, twin)
    arrived("wkv")
    for step in [0] + steps:
        arrived(f"mc{step}")
        arrived(f"mxc{step}")
    frame_tokens = frame_rows // 4
    width = wkv_ref.shape[1]
    weights = wkv_all[...].reshape(depth, width)
    for step in steps[::-1] + [0]:
        to = plane_at(step)
        block = merged_all[to].reshape(frame_tokens, depth)
        kv_out[step] = jnp.dot(block, weights, preferred_element_type=jnp.float32).astype(
            jnp.bfloat16
        )
        if step:
            send(f"kv{step}", kv_out.at[step], kv_in.at[step], at(to, y, x, c))
    visual = kv_out[0].astype(jnp.float32)
    for step in steps:
        arrived(f"kv{step}")
        visual = visual + kv_in[step].astype(jnp.float32)
    visual = visual.astype(jnp.bfloat16)

    for step in range(1, seq_count):
        arrived(f"ask{step}")
    all_rows = seq_count * asks_ref.shape[1]
    own_rows = asks_ref.shape[1]
    questions = range_ref.shape[0]
    seen = jnp.concatenate(
        [
            jnp.full(
                (asking, 1),
                jnp.where((range_ref[q, 0] <= me) & (me < range_ref[q, 1]), 0.0, -1e30),
                jnp.float32,
            )
            for q in range(questions)
        ],
        axis=0,
    )
    level_out[...] = jnp.zeros_like(level_out)
    diagonal = lax.broadcasted_iota(
        jnp.int32, (all_rows, all_rows), 0
    ) == lax.broadcasted_iota(jnp.int32, (all_rows, all_rows), 1)
    for g in range(kv_heads):
        ask = asks_all[:, g].reshape(all_rows, HD)
        keys = visual[:, g * HD : (g + 1) * HD]
        values = visual[:, (kv_heads + g) * HD : (kv_heads + g + 1) * HD]
        scores = (
            lax.dot_general(
                ask, keys, (((1,), (1,)), ((), ())), preferred_element_type=jnp.float32
            )
            * scale
        )
        highest = jnp.max(scores, axis=1, keepdims=True)
        weights = jnp.exp(scores - highest)
        total = jnp.sum(weights, axis=1, keepdims=True)
        mix = (
            jnp.dot(weights.astype(jnp.bfloat16), values, preferred_element_type=jnp.float32)
            / total
        )
        level = highest + jnp.log(total) + seen
        mixed_out[:, g] = mix.astype(jnp.bfloat16).reshape(seq_count, own_rows, HD)
        level_out[g : g + 1, :] = jnp.sum(
            jnp.where(diagonal, level, 0.0), axis=0, keepdims=True
        )
    mixed_in[me] = mixed_out[me]
    level_in[me] = level_out[...]
    for step in range(1, seq_count):
        to = lax.rem(me + step, seq_count)
        send(f"mix{step}", mixed_out.at[to], mixed_in.at[me], {"seq": to, "head": head})
        send(f"level{step}", level_out, level_in.at[me], {"seq": to, "head": head})
    for step in range(1, seq_count):
        arrived(f"mix{step}")
        arrived(f"level{step}")
    row = lax.broadcasted_iota(jnp.int32, (own_rows, all_rows), 0)
    place = lax.broadcasted_iota(jnp.int32, (own_rows, all_rows), 1)
    chosen = place == row + me * own_rows
    for g in range(kv_heads):
        mix, level = tails[g]
        levels = [
            jnp.sum(jnp.where(chosen, level_in[s, g : g + 1, :], 0.0), axis=1, keepdims=True)
            for s in range(seq_count)
        ]
        highest = level
        for other_level in levels:
            highest = jnp.maximum(highest, other_level)
        share_of = jnp.exp(level - highest)
        total = share_of
        answer = share_of * mix
        for s in range(seq_count):
            share_of = jnp.exp(levels[s] - highest)
            total = total + share_of
            answer = answer + share_of * mixed_in[s, g].astype(jnp.float32)
        out_ref[g] = (answer / total).astype(jnp.bfloat16)
    for copy in copies.values():
        copy.wait_send()


def fused(
    patches,
    norm_gain,
    w_qkv,
    w_out,
    window_order,
    merge_gain,
    w_kv,
    queries,
    suffix_kv,
    question_lengths,
    frame_range,
):
    seq_count, head_count = lax.axis_size("seq"), lax.axis_size("head")
    planes = seq_count // 2
    frame_rows, depth = patches.shape
    rows, _, columns = w_qkv.shape
    half = columns // 2
    quest_count = queries.shape[0]
    kv_columns = w_kv.shape[2]
    kv_heads = kv_columns // HD
    bf16 = jnp.bfloat16
    wq = w_qkv.transpose(1, 0, 2).reshape(3, rows, 2, half).transpose(2, 1, 0, 3)
    wq = wq.reshape(2, rows, 3 * half)
    wq_width = -(-3 * half // 128) * 128
    wq = jnp.pad(wq, ((0, 0), (0, 0), (0, wq_width - 3 * half)))
    wo_width = -(-columns // 128) * 128
    wo = jnp.pad(w_out.T, ((0, 0), (0, wo_width - columns)))
    wkv = w_kv.reshape(w_kv.shape[0], 2 * kv_columns)
    asks = queries.reshape(quest_count, kv_heads, -1, HD).transpose(1, 0, 2, 3)
    asking = asks.shape[2]
    asks = asks.reshape(kv_heads, quest_count * asking, HD)
    own_rows = quest_count * asking
    suffix = suffix_kv.transpose(0, 2, 1, 3)
    group_rows = frame_rows // head_count
    share = group_rows // 4
    messages = 160
    smem = pl.BlockSpec(memory_space=pltpu.SMEM)
    answers = pl.pallas_call(
        functools.partial(fused_kernel, seq_count, head_count),
        out_shape=jax.ShapeDtypeStruct((kv_heads, own_rows, HD), bf16),
        in_specs=[VMEM] * 9 + [smem] * 2,
        out_specs=VMEM,
        scratch_shapes=[
            pltpu.VMEM((2, frame_rows, depth), bf16),
            pltpu.VMEM((2,) + window_order.shape, jnp.int32),
            pltpu.VMEM((2, frame_rows, depth), bf16),
            pltpu.VMEM((seq_count, rows, wq_width), bf16),
            pltpu.VMEM((seq_count,) + wo.shape, bf16),
            pltpu.VMEM((2,) + wkv.shape, bf16),
            pltpu.VMEM((seq_count,) + asks.shape, bf16),
            pltpu.VMEM((frame_rows, 256), bf16),
            pltpu.VMEM((frame_rows, 256), bf16),
            pltpu.VMEM((2 * group_rows, depth), bf16),
            pltpu.VMEM((2 * group_rows, depth), bf16),
            pltpu.VMEM((group_rows, depth), bf16),
            pltpu.VMEM((group_rows, depth), bf16),
            pltpu.VMEM((planes, share, depth), bf16),
            pltpu.VMEM((planes, head_count, share, depth), bf16),
            pltpu.VMEM((planes, frame_rows // 4, 2 * kv_columns), bf16),
            pltpu.VMEM((planes, frame_rows // 4, 2 * kv_columns), bf16),
            pltpu.VMEM((seq_count,) + asks.shape, bf16),
            pltpu.VMEM((seq_count,) + asks.shape, bf16),
            pltpu.VMEM((8, seq_count * own_rows), jnp.float32),
            pltpu.VMEM((seq_count, 8, seq_count * own_rows), jnp.float32),
            pltpu.SemaphoreType.DMA((messages,)),
            pltpu.SemaphoreType.DMA((messages,)),
        ],
        compiler_params=pltpu.CompilerParams(
            collective_id=0, has_side_effects=True, vmem_limit_bytes=60 << 20
        ),
        name="fused",
    )(
        patches,
        norm_gain.reshape(1, -1),
        merge_gain.reshape(1, -1),
        wq,
        wo,
        window_order,
        wkv,
        asks,
        suffix,
        question_lengths,
        frame_range,
    )
    answers = answers.reshape(kv_heads, quest_count, asking, HD).transpose(1, 0, 2, 3)
    return answers.reshape(quest_count, -1)


def device_program(*arguments):
    patches, _, w_qkv, _, window_order = arguments[:5]
    paired = lax.axis_size("seq") == 8 and lax.axis_size("head") == 4
    whole = patches.shape[0] == FPATCH and window_order.shape[0] == 1
    if paired and whole and w_qkv.shape[0] % 16 == 0:
        return fused(*arguments)
    return on_device(*arguments)


def solution(mesh):
    placed = (
        P("seq", None),
        P(),
        P("seq", None, "head"),
        P("head", "seq"),
        P("seq", None),
        P(),
        P("seq", None, "head"),
        P("seq", "head"),
        P("seq", None, None, "head"),
        P("seq"),
        P(),
    )
    return jax.shard_map(
        device_program, mesh=mesh, in_specs=placed, out_specs=P("seq", "head"), check_vma=False
    )
```

```python
import functools

import jax
import jax.numpy as jnp
from jax import lax
from jax.experimental import pallas as pl
from jax.experimental.pallas import tpu as pltpu
from jax.sharding import PartitionSpec as P

VD = 1280
VH = 16
HD = 128
FPATCH = 256
WIN = 64

MESH = pl.DeviceIdType.MESH
VMEM = pl.BlockSpec(memory_space=pltpu.VMEM)


def rms_scale(values, gain):
    return values * lax.rsqrt(jnp.mean(values * values, axis=-1, keepdims=True) + 1e-06) * gain


def exchange_kernel(axis, count, gather, x_ref, out_ref, send_sem, recv_sem, own_sem):
    me = lax.axis_index(axis)
    barrier = pltpu.get_barrier_semaphore()
    for step in range(1, count):
        pl.semaphore_signal(
            barrier, inc=1, device_id={axis: lax.rem(me + step, count)}, device_id_type=MESH
        )
    pl.semaphore_wait(barrier, count - 1)
    copies = []
    for step in range(1, count):
        peer = lax.rem(me + step, count)
        copy = pltpu.make_async_remote_copy(
            src_ref=x_ref if gather else x_ref.at[peer],
            dst_ref=out_ref.at[me],
            send_sem=send_sem.at[step],
            recv_sem=recv_sem.at[step],
            device_id={axis: peer},
            device_id_type=MESH,
        )
        copy.start()
        copies.append(copy)
    own = pltpu.make_async_copy(x_ref if gather else x_ref.at[me], out_ref.at[me], own_sem)
    own.start()
    own.wait()
    for copy in copies:
        copy.wait()


def exchange(x, axis, gather, collective_id):
    count = lax.axis_size(axis)
    shape = ((count,) + x.shape) if gather else x.shape
    return pl.pallas_call(
        functools.partial(exchange_kernel, axis, count, gather),
        out_shape=jax.ShapeDtypeStruct(shape, x.dtype),
        in_specs=[VMEM],
        out_specs=VMEM,
        scratch_shapes=[
            pltpu.SemaphoreType.DMA((count,)),
            pltpu.SemaphoreType.DMA((count,)),
            pltpu.SemaphoreType.DMA,
        ],
        compiler_params=pltpu.CompilerParams(collective_id=collective_id, has_side_effects=True),
        name=f"exchange_{collective_id}",
    )(x)


def ring_kernel(count, qkv_ref, wout_ref, qkv_out, wout_out, send_sem, recv_sem, own_sem):
    me = lax.axis_index("seq")
    odd = lax.rem(me, 2)
    place = (1 - odd) * (me // 2) + odd * (count - 1 - me // 2)

    def index_of(position):
        position = lax.rem(position + count, count)
        late = position // (count // 2)
        return (1 - late) * 2 * position + late * (2 * (count - 1 - position) + 1)

    neighbours = (index_of(place + 1), index_of(place - 1))
    barrier = pltpu.get_barrier_semaphore()
    for neighbour in neighbours:
        pl.semaphore_signal(barrier, inc=1, device_id={"seq": neighbour}, device_id_type=MESH)
    pl.semaphore_wait(barrier, 2)
    far, near = count // 2, count - 1 - count // 2
    pieces = 4

    def slot(piece, source):
        return qkv_out.at[piece, source] if piece < 3 else wout_out.at[source]

    def own(piece):
        return qkv_ref.at[piece] if piece < 3 else wout_ref

    copies = {}
    for step in range(far):
        for piece in range(pieces):
            for way in range(2):
                hops = far if (piece < 2) == (way == 0) else near
                if step >= hops:
                    continue
                source = index_of(place - step if way == 0 else place + step)
                if step > 0:
                    copies[step - 1, piece, way].wait_recv()
                copy = pltpu.make_async_remote_copy(
                    src_ref=own(piece) if step == 0 else slot(piece, source),
                    dst_ref=slot(piece, source),
                    send_sem=send_sem.at[step, piece, way],
                    recv_sem=recv_sem.at[step, piece, way],
                    device_id={"seq": neighbours[way]},
                    device_id_type=MESH,
                )
                copy.start()
                copies[step, piece, way] = copy
    kept = [pltpu.make_async_copy(own(p), slot(p, me), own_sem.at[p]) for p in range(pieces)]
    for copy in kept:
        copy.start()
    for copy in kept:
        copy.wait()
    for (step, piece, way), copy in copies.items():
        if (step + 1, piece, way) not in copies:
            copy.wait_recv()
    for copy in copies.values():
        copy.wait_send()


def ring_weights(w_qkv, w_out):
    count = lax.axis_size("seq")
    far = count // 2
    return pl.pallas_call(
        functools.partial(ring_kernel, count),
        out_shape=(
            jax.ShapeDtypeStruct((3, count) + w_qkv.shape[1:], w_qkv.dtype),
            jax.ShapeDtypeStruct((count,) + w_out.shape, w_out.dtype),
        ),
        in_specs=[VMEM, VMEM],
        out_specs=(VMEM, VMEM),
        scratch_shapes=[
            pltpu.SemaphoreType.DMA((far, 4, 2)),
            pltpu.SemaphoreType.DMA((far, 4, 2)),
            pltpu.SemaphoreType.DMA((4,)),
        ],
        compiler_params=pltpu.CompilerParams(collective_id=0, has_side_effects=True),
        name="ring_weights",
    )(w_qkv, w_out)


def frame_attention(query, key, value, unit_order, head_size):
    unit_count = unit_order.shape[0]
    patch_count = unit_count * 4
    ranks = jnp.sum(
        jnp.where(
            unit_order[None, :] == (jnp.arange(patch_count) // 4)[:, None],
            jnp.arange(unit_count)[None, :] // (WIN // 4),
            0,
        ),
        axis=1,
    )
    same = ranks[:, None] == ranks[None, :]
    scores = jnp.einsum(
        "qhd,khd->hqk", query, key, preferred_element_type=jnp.float32
    ) * head_size ** (-0.5)
    scores = jnp.where(same[None], scores, -jnp.inf)
    weights = jax.nn.softmax(scores, axis=-1).astype(jnp.bfloat16)
    return jnp.einsum(
        "hqk,khd->qhd", weights, value, preferred_element_type=jnp.float32
    ).astype(jnp.bfloat16)


def on_device(
    patches,
    norm_gain,
    w_qkv,
    w_out,
    window_order,
    merge_gain,
    w_kv,
    queries,
    suffix_kv,
    question_lengths,
    frame_range,
):
    head_count = lax.axis_size("head")
    seq_count = lax.axis_size("seq")
    row_count = patches.shape[0]
    frame_count = window_order.shape[0]
    columns = w_qkv.shape[2]
    head_size = VD // VH
    local_heads = columns // head_size
    source = patches.astype(jnp.float32)
    normed = rms_scale(source, norm_gain).astype(jnp.bfloat16)
    qkv_all, w_out_all = ring_weights(w_qkv.transpose(1, 0, 2), w_out)
    qkv_all = qkv_all.reshape(3, -1, columns)
    query, key, value = [
        jnp.dot(normed, qkv_all[part], preferred_element_type=jnp.float32)
        .astype(jnp.bfloat16)
        .reshape(frame_count, -1, local_heads, head_size)
        for part in range(3)
    ]
    attended = jax.vmap(
        lambda q, k, v, order: frame_attention(q, k, v, order, head_size)
    )(query, key, value, window_order).reshape(row_count, columns)
    w_full = w_out_all.transpose(1, 0, 2).reshape(columns, VD)
    share_rows = row_count // head_count
    partial = jnp.dot(attended, w_full, preferred_element_type=jnp.float32).astype(jnp.bfloat16)
    parts = exchange(partial.reshape(head_count, share_rows, VD), "head", False, 1)
    shared = jnp.sum(parts.astype(jnp.float32), axis=0)
    own_rows = lax.dynamic_slice_in_dim(source, lax.axis_index("head") * share_rows, share_rows, 0)
    merged = rms_scale(own_rows + shared, merge_gain).astype(jnp.bfloat16)
    share_tokens = share_rows // 4
    depth = w_kv.shape[0]
    merged = merged.reshape(share_tokens, seq_count, depth).transpose(1, 0, 2)
    merged = exchange(merged, "seq", False, 2)
    merged = exchange(merged, "head", True, 3)
    merged = merged.transpose(1, 0, 2, 3).reshape(-1, depth)
    kv_columns = w_kv.shape[2]
    partial = jnp.dot(
        merged, w_kv.reshape(depth, 2 * kv_columns), preferred_element_type=jnp.float32
    ).astype(jnp.bfloat16)
    parts = exchange(partial.reshape(seq_count, -1, 2 * kv_columns), "seq", False, 4)
    visual = jnp.sum(parts.astype(jnp.float32), axis=0).astype(jnp.bfloat16)
    visual = exchange(visual, "seq", True, 5).reshape(-1, 2 * kv_columns)

    token_count = visual.shape[0]
    quest_count = queries.shape[0]
    span = suffix_kv.shape[1]
    kv_local = kv_columns // HD
    asking = queries.reshape(quest_count, kv_local, -1, HD)
    frame_tokens = FPATCH // 4
    seq_index = lax.axis_index("seq")
    bounds = lax.dynamic_slice_in_dim(frame_range, seq_index * quest_count, quest_count, 0)
    frame_index = jnp.arange(token_count) // frame_tokens
    live = (frame_index[None, :] >= bounds[:, 0:1]) & (frame_index[None, :] < bounds[:, 1:2])
    suffix_live = jnp.arange(span)[None, :] < question_lengths[:, None]
    suffix = suffix_kv.reshape(quest_count, span, 2, kv_local, HD)
    answers = []
    for g in range(kv_local):
        ask = asking[:, g]
        keys = visual[:, g * HD : (g + 1) * HD]
        values = visual[:, kv_columns + g * HD : kv_columns + (g + 1) * HD]
        scores = jnp.einsum(
            "qjd,nd->qjn", ask, keys, preferred_element_type=jnp.float32
        ) * HD ** (-0.5)
        scores = jnp.where(live[:, None, :], scores, -jnp.inf)
        tail = jnp.einsum(
            "qjd,qsd->qjs", ask, suffix[:, :, 0, g], preferred_element_type=jnp.float32
        ) * HD ** (-0.5)
        tail = jnp.where(suffix_live[:, None, :], tail, -jnp.inf)
        highest = jnp.maximum(
            jnp.max(scores, axis=-1, keepdims=True), jnp.max(tail, axis=-1, keepdims=True)
        )
        weights = jnp.exp(scores - highest)
        tail_weights = jnp.exp(tail - highest)
        totals = jnp.sum(weights, axis=-1, keepdims=True) + jnp.sum(
            tail_weights, axis=-1, keepdims=True
        )
        mixed = jnp.einsum(
            "qjn,nd->qjd", weights.astype(jnp.bfloat16), values, preferred_element_type=jnp.float32
        ) + jnp.einsum(
            "qjs,qsd->qjd",
            tail_weights.astype(jnp.bfloat16),
            suffix[:, :, 1, g],
            preferred_element_type=jnp.float32,
        )
        answers.append((mixed / totals).astype(jnp.bfloat16))
    return jnp.stack(answers, axis=1).reshape(quest_count, -1)


def fused_kernel(
    seq_count,
    head_count,
    patches_ref,
    norm_gain_ref,
    merge_gain_ref,
    wqkv_ref,
    wo_ref,
    order_ref,
    wkv_ref,
    queries_ref,
    suffix_ref,
    lengths_ref,
    range_ref,
    out_ref,
    wide,
    wq_ref,
    kv_ref,
    asks_ref,
    rows_all,
    order_all,
    normed,
    wq_all,
    wo_packed,
    wo_all,
    wo_full,
    wkv_all,
    asks_all,
    swap_out,
    swap_in,
    core_out,
    core_in,
    side_out,
    side_in,
    merged_out,
    merged_all,
    key_out,
    key_in,
    value_out,
    value_in,
    mixed_out,
    mixed_in,
    level_out,
    level_in,
    send_sems,
    recv_sems,
):
    planes = seq_count // 2
    me = lax.axis_index("seq")
    head = lax.axis_index("head")
    z, y = me // 2, lax.rem(me, 2)
    x, c = head // 2, lax.rem(head, 2)
    half = lax.rem(z, 2)
    group = 2 * c + x
    frame_rows, depth = patches_ref.shape
    group_rows = frame_rows // head_count
    share = group_rows // 4
    head_size = VD // VH
    own_width = 2 * head_size

    def at(z_to, y_to, x_to, c_to):
        return {"seq": 2 * z_to + y_to, "head": 2 * x_to + c_to}

    partner = z + 1 - 2 * half
    across = at(z, 1 - y, x, c)
    beside = at(z, y, 1 - x, c)
    twin = at(z, y, x, 1 - c)
    paired = at(partner, y, x, c)

    low = z < planes // 2
    inner = (z > 0) & (z < planes - 1)

    def target(k):
        if k and planes > 2:
            k = k + jnp.where(inner, 3 - 2 * k, 0)
        return jnp.where(
            low, lax.rem(z + 1 + k, planes), lax.rem(z - 1 - k + 2 * planes, planes)
        )

    def source(j):
        depth_in = jnp.where(low, z, planes - 1 - z)
        counted = j + jnp.where(j >= depth_in, 1, 0)
        return jnp.where(low, counted, planes - 1 - counted)

    barrier = pltpu.get_barrier_semaphore()
    peers = [
        {"seq": lax.rem(me + step, seq_count), "head": head} for step in range(1, seq_count)
    ] + [beside, twin]
    for peer in peers:
        pl.semaphore_signal(barrier, inc=1, device_id=peer, device_id_type=MESH)

    taken = []
    started = []
    guarded = []

    def slots(count=1):
        taken.append(count)
        return sum(taken) - count

    def copy_of(src, dst, device, send_slot, recv_slot):
        return pltpu.make_async_remote_copy(
            src_ref=src,
            dst_ref=dst,
            send_sem=send_sems.at[send_slot],
            recv_sem=recv_sems.at[recv_slot],
            device_id=device,
            device_id_type=MESH,
        )

    def send(src, dst, device, send_slot, recv_slot):
        copy = copy_of(src, dst, device, send_slot, recv_slot)
        copy.start()
        started.append(copy)
        return copy

    def send_if(inside, src, dst, device, send_slot, recv_slot):
        copy = copy_of(src, dst, device, send_slot, recv_slot)

        @pl.when(inside)
        def _():
            copy.start()

        guarded.append((inside, copy))

    def send_all(count, slot, copy_at):
        for step in range(1, count):
            src, dst, device = copy_at(step)
            copy_of(src, dst, device, slot, slot).start()

    def left(copy):
        started[:] = [kept for kept in started if kept is not copy]
        copy.wait_send()

    def arrived(ref, slot, name):
        copy_of(ref, ref, twin, slot, slot).wait_recv()

    for part in range(head_count):
        row = lax.broadcasted_iota(jnp.int32, (group_rows, frame_rows), 0)
        place = lax.broadcasted_iota(jnp.int32, (group_rows, frame_rows), 1)
        picked = 4 * (share * part + lax.rem(row, share)) + row // share
        pick = jnp.where(place == picked, 1.0, 0.0).astype(jnp.bfloat16)
        rows_all[half, pl.ds(part * group_rows, group_rows), :] = jnp.dot(
            pick, patches_ref[...], preferred_element_type=jnp.float32
        ).astype(jnp.bfloat16)
    columns = wqkv_ref.shape[2]
    wq_width = wq_ref.shape[2]
    lane = lax.broadcasted_iota(jnp.int32, wq_ref.shape[1:], 1)
    packed = [jnp.zeros(wq_ref.shape[1:], jnp.float32)] * 2
    wide[...] = jnp.zeros_like(wide)
    for part in range(3):
        wide[part, :, :columns] = wqkv_ref[part].astype(jnp.float32)
        for side in range(2):
            shift = (part - side) * own_width
            moved = wide[part] if shift == 0 else pltpu.roll(wide[part], shift % wq_width, 1)
            inside = (lane >= part * own_width) & (lane < (part + 1) * own_width)
            packed[side] = jnp.where(inside, moved, packed[side])
    for side in range(2):
        wq_ref[side] = packed[side].astype(jnp.bfloat16)
    order_all[half] = order_ref[...]
    pl.semaphore_wait(barrier, len(peers))

    quarter = pl.ds(pl.multiple_of(group * group_rows, group_rows), group_rows)
    far = planes - 1
    order_slot, rows_slot, rows_x_slot, rows_c_slot, rows_xc_slot = (slots() for _ in range(5))
    wq_z, wq_y, wo_z, wo_y = (slots(planes) for _ in range(4))
    send(order_all.at[half], order_all.at[half], paired, order_slot, order_slot)

    def wq_send(k, inside=None):
        to = target(k)
        copy = (
            wq_ref.at[lax.rem(to, 2)],
            wq_all.at[me],
            at(to, y, x, c),
            wq_z + k,
            wq_z + z,
        )
        return send(*copy) if inside is None else send_if(inside, *copy)

    def over_y(ref, plane, base):
        own = ref.at[2 * plane + y]
        return send(own, own, across, base + plane, base + plane)

    def hear_y(ref, plane, base, name):
        arrived(ref.at[2 * plane + 1 - y], base + plane, name)

    def wq_hear(j):
        plane = source(j)
        arrived(wq_all.at[2 * plane + y], wq_z + plane, "wq_z")
        return over_y(wq_all, plane, wq_y)

    outer = jnp.logical_not(inner)
    wq_first = wq_send(0)
    wq_send(1, inner)
    wq_all[me] = wq_ref[half]
    send(wq_ref.at[half], wq_all.at[me], across, wq_y + z, wq_y + z)

    kv_columns = wkv_ref.shape[2]
    for side in range(2):
        kv_ref[:, side * kv_columns : (side + 1) * kv_columns] = wkv_ref[:, side, :]
    early = kv_ref.shape[0] // 4
    wkv_slot = slots(2)
    wkv_parts = (pl.ds(0, early), pl.ds(early, kv_ref.shape[0] - early))

    def wkv_send(i):
        part = wkv_parts[i]
        send(kv_ref.at[part], wkv_all.at[y, part], across, wkv_slot + i, wkv_slot + i)

    wkv_send(0)
    wkv_all[y] = kv_ref[...]
    for i in range(2):
        for j in range(2):
            wo_packed[2 * i + j] = wo_ref[i * 80 : (i + 1) * 80, j * 128 : (j + 1) * 128]
    wo_packed[4] = jnp.concatenate(
        [wo_ref[:80, 256:320], wo_ref[80:, 256:320]], axis=1
    )
    wo_all[me] = wo_packed[...]
    asked = queries_ref[...].astype(jnp.float32)
    quest_count = asked.shape[0]
    kv_heads = wkv_ref.shape[2] // HD
    asking = asked.shape[1] // (kv_heads * HD)
    for g in range(kv_heads):
        asks_ref[g] = jnp.concatenate(
            [
                asked[q : q + 1, (g * asking + j) * HD : (g * asking + j + 1) * HD]
                for q in range(quest_count)
                for j in range(asking)
            ],
            axis=0,
        ).astype(jnp.bfloat16)
    asks_all[me] = asks_ref[...]

    def normalise(slot):
        for part in range(head_count):
            rows = pl.ds(part * group_rows, group_rows)
            source = rows_all[slot, rows, :].astype(jnp.float32)
            normed[slot, rows, :] = rms_scale(source, norm_gain_ref[...].reshape(1, -1)).astype(jnp.bfloat16)

    normalise(half)

    left(wq_first)
    rows_copy = send(
        rows_all.at[half, quarter], rows_all.at[half, quarter], paired, rows_slot, rows_slot
    )
    wq_send(2, inner)
    wq_send(1, outer)
    wq_hear(0)
    over_y(wo_all, z, wo_y)
    left(rows_copy)
    wq_send(2, outer)

    scale = HD ** (-0.5)
    tails = []
    for g in range(kv_heads):
        columns = slice(g * HD, (g + 1) * HD)
        mixes, levels = [], []
        for q in range(quest_count):
            ask = asks_ref[g, q * asking : (q + 1) * asking, :]
            keys = suffix_ref[q, :, 0, columns]
            values = suffix_ref[q, :, 1, columns]
            scores = (
                lax.dot_general(
                    ask, keys, (((1,), (1,)), ((), ())), preferred_element_type=jnp.float32
                )
                * scale
            )
            place = lax.broadcasted_iota(jnp.int32, scores.shape, 1)
            scores = jnp.where(place < lengths_ref[q], scores, -1e30)
            highest = jnp.max(scores, axis=1, keepdims=True)
            weights = jnp.exp(scores - highest)
            total = jnp.sum(weights, axis=1, keepdims=True)
            mix = jnp.dot(
                weights.astype(jnp.bfloat16), values, preferred_element_type=jnp.float32
            )
            mixes.append(mix / total)
            levels.append(highest + jnp.log(total))
        tails.append((jnp.concatenate(mixes, axis=0), jnp.concatenate(levels, axis=0)))

    other = 1 - half
    wo_slots = slots(far + 2)

    def wo_send(plane, to, count):
        own = wo_all.at[2 * plane + y]
        send_if(
            (to >= 0) & (to < planes), own, own, at(to, y, x, c), wo_slots + count, wo_z + plane
        )

    theirs = rows_all.at[other, quarter]
    arrived(theirs, rows_slot, "rows")
    send(theirs, theirs, beside, rows_x_slot, rows_x_slot)
    send(theirs, theirs, twin, rows_c_slot, rows_c_slot)
    wq_hear(1)
    wo_send(z, z + 1, 0)
    wo_send(z, z - 1, 1)
    for j in range(2, far):
        wq_hear(j)

    def unpack(slice_at):
        for i in range(2):
            for j in range(2):
                wo_full[slice_at, i * 80 : (i + 1) * 80, j * 128 : (j + 1) * 128] = wo_all[
                    slice_at, 2 * i + j
                ]
        last = wo_all[slice_at, 4]
        wo_full[slice_at, :80, 256:384] = last
        wo_full[slice_at, 80:, 256:384] = pltpu.roll(last.astype(jnp.float32), 64, 1).astype(
            jnp.bfloat16
        )

    def wo_hear(j):
        plane = source(j)
        arrived(wo_all.at[2 * plane + y], wo_z + plane, "wo_z")
        wo_send(plane, jnp.where(plane < z, z + 1, z - 1), 2 + j)
        over_y(wo_all, plane, wo_y)
        unpack(2 * plane + y)

    side_quarter = pl.ds(
        pl.multiple_of((2 * c + 1 - x) * group_rows, group_rows), group_rows
    )
    beside_rows = rows_all.at[other, side_quarter]
    arrived(beside_rows, rows_x_slot, "rows_x")
    send(beside_rows, beside_rows, twin, rows_xc_slot, rows_xc_slot)
    twin_quarter = pl.ds(
        pl.multiple_of((2 * (1 - c) + x) * group_rows, group_rows), group_rows
    )
    arrived(rows_all.at[other, twin_quarter], rows_c_slot, "rows_c")
    arrived(rows_all.at[other, twin_quarter], rows_xc_slot, "rows_xc")
    arrived(order_all.at[other], order_slot, "order")
    normalise(other)
    unpack(me)
    wo_hear(0)
    for plane in range(planes):
        hear_y(wq_all, plane, wq_y, "wq_y")
        if plane == 1:
            wo_hear(1)

    lane = lax.broadcasted_iota(jnp.int32, (frame_rows, 256), 1)

    def attend(slot):
        unit_count = order_ref.shape[1]
        row = lax.broadcasted_iota(jnp.int32, (frame_rows, unit_count), 0)
        unit = row // group_rows * share + lax.rem(row, share)
        place = lax.broadcasted_iota(jnp.int32, (frame_rows, unit_count), 1)
        window = jnp.sum(
            jnp.where(order_all[slot] == unit, place // (WIN // 4), 0).astype(jnp.float32),
            axis=1,
            keepdims=True,
        )
        sort = lax.broadcasted_iota(jnp.int32, (frame_rows, 128), 1).astype(jnp.float32)
        member = jnp.where(window == sort, 1.0, 0.0).astype(jnp.bfloat16)
        same = (
            lax.dot_general(
                member, member, (((1,), (1,)), ((), ())), preferred_element_type=jnp.float32
            )
            > 0.5
        )
        qkv = jnp.dot(
            normed[slot],
            wq_all[...].reshape(depth, wq_ref.shape[2]),
            preferred_element_type=jnp.float32,
        )
        width = qkv.shape[1]
        query = qkv[:, :256].astype(jnp.bfloat16)
        key = pltpu.roll(qkv, width - own_width, 1)[:, :256].astype(jnp.bfloat16)
        value = pltpu.roll(qkv, width - 2 * own_width, 1)[:, :256].astype(jnp.bfloat16)
        mixed = jnp.zeros((frame_rows, 256), jnp.float32)
        for i in range(2):
            inside = (lane >= i * head_size) & (lane < (i + 1) * head_size)
            scores = lax.dot_general(
                jnp.where(inside, query, jnp.zeros_like(query)),
                key,
                (((1,), (1,)), ((), ())),
                preferred_element_type=jnp.float32,
            ) * head_size ** (-0.5)
            scores = jnp.where(same, scores, -1e30)
            weights = jnp.exp(scores - jnp.max(scores, axis=1, keepdims=True))
            weights = weights / jnp.sum(weights, axis=1, keepdims=True)
            product = jnp.dot(
                weights.astype(jnp.bfloat16), value, preferred_element_type=jnp.float32
            )
            mixed = jnp.where(inside, product, mixed)
        shifted = pltpu.roll(mixed, own_width - 128, 1)
        return jnp.where(half == 0, mixed, shifted).astype(jnp.bfloat16)

    swap_slot, core_slot, side_slot = (slots() for _ in range(3))
    swap_out[...] = attend(other)
    send(swap_out, swap_in, paired, swap_slot, swap_slot)
    for j in range(2, far):
        wo_hear(j)
    ask_slot, mix_slot, level_slot = (slots() for _ in range(3))

    def owner(step):
        to = lax.rem(me + step, seq_count)
        return to, {"seq": to, "head": head}

    send_all(seq_count, ask_slot, lambda step: (asks_ref, asks_all.at[me], owner(step)[1]))
    others = pl.ds(0, seq_count - 1)
    mine = attend(half)
    arrived(swap_in, swap_slot, "swap")
    theirs = swap_in[...]
    front = jnp.where(half == 0, mine, theirs)
    back = jnp.where(half == 0, theirs, mine)
    attended = jnp.concatenate(
        [front[:, :128], front[:, 128:] + back[:, :128], back[:, 128:]], axis=1
    )
    for plane in range(planes):
        hear_y(wo_all, plane, wo_y, "wo_y")
        unpack(2 * plane + 1 - y)
    wkv_send(1)
    partial = lax.dot_general(
        attended,
        wo_full[...].reshape(depth, wo_full.shape[2]),
        (((1,), (1,)), ((), ())),
        preferred_element_type=jnp.float32,
    )
    both = 2 * group_rows
    top, bottom = partial[:both], partial[both:]
    core_out[...] = jnp.where(c == 0, bottom, top).astype(jnp.bfloat16)
    send(core_out, core_in, twin, core_slot, core_slot)
    kept = jnp.where(c == 0, top, bottom)
    arrived(core_in, core_slot, "core")
    kept = kept + core_in[...].astype(jnp.float32)
    top, bottom = kept[:group_rows], kept[group_rows:]
    side_out[...] = jnp.where(x == 0, bottom, top).astype(jnp.bfloat16)
    send(side_out, side_in, beside, side_slot, side_slot)
    kept = jnp.where(x == 0, top, bottom) + rows_all[half, quarter, :].astype(jnp.float32)
    arrived(side_in, side_slot, "side")
    hidden = kept + side_in[...].astype(jnp.float32)
    merged = rms_scale(hidden, merge_gain_ref[...].reshape(1, -1)).astype(jnp.bfloat16)
    merged_out[...] = merged.reshape(planes, share, depth)

    mz, mx, mc, mxc, key_slots, value_slots = (slots(planes) for _ in range(6))
    for k in range(far):
        to = target(k)
        send(merged_out.at[to], merged_all.at[z, group], at(to, y, x, c), mz + k, mz + z)
    merged_all[z, group] = merged_out[z]
    side_group, twin_group = 2 * c + 1 - x, 2 * (1 - c) + x
    cross_group = 2 * (1 - c) + 1 - x

    def spread(plane, block):
        here = merged_all.at[plane, group]
        send(block, here, beside, mx + plane, mx + plane)
        send(block, here, twin, mc + plane, mc + plane)

    def relay(plane):
        block = merged_all.at[plane, side_group]
        arrived(block, mx + plane, "mx")
        send(block, block, twin, mxc + plane, mxc + plane)

    frame_tokens = frame_rows // 4

    def project(plane):
        arrived(merged_all.at[plane, twin_group], mc + plane, "mc")
        arrived(merged_all.at[plane, cross_group], mxc + plane, "mxc")
        block = merged_all[plane].reshape(frame_tokens, depth)
        weights = wkv_all[...].reshape(depth, kv_ref.shape[1])
        return jnp.dot(block, weights, preferred_element_type=jnp.float32)

    def project_to(plane):
        product = project(plane)
        key_out[plane] = product[:, :kv_columns]
        value_out[plane] = product[:, kv_columns:].astype(jnp.bfloat16)
        to = at(plane, y, x, c)
        send(key_out.at[plane], key_in.at[z], to, key_slots + plane, key_slots + z)
        send(value_out.at[plane], value_in.at[z], to, value_slots + plane, value_slots + z)

    planes_heard = [source(j) for j in range(far)]
    spread(z, merged_out.at[z])
    for j in range(far):
        plane = planes_heard[j]
        arrived(merged_all.at[plane, group], mz + plane, "mz")
        spread(plane, merged_all.at[plane, group])
        relay(planes_heard[j - 1] if j else z)
    for i in range(2):
        arrived(wkv_all.at[1 - y, wkv_parts[i]], wkv_slot + i, "wkv")
    for plane in planes_heard[:-2]:
        project_to(plane)
    relay(planes_heard[-1])
    for plane in planes_heard[-2:]:
        project_to(plane)
    visual = project(z)
    keys, values = visual[:, :kv_columns], visual[:, kv_columns:]
    for plane in planes_heard:
        arrived(key_in.at[plane], key_slots + plane, "key")
        arrived(value_in.at[plane], value_slots + plane, "value")
        keys = keys + key_in[plane]
        values = values + value_in[plane].astype(jnp.float32)
    all_keys, all_values = keys.astype(jnp.bfloat16), values.astype(jnp.bfloat16)

    arrived(asks_all.at[others], ask_slot, "ask")
    all_rows = seq_count * asks_ref.shape[1]
    own_rows = asks_ref.shape[1]
    questions = range_ref.shape[1]
    seen = jnp.concatenate(
        [
            jnp.full(
                (asking, 1),
                jnp.where((range_ref[0, q] <= me) & (me < range_ref[1, q]), 0.0, -1e30),
                jnp.float32,
            )
            for q in range(questions)
        ],
        axis=0,
    )
    level_out[...] = jnp.zeros_like(level_out)
    diagonal = lax.broadcasted_iota(
        jnp.int32, (all_rows, all_rows), 0
    ) == lax.broadcasted_iota(jnp.int32, (all_rows, all_rows), 1)
    for g in range(kv_heads):
        ask = asks_all[:, g].reshape(all_rows, HD)
        keys = all_keys[:, g * HD : (g + 1) * HD]
        values = all_values[:, g * HD : (g + 1) * HD]
        scores = (
            lax.dot_general(
                ask, keys, (((1,), (1,)), ((), ())), preferred_element_type=jnp.float32
            )
            * scale
        )
        highest = jnp.max(scores, axis=1, keepdims=True)
        weights = jnp.exp(scores - highest)
        total = jnp.sum(weights, axis=1, keepdims=True)
        mix = (
            jnp.dot(weights.astype(jnp.bfloat16), values, preferred_element_type=jnp.float32)
            / total
        )
        level = highest + jnp.log(total) + seen
        mixed_out[:, g] = mix.astype(jnp.bfloat16).reshape(seq_count, own_rows, HD)
        level_out[g : g + 1, :] = jnp.sum(
            jnp.where(diagonal, level, 0.0), axis=0, keepdims=True
        )
    mixed_in[me] = mixed_out[me]
    level_in[me] = level_out[...]
    send_all(
        seq_count,
        mix_slot,
        lambda step: (mixed_out.at[owner(step)[0]], mixed_in.at[me], owner(step)[1]),
    )
    send_all(seq_count, level_slot, lambda step: (level_out, level_in.at[me], owner(step)[1]))
    arrived(mixed_in.at[others], mix_slot, "mix")
    arrived(level_in.at[others], level_slot, "level")
    row = lax.broadcasted_iota(jnp.int32, (own_rows, all_rows), 0)
    place = lax.broadcasted_iota(jnp.int32, (own_rows, all_rows), 1)
    chosen = place == row + me * own_rows
    answers = []
    for g in range(kv_heads):
        mix, level = tails[g]
        levels = [
            jnp.sum(jnp.where(chosen, level_in[s, g : g + 1, :], 0.0), axis=1, keepdims=True)
            for s in range(seq_count)
        ]
        highest = level
        for other_level in levels:
            highest = jnp.maximum(highest, other_level)
        share_of = jnp.exp(level - highest)
        total = share_of
        answer = share_of * mix
        for s in range(seq_count):
            share_of = jnp.exp(levels[s] - highest)
            total = total + share_of
            answer = answer + share_of * mixed_in[s, g].astype(jnp.float32)
        answers.append(answer / total)
    out_ref[...] = jnp.concatenate(
        [
            jnp.concatenate(
                [
                    answers[g][q * asking + j : q * asking + j + 1]
                    for g in range(kv_heads)
                    for j in range(asking)
                ],
                axis=1,
            )
            for q in range(quest_count)
        ],
        axis=0,
    ).astype(jnp.bfloat16)
    for copy in started:
        copy.wait_send()
    for block, slot in (
        (asks_all.at[others], ask_slot),
        (mixed_in.at[others], mix_slot),
        (level_in.at[others], level_slot),
    ):
        copy_of(block, block, twin, slot, slot).wait_send()
    for inside, copy in guarded:

        @pl.when(inside)
        def _(copy=copy):
            copy.wait_send()


def fused(
    patches,
    norm_gain,
    w_qkv,
    w_out,
    window_order,
    merge_gain,
    w_kv,
    queries,
    suffix_kv,
    question_lengths,
    frame_range,
):
    seq_count, head_count = lax.axis_size("seq"), lax.axis_size("head")
    planes = seq_count // 2
    frame_rows, depth = patches.shape
    rows, _, columns = w_qkv.shape
    half = columns // 2
    kv_columns = w_kv.shape[2]
    kv_heads = kv_columns // HD
    bf16 = jnp.bfloat16
    wq_width = -(-3 * half // 128) * 128
    asks_shape = (kv_heads, queries.size // (kv_heads * HD), HD)
    own_rows = asks_shape[1]
    group_rows = frame_rows // head_count
    share = group_rows // 4
    messages = 14 + 11 * (seq_count // 2)
    smem = pl.BlockSpec(memory_space=pltpu.SMEM)
    answers = pl.pallas_call(
        functools.partial(fused_kernel, seq_count, head_count),
        out_shape=jax.ShapeDtypeStruct(queries.shape, bf16),
        in_specs=[VMEM] * 9 + [smem] * 2,
        out_specs=VMEM,
        scratch_shapes=[
            pltpu.VMEM((3, rows, wq_width), jnp.float32),
            pltpu.VMEM((2, rows, wq_width), bf16),
            pltpu.VMEM((w_kv.shape[0], 2 * kv_columns), bf16),
            pltpu.VMEM(asks_shape, bf16),
            pltpu.VMEM((2, frame_rows, depth), bf16),
            pltpu.VMEM((2,) + window_order.shape, jnp.int32),
            pltpu.VMEM((2, frame_rows, depth), bf16),
            pltpu.VMEM((seq_count, rows, wq_width), bf16),
            pltpu.VMEM((5, 80, 128), bf16),
            pltpu.VMEM((seq_count, 5, 80, 128), bf16),
            pltpu.VMEM((seq_count, rows, 384), bf16),
            pltpu.VMEM((2, w_kv.shape[0], 2 * kv_columns), bf16),
            pltpu.VMEM((seq_count,) + asks_shape, bf16),
            pltpu.VMEM((frame_rows, 256), bf16),
            pltpu.VMEM((frame_rows, 256), bf16),
            pltpu.VMEM((2 * group_rows, depth), bf16),
            pltpu.VMEM((2 * group_rows, depth), bf16),
            pltpu.VMEM((group_rows, depth), bf16),
            pltpu.VMEM((group_rows, depth), bf16),
            pltpu.VMEM((planes, share, depth), bf16),
            pltpu.VMEM((planes, head_count, share, depth), bf16),
            pltpu.VMEM((planes, frame_rows // 4, kv_columns), jnp.float32),
            pltpu.VMEM((planes, frame_rows // 4, kv_columns), jnp.float32),
            pltpu.VMEM((planes, frame_rows // 4, kv_columns), bf16),
            pltpu.VMEM((planes, frame_rows // 4, kv_columns), bf16),
            pltpu.VMEM((seq_count,) + asks_shape, bf16),
            pltpu.VMEM((seq_count,) + asks_shape, bf16),
            pltpu.VMEM((8, seq_count * own_rows), jnp.float32),
            pltpu.VMEM((seq_count, 8, seq_count * own_rows), jnp.float32),
            pltpu.SemaphoreType.DMA((messages,)),
            pltpu.SemaphoreType.DMA((messages,)),
        ],
        compiler_params=pltpu.CompilerParams(
            collective_id=0, has_side_effects=True, vmem_limit_bytes=60 << 20
        ),
        name="fused",
    )(
        patches,
        norm_gain,
        merge_gain,
        w_qkv.transpose(1, 0, 2),
        w_out.T,
        window_order,
        w_kv,
        queries,
        suffix_kv,
        question_lengths,
        frame_range.T,
    )
    return answers


def device_program(*arguments):
    patches, _, w_qkv, _, window_order = arguments[:5]
    paired = lax.axis_size("seq") == 8 and lax.axis_size("head") == 4
    whole = patches.shape[0] == FPATCH and window_order.shape[0] == 1
    if paired and whole and w_qkv.shape[0] % 16 == 0:
        return fused(*arguments)
    return on_device(*arguments)


def solution(mesh):
    placed = (
        P("seq", None),
        P(),
        P("seq", None, "head"),
        P("head", "seq"),
        P("seq", None),
        P(),
        P("seq", None, "head"),
        P("seq", "head"),
        P("seq", None, None, "head"),
        P("seq"),
        P(),
    )
    return jax.shard_map(
        device_program, mesh=mesh, in_specs=placed, out_specs=P("seq", "head"), check_vma=False
    )
```

```python
import functools

import jax
import jax.numpy as jnp
from jax import lax
from jax.experimental import pallas as pl
from jax.experimental.pallas import tpu as pltpu
from jax.sharding import PartitionSpec as P

VD = 1280
VH = 16
HD = 128
FPATCH = 256
WIN = 64

MESH = pl.DeviceIdType.MESH
VMEM = pl.BlockSpec(memory_space=pltpu.VMEM)


def rms_scale(values, gain):
    return values * lax.rsqrt(jnp.mean(values * values, axis=-1, keepdims=True) + 1e-06) * gain


def exchange_kernel(axis, count, gather, x_ref, out_ref, send_sem, recv_sem, own_sem):
    me = lax.axis_index(axis)
    barrier = pltpu.get_barrier_semaphore()
    for step in range(1, count):
        pl.semaphore_signal(
            barrier, inc=1, device_id={axis: lax.rem(me + step, count)}, device_id_type=MESH
        )
    pl.semaphore_wait(barrier, count - 1)
    copies = []
    for step in range(1, count):
        peer = lax.rem(me + step, count)
        copy = pltpu.make_async_remote_copy(
            src_ref=x_ref if gather else x_ref.at[peer],
            dst_ref=out_ref.at[me],
            send_sem=send_sem.at[step],
            recv_sem=recv_sem.at[step],
            device_id={axis: peer},
            device_id_type=MESH,
        )
        copy.start()
        copies.append(copy)
    own = pltpu.make_async_copy(x_ref if gather else x_ref.at[me], out_ref.at[me], own_sem)
    own.start()
    own.wait()
    for copy in copies:
        copy.wait()


def exchange(x, axis, gather, collective_id):
    count = lax.axis_size(axis)
    shape = ((count,) + x.shape) if gather else x.shape
    return pl.pallas_call(
        functools.partial(exchange_kernel, axis, count, gather),
        out_shape=jax.ShapeDtypeStruct(shape, x.dtype),
        in_specs=[VMEM],
        out_specs=VMEM,
        scratch_shapes=[
            pltpu.SemaphoreType.DMA((count,)),
            pltpu.SemaphoreType.DMA((count,)),
            pltpu.SemaphoreType.DMA,
        ],
        compiler_params=pltpu.CompilerParams(collective_id=collective_id, has_side_effects=True),
        name=f"exchange_{collective_id}",
    )(x)


def ring_kernel(count, qkv_ref, wout_ref, qkv_out, wout_out, send_sem, recv_sem, own_sem):
    me = lax.axis_index("seq")
    odd = lax.rem(me, 2)
    place = (1 - odd) * (me // 2) + odd * (count - 1 - me // 2)

    def index_of(position):
        position = lax.rem(position + count, count)
        late = position // (count // 2)
        return (1 - late) * 2 * position + late * (2 * (count - 1 - position) + 1)

    neighbours = (index_of(place + 1), index_of(place - 1))
    barrier = pltpu.get_barrier_semaphore()
    for neighbour in neighbours:
        pl.semaphore_signal(barrier, inc=1, device_id={"seq": neighbour}, device_id_type=MESH)
    pl.semaphore_wait(barrier, 2)
    far, near = count // 2, count - 1 - count // 2
    pieces = 4

    def slot(piece, source):
        return qkv_out.at[piece, source] if piece < 3 else wout_out.at[source]

    def own(piece):
        return qkv_ref.at[piece] if piece < 3 else wout_ref

    copies = {}
    for step in range(far):
        for piece in range(pieces):
            for way in range(2):
                hops = far if (piece < 2) == (way == 0) else near
                if step >= hops:
                    continue
                source = index_of(place - step if way == 0 else place + step)
                if step > 0:
                    copies[step - 1, piece, way].wait_recv()
                copy = pltpu.make_async_remote_copy(
                    src_ref=own(piece) if step == 0 else slot(piece, source),
                    dst_ref=slot(piece, source),
                    send_sem=send_sem.at[step, piece, way],
                    recv_sem=recv_sem.at[step, piece, way],
                    device_id={"seq": neighbours[way]},
                    device_id_type=MESH,
                )
                copy.start()
                copies[step, piece, way] = copy
    kept = [pltpu.make_async_copy(own(p), slot(p, me), own_sem.at[p]) for p in range(pieces)]
    for copy in kept:
        copy.start()
    for copy in kept:
        copy.wait()
    for (step, piece, way), copy in copies.items():
        if (step + 1, piece, way) not in copies:
            copy.wait_recv()
    for copy in copies.values():
        copy.wait_send()


def ring_weights(w_qkv, w_out):
    count = lax.axis_size("seq")
    far = count // 2
    return pl.pallas_call(
        functools.partial(ring_kernel, count),
        out_shape=(
            jax.ShapeDtypeStruct((3, count) + w_qkv.shape[1:], w_qkv.dtype),
            jax.ShapeDtypeStruct((count,) + w_out.shape, w_out.dtype),
        ),
        in_specs=[VMEM, VMEM],
        out_specs=(VMEM, VMEM),
        scratch_shapes=[
            pltpu.SemaphoreType.DMA((far, 4, 2)),
            pltpu.SemaphoreType.DMA((far, 4, 2)),
            pltpu.SemaphoreType.DMA((4,)),
        ],
        compiler_params=pltpu.CompilerParams(collective_id=0, has_side_effects=True),
        name="ring_weights",
    )(w_qkv, w_out)


def frame_attention(query, key, value, unit_order, head_size):
    unit_count = unit_order.shape[0]
    patch_count = unit_count * 4
    ranks = jnp.sum(
        jnp.where(
            unit_order[None, :] == (jnp.arange(patch_count) // 4)[:, None],
            jnp.arange(unit_count)[None, :] // (WIN // 4),
            0,
        ),
        axis=1,
    )
    same = ranks[:, None] == ranks[None, :]
    scores = jnp.einsum(
        "qhd,khd->hqk", query, key, preferred_element_type=jnp.float32
    ) * head_size ** (-0.5)
    scores = jnp.where(same[None], scores, -jnp.inf)
    weights = jax.nn.softmax(scores, axis=-1).astype(jnp.bfloat16)
    return jnp.einsum(
        "hqk,khd->qhd", weights, value, preferred_element_type=jnp.float32
    ).astype(jnp.bfloat16)


def on_device(
    patches,
    norm_gain,
    w_qkv,
    w_out,
    window_order,
    merge_gain,
    w_kv,
    queries,
    suffix_kv,
    question_lengths,
    frame_range,
):
    head_count = lax.axis_size("head")
    seq_count = lax.axis_size("seq")
    row_count = patches.shape[0]
    frame_count = window_order.shape[0]
    columns = w_qkv.shape[2]
    head_size = VD // VH
    local_heads = columns // head_size
    source = patches.astype(jnp.float32)
    normed = rms_scale(source, norm_gain).astype(jnp.bfloat16)
    qkv_all, w_out_all = ring_weights(w_qkv.transpose(1, 0, 2), w_out)
    qkv_all = qkv_all.reshape(3, -1, columns)
    query, key, value = [
        jnp.dot(normed, qkv_all[part], preferred_element_type=jnp.float32)
        .astype(jnp.bfloat16)
        .reshape(frame_count, -1, local_heads, head_size)
        for part in range(3)
    ]
    attended = jax.vmap(
        lambda q, k, v, order: frame_attention(q, k, v, order, head_size)
    )(query, key, value, window_order).reshape(row_count, columns)
    w_full = w_out_all.transpose(1, 0, 2).reshape(columns, VD)
    share_rows = row_count // head_count
    partial = jnp.dot(attended, w_full, preferred_element_type=jnp.float32).astype(jnp.bfloat16)
    parts = exchange(partial.reshape(head_count, share_rows, VD), "head", False, 1)
    shared = jnp.sum(parts.astype(jnp.float32), axis=0)
    own_rows = lax.dynamic_slice_in_dim(source, lax.axis_index("head") * share_rows, share_rows, 0)
    merged = rms_scale(own_rows + shared, merge_gain).astype(jnp.bfloat16)
    share_tokens = share_rows // 4
    depth = w_kv.shape[0]
    merged = merged.reshape(share_tokens, seq_count, depth).transpose(1, 0, 2)
    merged = exchange(merged, "seq", False, 2)
    merged = exchange(merged, "head", True, 3)
    merged = merged.transpose(1, 0, 2, 3).reshape(-1, depth)
    kv_columns = w_kv.shape[2]
    partial = jnp.dot(
        merged, w_kv.reshape(depth, 2 * kv_columns), preferred_element_type=jnp.float32
    ).astype(jnp.bfloat16)
    parts = exchange(partial.reshape(seq_count, -1, 2 * kv_columns), "seq", False, 4)
    visual = jnp.sum(parts.astype(jnp.float32), axis=0).astype(jnp.bfloat16)
    visual = exchange(visual, "seq", True, 5).reshape(-1, 2 * kv_columns)

    token_count = visual.shape[0]
    quest_count = queries.shape[0]
    span = suffix_kv.shape[1]
    kv_local = kv_columns // HD
    asking = queries.reshape(quest_count, kv_local, -1, HD)
    frame_tokens = FPATCH // 4
    seq_index = lax.axis_index("seq")
    bounds = lax.dynamic_slice_in_dim(frame_range, seq_index * quest_count, quest_count, 0)
    frame_index = jnp.arange(token_count) // frame_tokens
    live = (frame_index[None, :] >= bounds[:, 0:1]) & (frame_index[None, :] < bounds[:, 1:2])
    suffix_live = jnp.arange(span)[None, :] < question_lengths[:, None]
    suffix = suffix_kv.reshape(quest_count, span, 2, kv_local, HD)
    answers = []
    for g in range(kv_local):
        ask = asking[:, g]
        keys = visual[:, g * HD : (g + 1) * HD]
        values = visual[:, kv_columns + g * HD : kv_columns + (g + 1) * HD]
        scores = jnp.einsum(
            "qjd,nd->qjn", ask, keys, preferred_element_type=jnp.float32
        ) * HD ** (-0.5)
        scores = jnp.where(live[:, None, :], scores, -jnp.inf)
        tail = jnp.einsum(
            "qjd,qsd->qjs", ask, suffix[:, :, 0, g], preferred_element_type=jnp.float32
        ) * HD ** (-0.5)
        tail = jnp.where(suffix_live[:, None, :], tail, -jnp.inf)
        highest = jnp.maximum(
            jnp.max(scores, axis=-1, keepdims=True), jnp.max(tail, axis=-1, keepdims=True)
        )
        weights = jnp.exp(scores - highest)
        tail_weights = jnp.exp(tail - highest)
        totals = jnp.sum(weights, axis=-1, keepdims=True) + jnp.sum(
            tail_weights, axis=-1, keepdims=True
        )
        mixed = jnp.einsum(
            "qjn,nd->qjd", weights.astype(jnp.bfloat16), values, preferred_element_type=jnp.float32
        ) + jnp.einsum(
            "qjs,qsd->qjd",
            tail_weights.astype(jnp.bfloat16),
            suffix[:, :, 1, g],
            preferred_element_type=jnp.float32,
        )
        answers.append((mixed / totals).astype(jnp.bfloat16))
    return jnp.stack(answers, axis=1).reshape(quest_count, -1)


def fused_kernel(
    seq_count,
    head_count,
    patches_in,
    norm_gain_in,
    merge_gain_in,
    wqkv_in,
    wo_in,
    order_in,
    wkv_in,
    queries_in,
    suffix_in,
    lengths_in,
    range_in,
    out_ref,
    patches_ref,
    norm_gain_ref,
    merge_gain_ref,
    wqkv_ref,
    wo_ref,
    order_ref,
    wkv_ref,
    queries_ref,
    suffix_ref,
    lengths_ref,
    range_ref,
    wide,
    wq_ref,
    kv_ref,
    asks_ref,
    rows_all,
    order_all,
    normed,
    wq_all,
    wo_packed,
    wo_all,
    wo_full,
    wkv_all,
    asks_all,
    swap_out,
    swap_in,
    core_out,
    core_in,
    side_out,
    side_in,
    merged_out,
    merged_all,
    key_out,
    key_in,
    value_out,
    value_in,
    mixed_out,
    mixed_in,
    level_out,
    level_in,
    load_sems,
    send_sems,
    recv_sems,
):
    planes = seq_count // 2
    me = lax.axis_index("seq")
    head = lax.axis_index("head")
    z, y = me // 2, lax.rem(me, 2)
    x, c = head // 2, lax.rem(head, 2)
    half = lax.rem(z, 2)
    group = 2 * c + x
    frame_rows, depth = patches_ref.shape
    group_rows = frame_rows // head_count
    share = group_rows // 4
    head_size = VD // VH
    own_width = 2 * head_size

    def at(z_to, y_to, x_to, c_to):
        return {"seq": 2 * z_to + y_to, "head": 2 * x_to + c_to}

    partner = z + 1 - 2 * half
    across = at(z, 1 - y, x, c)
    beside = at(z, y, 1 - x, c)
    twin = at(z, y, x, 1 - c)
    paired = at(partner, y, x, c)

    low = z < planes // 2
    inner = (z > 0) & (z < planes - 1)

    def ordered(outer_plane, inner_plane):
        plane = jnp.where(inner, inner_plane, outer_plane)
        return jnp.where(low, plane, planes - 1 - plane)

    def target(k):
        return ordered((3, 2, 1)[k], (2, 0, 3)[k])

    def source(j):
        return ordered((1, 3, 2)[j], (2, 3, 0)[j])

    barrier = pltpu.get_barrier_semaphore()
    peers = [
        {"seq": lax.rem(me + step, seq_count), "head": head} for step in range(1, seq_count)
    ] + [beside, twin]
    for peer in peers:
        pl.semaphore_signal(barrier, inc=1, device_id=peer, device_id_type=MESH)

    pairs = (
        (wqkv_in, wqkv_ref),
        (patches_in, patches_ref),
        (order_in, order_ref),
        (norm_gain_in, norm_gain_ref),
        (wo_in, wo_ref),
        (wkv_in, wkv_ref),
        (queries_in, queries_ref),
        (suffix_in, suffix_ref),
        (lengths_in, lengths_ref),
        (merge_gain_in, merge_gain_ref),
        (range_in, range_ref),
    )
    loads = [
        pltpu.make_async_copy(src, dst, load_sems.at[i]) for i, (src, dst) in enumerate(pairs)
    ]
    for load in loads:
        load.start()
    taken = []
    started = []
    guarded = []

    def slots(count=1):
        taken.append(count)
        return sum(taken) - count

    def copy_of(src, dst, device, send_slot, recv_slot):
        return pltpu.make_async_remote_copy(
            src_ref=src,
            dst_ref=dst,
            send_sem=send_sems.at[send_slot],
            recv_sem=recv_sems.at[recv_slot],
            device_id=device,
            device_id_type=MESH,
        )

    def send(src, dst, device, send_slot, recv_slot):
        copy = copy_of(src, dst, device, send_slot, recv_slot)
        copy.start()
        started.append(copy)
        return copy

    def send_if(inside, src, dst, device, send_slot, recv_slot):
        copy = copy_of(src, dst, device, send_slot, recv_slot)

        @pl.when(inside)
        def _():
            copy.start()

        guarded.append((inside, copy))

    def send_all(count, slot, copy_at):
        for step in range(1, count):
            src, dst, device = copy_at(step)
            copy_of(src, dst, device, slot, slot).start()

    def left(copy):
        started[:] = [kept for kept in started if kept is not copy]
        copy.wait_send()

    def arrived(ref, slot, name):
        copy_of(ref, ref, twin, slot, slot).wait_recv()

    for load in loads[:3]:
        load.wait()

    for part in range(head_count):
        row = lax.broadcasted_iota(jnp.int32, (group_rows, frame_rows), 0)
        place = lax.broadcasted_iota(jnp.int32, (group_rows, frame_rows), 1)
        picked = 4 * (share * part + lax.rem(row, share)) + row // share
        pick = jnp.where(place == picked, 1.0, 0.0).astype(jnp.bfloat16)
        rows_all[half, pl.ds(part * group_rows, group_rows), :] = jnp.dot(
            pick, patches_ref[...], preferred_element_type=jnp.float32
        ).astype(jnp.bfloat16)
    columns = wqkv_ref.shape[2]
    wq_width = wq_ref.shape[2]
    lane = lax.broadcasted_iota(jnp.int32, wq_ref.shape[1:], 1)
    packed = [jnp.zeros(wq_ref.shape[1:], jnp.float32)] * 2
    wide[...] = jnp.zeros_like(wide)
    for part in range(3):
        wide[part, :, :columns] = wqkv_ref[part].astype(jnp.float32)
        for side in range(2):
            shift = (part - side) * own_width
            moved = wide[part] if shift == 0 else pltpu.roll(wide[part], shift % wq_width, 1)
            inside = (lane >= part * own_width) & (lane < (part + 1) * own_width)
            packed[side] = jnp.where(inside, moved, packed[side])
    for side in range(2):
        wq_ref[side] = packed[side].astype(jnp.bfloat16)
    order_all[half] = order_ref[...]
    pl.semaphore_wait(barrier, len(peers))

    quarter = pl.ds(pl.multiple_of(group * group_rows, group_rows), group_rows)
    far = planes - 1
    order_slot, rows_slot, rows_x_slot, rows_c_slot, rows_xc_slot = (slots() for _ in range(5))
    wq_z, wq_y, wo_z, wo_y = (slots(planes) for _ in range(4))
    send(order_all.at[half], order_all.at[half], paired, order_slot, order_slot)

    def wq_send(k, inside=None):
        to = target(k)
        copy = (
            wq_ref.at[lax.rem(to, 2)],
            wq_all.at[me],
            at(to, y, x, c),
            wq_z + k,
            wq_z + z,
        )
        return send(*copy) if inside is None else send_if(inside, *copy)

    def over_y(ref, plane, base):
        own = ref.at[2 * plane + y]
        return send(own, own, across, base + plane, base + plane)

    def hear_y(ref, plane, base, name):
        arrived(ref.at[2 * plane + 1 - y], base + plane, name)

    def wq_hear(j):
        plane = source(j)
        arrived(wq_all.at[2 * plane + y], wq_z + plane, "wq_z")
        return over_y(wq_all, plane, wq_y)

    outer = jnp.logical_not(inner)
    wq_first = wq_send(0)
    wq_send(1, inner)
    wq_all[me] = wq_ref[half]
    send(wq_ref.at[half], wq_all.at[me], across, wq_y + z, wq_y + z)

    for load in loads[3:]:
        load.wait()
    kv_columns = wkv_ref.shape[2]
    for side in range(2):
        kv_ref[:, side * kv_columns : (side + 1) * kv_columns] = wkv_ref[:, side, :]
    early = kv_ref.shape[0] // 4
    wkv_slot = slots(2)
    wkv_parts = (pl.ds(0, early), pl.ds(early, kv_ref.shape[0] - early))

    def wkv_send(i):
        part = wkv_parts[i]
        send(kv_ref.at[part], wkv_all.at[y, part], across, wkv_slot + i, wkv_slot + i)

    wkv_send(0)
    wkv_all[y] = kv_ref[...]
    for i in range(2):
        for j in range(2):
            wo_packed[2 * i + j] = wo_ref[i * 80 : (i + 1) * 80, j * 128 : (j + 1) * 128]
    wo_packed[4] = jnp.concatenate(
        [wo_ref[:80, 256:320], wo_ref[80:, 256:320]], axis=1
    )
    wo_all[me] = wo_packed[...]
    asked = queries_ref[...].astype(jnp.float32)
    quest_count = asked.shape[0]
    kv_heads = wkv_ref.shape[2] // HD
    asking = asked.shape[1] // (kv_heads * HD)
    for g in range(kv_heads):
        asks_ref[g] = jnp.concatenate(
            [
                asked[q : q + 1, (g * asking + j) * HD : (g * asking + j + 1) * HD]
                for q in range(quest_count)
                for j in range(asking)
            ],
            axis=0,
        ).astype(jnp.bfloat16)
    asks_all[me] = asks_ref[...]

    def normalise(slot):
        for part in range(head_count):
            rows = pl.ds(part * group_rows, group_rows)
            source = rows_all[slot, rows, :].astype(jnp.float32)
            normed[slot, rows, :] = rms_scale(source, norm_gain_ref[...].reshape(1, -1)).astype(jnp.bfloat16)

    normalise(half)

    left(wq_first)
    rows_copy = send(
        rows_all.at[half, quarter], rows_all.at[half, quarter], paired, rows_slot, rows_slot
    )
    wq_send(2, inner)
    wq_send(1, outer)
    wq_hear(0)
    over_y(wo_all, z, wo_y)
    left(rows_copy)
    wq_send(2, outer)

    scale = HD ** (-0.5)
    tails = []
    for g in range(kv_heads):
        columns = slice(g * HD, (g + 1) * HD)
        mixes, levels = [], []
        for q in range(quest_count):
            ask = asks_ref[g, q * asking : (q + 1) * asking, :]
            keys = suffix_ref[q, :, 0, columns]
            values = suffix_ref[q, :, 1, columns]
            scores = (
                lax.dot_general(
                    ask, keys, (((1,), (1,)), ((), ())), preferred_element_type=jnp.float32
                )
                * scale
            )
            place = lax.broadcasted_iota(jnp.int32, scores.shape, 1)
            scores = jnp.where(place < lengths_ref[q], scores, -1e30)
            highest = jnp.max(scores, axis=1, keepdims=True)
            weights = jnp.exp(scores - highest)
            total = jnp.sum(weights, axis=1, keepdims=True)
            mix = jnp.dot(
                weights.astype(jnp.bfloat16), values, preferred_element_type=jnp.float32
            )
            mixes.append(mix / total)
            levels.append(highest + jnp.log(total))
        tails.append((jnp.concatenate(mixes, axis=0), jnp.concatenate(levels, axis=0)))

    other = 1 - half
    def wo_send(k):
        send(wo_packed, wo_all.at[me], at(target(k), y, x, c), wo_z + k, wo_z + z)

    theirs = rows_all.at[other, quarter]
    arrived(theirs, rows_slot, "rows")
    send(theirs, theirs, beside, rows_x_slot, rows_x_slot)
    send(theirs, theirs, twin, rows_c_slot, rows_c_slot)
    wq_hear(1)
    for k in range(far - 1):
        wo_send(k)
    for j in range(2, far):
        wq_hear(j)
    wo_send(far - 1)

    def unpack(slice_at):
        for i in range(2):
            for j in range(2):
                wo_full[slice_at, i * 80 : (i + 1) * 80, j * 128 : (j + 1) * 128] = wo_all[
                    slice_at, 2 * i + j
                ]
        last = wo_all[slice_at, 4]
        wo_full[slice_at, :80, 256:384] = last
        wo_full[slice_at, 80:, 256:384] = pltpu.roll(last.astype(jnp.float32), 64, 1).astype(
            jnp.bfloat16
        )

    wo_relays = {}

    def wo_hear(j, inside=None):
        plane = source(j)
        own = wo_all.at[2 * plane + y]
        if j not in wo_relays:
            wo_relays[j] = copy_of(own, own, across, wo_y + plane, wo_y + plane)
            started.append(wo_relays[j])
        copy = wo_relays[j]

        def take():
            arrived(own, wo_z + plane, "wo_z")
            copy.start()
            unpack(2 * plane + y)

        if inside is None:
            take()
        else:
            pl.when(inside)(take)

    side_quarter = pl.ds(
        pl.multiple_of((2 * c + 1 - x) * group_rows, group_rows), group_rows
    )
    beside_rows = rows_all.at[other, side_quarter]
    arrived(beside_rows, rows_x_slot, "rows_x")
    send(beside_rows, beside_rows, twin, rows_xc_slot, rows_xc_slot)
    twin_quarter = pl.ds(
        pl.multiple_of((2 * (1 - c) + x) * group_rows, group_rows), group_rows
    )
    arrived(rows_all.at[other, twin_quarter], rows_c_slot, "rows_c")
    arrived(rows_all.at[other, twin_quarter], rows_xc_slot, "rows_xc")
    arrived(order_all.at[other], order_slot, "order")
    normalise(other)
    unpack(me)
    wo_hear(0, outer)
    for plane in range(planes):
        hear_y(wq_all, plane, wq_y, "wq_y")
        if plane == 1:
            wo_hear(1, outer)

    lane = lax.broadcasted_iota(jnp.int32, (frame_rows, 256), 1)

    def attend(slot):
        unit_count = order_ref.shape[1]
        row = lax.broadcasted_iota(jnp.int32, (frame_rows, unit_count), 0)
        unit = row // group_rows * share + lax.rem(row, share)
        place = lax.broadcasted_iota(jnp.int32, (frame_rows, unit_count), 1)
        window = jnp.sum(
            jnp.where(order_all[slot] == unit, place // (WIN // 4), 0).astype(jnp.float32),
            axis=1,
            keepdims=True,
        )
        sort = lax.broadcasted_iota(jnp.int32, (frame_rows, 128), 1).astype(jnp.float32)
        member = jnp.where(window == sort, 1.0, 0.0).astype(jnp.bfloat16)
        same = (
            lax.dot_general(
                member, member, (((1,), (1,)), ((), ())), preferred_element_type=jnp.float32
            )
            > 0.5
        )
        qkv = jnp.dot(
            normed[slot],
            wq_all[...].reshape(depth, wq_ref.shape[2]),
            preferred_element_type=jnp.float32,
        )
        width = qkv.shape[1]
        query = qkv[:, :256].astype(jnp.bfloat16)
        key = pltpu.roll(qkv, width - own_width, 1)[:, :256].astype(jnp.bfloat16)
        value = pltpu.roll(qkv, width - 2 * own_width, 1)[:, :256].astype(jnp.bfloat16)
        mixed = jnp.zeros((frame_rows, 256), jnp.float32)
        for i in range(2):
            inside = (lane >= i * head_size) & (lane < (i + 1) * head_size)
            scores = lax.dot_general(
                jnp.where(inside, query, jnp.zeros_like(query)),
                key,
                (((1,), (1,)), ((), ())),
                preferred_element_type=jnp.float32,
            ) * head_size ** (-0.5)
            scores = jnp.where(same, scores, -1e30)
            weights = jnp.exp(scores - jnp.max(scores, axis=1, keepdims=True))
            weights = weights / jnp.sum(weights, axis=1, keepdims=True)
            product = jnp.dot(
                weights.astype(jnp.bfloat16), value, preferred_element_type=jnp.float32
            )
            mixed = jnp.where(inside, product, mixed)
        shifted = pltpu.roll(mixed, own_width - 128, 1)
        return jnp.where(half == 0, mixed, shifted).astype(jnp.bfloat16)

    swap_slot, core_slot, side_slot = (slots() for _ in range(3))
    swap_out[...] = attend(other)
    send(swap_out, swap_in, paired, swap_slot, swap_slot)
    for j in range(2):
        wo_hear(j, inner)
    for j in range(2, far):
        wo_hear(j)
    ask_slot, mix_slot, level_slot = (slots() for _ in range(3))

    def owner(step):
        to = lax.rem(me + step, seq_count)
        return to, {"seq": to, "head": head}

    send_all(seq_count, ask_slot, lambda step: (asks_ref, asks_all.at[me], owner(step)[1]))
    others = pl.ds(0, seq_count - 1)
    mine = attend(half)
    arrived(swap_in, swap_slot, "swap")
    theirs = swap_in[...]
    front = jnp.where(half == 0, mine, theirs)
    back = jnp.where(half == 0, theirs, mine)
    attended = jnp.concatenate(
        [front[:, :128], front[:, 128:] + back[:, :128], back[:, 128:]], axis=1
    )
    for plane in range(planes):
        hear_y(wo_all, plane, wo_y, "wo_y")
        unpack(2 * plane + 1 - y)
    partial = lax.dot_general(
        attended,
        wo_full[...].reshape(depth, wo_full.shape[2]),
        (((1,), (1,)), ((), ())),
        preferred_element_type=jnp.float32,
    )
    both = 2 * group_rows
    top, bottom = partial[:both], partial[both:]
    core_out[...] = jnp.where(c == 0, bottom, top).astype(jnp.bfloat16)
    send(core_out, core_in, twin, core_slot, core_slot)
    kept = jnp.where(c == 0, top, bottom)
    arrived(core_in, core_slot, "core")
    wkv_send(1)
    kept = kept + core_in[...].astype(jnp.float32)
    top, bottom = kept[:group_rows], kept[group_rows:]
    side_out[...] = jnp.where(x == 0, bottom, top).astype(jnp.bfloat16)
    send(side_out, side_in, beside, side_slot, side_slot)
    kept = jnp.where(x == 0, top, bottom) + rows_all[half, quarter, :].astype(jnp.float32)
    arrived(side_in, side_slot, "side")
    hidden = kept + side_in[...].astype(jnp.float32)
    merged = rms_scale(hidden, merge_gain_ref[...].reshape(1, -1)).astype(jnp.bfloat16)
    merged_out[...] = merged.reshape(planes, share, depth)

    mz, mx, mc, mxc, key_slots, value_slots = (slots(planes) for _ in range(6))
    for k in range(far):
        to = target(k)
        send(merged_out.at[to], merged_all.at[z, group], at(to, y, x, c), mz + k, mz + z)
    merged_all[z, group] = merged_out[z]
    side_group, twin_group = 2 * c + 1 - x, 2 * (1 - c) + x
    cross_group = 2 * (1 - c) + 1 - x

    def spread(plane, block):
        here = merged_all.at[plane, group]
        send(block, here, beside, mx + plane, mx + plane)
        send(block, here, twin, mc + plane, mc + plane)

    def relay(plane):
        block = merged_all.at[plane, side_group]
        arrived(block, mx + plane, "mx")
        send(block, block, twin, mxc + plane, mxc + plane)

    frame_tokens = frame_rows // 4

    def project(plane):
        arrived(merged_all.at[plane, twin_group], mc + plane, "mc")
        arrived(merged_all.at[plane, cross_group], mxc + plane, "mxc")
        block = merged_all[plane].reshape(frame_tokens, depth)
        weights = wkv_all[...].reshape(depth, kv_ref.shape[1])
        return jnp.dot(block, weights, preferred_element_type=jnp.float32)

    def project_to(plane):
        product = project(plane)
        key_out[plane] = product[:, :kv_columns]
        value_out[plane] = product[:, kv_columns:].astype(jnp.bfloat16)
        to = at(plane, y, x, c)
        send(key_out.at[plane], key_in.at[z], to, key_slots + plane, key_slots + z)
        send(value_out.at[plane], value_in.at[z], to, value_slots + plane, value_slots + z)

    planes_heard = [source(j) for j in range(far)]
    spread(z, merged_out.at[z])
    for j in range(far):
        plane = planes_heard[j]
        arrived(merged_all.at[plane, group], mz + plane, "mz")
        spread(plane, merged_all.at[plane, group])
        relay(planes_heard[j - 1] if j else z)
    for i in range(2):
        arrived(wkv_all.at[1 - y, wkv_parts[i]], wkv_slot + i, "wkv")
    for plane in planes_heard[:-1]:
        project_to(plane)
    relay(planes_heard[-1])
    project_to(planes_heard[-1])
    visual = project(z)
    keys, values = visual[:, :kv_columns], visual[:, kv_columns:]
    for plane in planes_heard:
        arrived(key_in.at[plane], key_slots + plane, "key")
        arrived(value_in.at[plane], value_slots + plane, "value")
        keys = keys + key_in[plane]
        values = values + value_in[plane].astype(jnp.float32)
    all_keys, all_values = keys.astype(jnp.bfloat16), values.astype(jnp.bfloat16)

    arrived(asks_all.at[others], ask_slot, "ask")
    all_rows = seq_count * asks_ref.shape[1]
    own_rows = asks_ref.shape[1]
    questions = range_ref.shape[1]
    seen = jnp.concatenate(
        [
            jnp.full(
                (asking, 1),
                jnp.where((range_ref[0, q] <= me) & (me < range_ref[1, q]), 0.0, -1e30),
                jnp.float32,
            )
            for q in range(questions)
        ],
        axis=0,
    )
    level_out[...] = jnp.zeros_like(level_out)
    diagonal = lax.broadcasted_iota(
        jnp.int32, (all_rows, all_rows), 0
    ) == lax.broadcasted_iota(jnp.int32, (all_rows, all_rows), 1)
    for g in range(kv_heads):
        ask = asks_all[:, g].reshape(all_rows, HD)
        keys = all_keys[:, g * HD : (g + 1) * HD]
        values = all_values[:, g * HD : (g + 1) * HD]
        scores = (
            lax.dot_general(
                ask, keys, (((1,), (1,)), ((), ())), preferred_element_type=jnp.float32
            )
            * scale
        )
        highest = jnp.max(scores, axis=1, keepdims=True)
        weights = jnp.exp(scores - highest)
        total = jnp.sum(weights, axis=1, keepdims=True)
        mix = (
            jnp.dot(weights.astype(jnp.bfloat16), values, preferred_element_type=jnp.float32)
            / total
        )
        level = highest + jnp.log(total) + seen
        mixed_out[:, g] = mix.astype(jnp.bfloat16).reshape(seq_count, own_rows, HD)
        level_out[g : g + 1, :] = jnp.sum(
            jnp.where(diagonal, level, 0.0), axis=0, keepdims=True
        )
    mixed_in[me] = mixed_out[me]
    level_in[me] = level_out[...]
    send_all(
        seq_count,
        mix_slot,
        lambda step: (mixed_out.at[owner(step)[0]], mixed_in.at[me], owner(step)[1]),
    )
    send_all(seq_count, level_slot, lambda step: (level_out, level_in.at[me], owner(step)[1]))
    arrived(mixed_in.at[others], mix_slot, "mix")
    arrived(level_in.at[others], level_slot, "level")
    row = lax.broadcasted_iota(jnp.int32, (own_rows, all_rows), 0)
    place = lax.broadcasted_iota(jnp.int32, (own_rows, all_rows), 1)
    chosen = place == row + me * own_rows
    answers = []
    for g in range(kv_heads):
        mix, level = tails[g]
        levels = [
            jnp.sum(jnp.where(chosen, level_in[s, g : g + 1, :], 0.0), axis=1, keepdims=True)
            for s in range(seq_count)
        ]
        highest = level
        for other_level in levels:
            highest = jnp.maximum(highest, other_level)
        share_of = jnp.exp(level - highest)
        total = share_of
        answer = share_of * mix
        for s in range(seq_count):
            share_of = jnp.exp(levels[s] - highest)
            total = total + share_of
            answer = answer + share_of * mixed_in[s, g].astype(jnp.float32)
        answers.append(answer / total)
    out_ref[...] = jnp.concatenate(
        [
            jnp.concatenate(
                [
                    answers[g][q * asking + j : q * asking + j + 1]
                    for g in range(kv_heads)
                    for j in range(asking)
                ],
                axis=1,
            )
            for q in range(quest_count)
        ],
        axis=0,
    ).astype(jnp.bfloat16)
    for copy in started:
        copy.wait_send()
    for block, slot in (
        (asks_all.at[others], ask_slot),
        (mixed_in.at[others], mix_slot),
        (level_in.at[others], level_slot),
    ):
        copy_of(block, block, twin, slot, slot).wait_send()
    for inside, copy in guarded:

        @pl.when(inside)
        def _(copy=copy):
            copy.wait_send()


def fused(
    patches,
    norm_gain,
    w_qkv,
    w_out,
    window_order,
    merge_gain,
    w_kv,
    queries,
    suffix_kv,
    question_lengths,
    frame_range,
):
    seq_count, head_count = lax.axis_size("seq"), lax.axis_size("head")
    planes = seq_count // 2
    frame_rows, depth = patches.shape
    rows, _, columns = w_qkv.shape
    half = columns // 2
    kv_columns = w_kv.shape[2]
    kv_heads = kv_columns // HD
    bf16 = jnp.bfloat16
    wq_width = -(-3 * half // 128) * 128
    asks_shape = (kv_heads, queries.size // (kv_heads * HD), HD)
    own_rows = asks_shape[1]
    group_rows = frame_rows // head_count
    share = group_rows // 4
    messages = 9 + 11 * (seq_count // 2)
    arguments = (
        patches,
        norm_gain,
        merge_gain,
        w_qkv.transpose(1, 0, 2),
        w_out.T,
        window_order,
        w_kv,
        queries,
        suffix_kv,
        question_lengths,
        frame_range.T,
    )
    answers = pl.pallas_call(
        functools.partial(fused_kernel, seq_count, head_count),
        out_shape=pltpu.VMEM(queries.shape, bf16),
        in_specs=[pl.BlockSpec(memory_space=pl.ANY)] * len(arguments),
        out_specs=VMEM,
        scratch_shapes=[pltpu.VMEM(array.shape, array.dtype) for array in arguments[:-2]]
        + [pltpu.SMEM(array.shape, array.dtype) for array in arguments[-2:]]
        + [
            pltpu.VMEM((3, rows, wq_width), jnp.float32),
            pltpu.VMEM((2, rows, wq_width), bf16),
            pltpu.VMEM((w_kv.shape[0], 2 * kv_columns), bf16),
            pltpu.VMEM(asks_shape, bf16),
            pltpu.VMEM((2, frame_rows, depth), bf16),
            pltpu.VMEM((2,) + window_order.shape, jnp.int32),
            pltpu.VMEM((2, frame_rows, depth), bf16),
            pltpu.VMEM((seq_count, rows, wq_width), bf16),
            pltpu.VMEM((5, 80, 128), bf16),
            pltpu.VMEM((seq_count, 5, 80, 128), bf16),
            pltpu.VMEM((seq_count, rows, 384), bf16),
            pltpu.VMEM((2, w_kv.shape[0], 2 * kv_columns), bf16),
            pltpu.VMEM((seq_count,) + asks_shape, bf16),
            pltpu.VMEM((frame_rows, 256), bf16),
            pltpu.VMEM((frame_rows, 256), bf16),
            pltpu.VMEM((2 * group_rows, depth), bf16),
            pltpu.VMEM((2 * group_rows, depth), bf16),
            pltpu.VMEM((group_rows, depth), bf16),
            pltpu.VMEM((group_rows, depth), bf16),
            pltpu.VMEM((planes, share, depth), bf16),
            pltpu.VMEM((planes, head_count, share, depth), bf16),
            pltpu.VMEM((planes, frame_rows // 4, kv_columns), jnp.float32),
            pltpu.VMEM((planes, frame_rows // 4, kv_columns), jnp.float32),
            pltpu.VMEM((planes, frame_rows // 4, kv_columns), bf16),
            pltpu.VMEM((planes, frame_rows // 4, kv_columns), bf16),
            pltpu.VMEM((seq_count,) + asks_shape, bf16),
            pltpu.VMEM((seq_count,) + asks_shape, bf16),
            pltpu.VMEM((8, seq_count * own_rows), jnp.float32),
            pltpu.VMEM((seq_count, 8, seq_count * own_rows), jnp.float32),
            pltpu.SemaphoreType.DMA((len(arguments),)),
            pltpu.SemaphoreType.DMA((messages,)),
            pltpu.SemaphoreType.DMA((messages,)),
        ],
        compiler_params=pltpu.CompilerParams(
            collective_id=0, has_side_effects=True, vmem_limit_bytes=60 << 20
        ),
        name="fused",
    )(*arguments)
    return answers


def device_program(*arguments):
    patches, _, w_qkv, _, window_order = arguments[:5]
    paired = lax.axis_size("seq") == 8 and lax.axis_size("head") == 4
    whole = patches.shape[0] == FPATCH and window_order.shape[0] == 1
    if paired and whole and w_qkv.shape[0] % 16 == 0:
        return fused(*arguments)
    return on_device(*arguments)


def solution(mesh):
    placed = (
        P("seq", None),
        P(),
        P("seq", None, "head"),
        P("head", "seq"),
        P("seq", None),
        P(),
        P("seq", None, "head"),
        P("seq", "head"),
        P("seq", None, None, "head"),
        P("seq"),
        P(),
    )
    return jax.shard_map(
        device_program, mesh=mesh, in_specs=placed, out_specs=P("seq", "head"), check_vma=False
    )
```

```python
import functools

import jax
import jax.numpy as jnp
from jax import lax
from jax.experimental import pallas as pl
from jax.experimental.pallas import tpu as pltpu
from jax.sharding import PartitionSpec as P

VD = 1280
VH = 16
HD = 128
FPATCH = 256
WIN = 64

MESH = pl.DeviceIdType.MESH
VMEM = pl.BlockSpec(memory_space=pltpu.VMEM)


def rms_scale(values, gain):
    return values * lax.rsqrt(jnp.mean(values * values, axis=-1, keepdims=True) + 1e-06) * gain


def exchange_kernel(axis, count, gather, x_ref, out_ref, send_sem, recv_sem, own_sem):
    me = lax.axis_index(axis)
    barrier = pltpu.get_barrier_semaphore()
    for step in range(1, count):
        pl.semaphore_signal(
            barrier, inc=1, device_id={axis: lax.rem(me + step, count)}, device_id_type=MESH
        )
    pl.semaphore_wait(barrier, count - 1)
    copies = []
    for step in range(1, count):
        peer = lax.rem(me + step, count)
        copy = pltpu.make_async_remote_copy(
            src_ref=x_ref if gather else x_ref.at[peer],
            dst_ref=out_ref.at[me],
            send_sem=send_sem.at[step],
            recv_sem=recv_sem.at[step],
            device_id={axis: peer},
            device_id_type=MESH,
        )
        copy.start()
        copies.append(copy)
    own = pltpu.make_async_copy(x_ref if gather else x_ref.at[me], out_ref.at[me], own_sem)
    own.start()
    own.wait()
    for copy in copies:
        copy.wait()


def exchange(x, axis, gather, collective_id):
    count = lax.axis_size(axis)
    shape = ((count,) + x.shape) if gather else x.shape
    return pl.pallas_call(
        functools.partial(exchange_kernel, axis, count, gather),
        out_shape=jax.ShapeDtypeStruct(shape, x.dtype),
        in_specs=[VMEM],
        out_specs=VMEM,
        scratch_shapes=[
            pltpu.SemaphoreType.DMA((count,)),
            pltpu.SemaphoreType.DMA((count,)),
            pltpu.SemaphoreType.DMA,
        ],
        compiler_params=pltpu.CompilerParams(collective_id=collective_id, has_side_effects=True),
        name=f"exchange_{collective_id}",
    )(x)


def ring_kernel(count, qkv_ref, wout_ref, qkv_out, wout_out, send_sem, recv_sem, own_sem):
    me = lax.axis_index("seq")
    odd = lax.rem(me, 2)
    place = (1 - odd) * (me // 2) + odd * (count - 1 - me // 2)

    def index_of(position):
        position = lax.rem(position + count, count)
        late = position // (count // 2)
        return (1 - late) * 2 * position + late * (2 * (count - 1 - position) + 1)

    neighbours = (index_of(place + 1), index_of(place - 1))
    barrier = pltpu.get_barrier_semaphore()
    for neighbour in neighbours:
        pl.semaphore_signal(barrier, inc=1, device_id={"seq": neighbour}, device_id_type=MESH)
    pl.semaphore_wait(barrier, 2)
    far, near = count // 2, count - 1 - count // 2
    pieces = 4

    def slot(piece, source):
        return qkv_out.at[piece, source] if piece < 3 else wout_out.at[source]

    def own(piece):
        return qkv_ref.at[piece] if piece < 3 else wout_ref

    copies = {}
    for step in range(far):
        for piece in range(pieces):
            for way in range(2):
                hops = far if (piece < 2) == (way == 0) else near
                if step >= hops:
                    continue
                source = index_of(place - step if way == 0 else place + step)
                if step > 0:
                    copies[step - 1, piece, way].wait_recv()
                copy = pltpu.make_async_remote_copy(
                    src_ref=own(piece) if step == 0 else slot(piece, source),
                    dst_ref=slot(piece, source),
                    send_sem=send_sem.at[step, piece, way],
                    recv_sem=recv_sem.at[step, piece, way],
                    device_id={"seq": neighbours[way]},
                    device_id_type=MESH,
                )
                copy.start()
                copies[step, piece, way] = copy
    kept = [pltpu.make_async_copy(own(p), slot(p, me), own_sem.at[p]) for p in range(pieces)]
    for copy in kept:
        copy.start()
    for copy in kept:
        copy.wait()
    for (step, piece, way), copy in copies.items():
        if (step + 1, piece, way) not in copies:
            copy.wait_recv()
    for copy in copies.values():
        copy.wait_send()


def ring_weights(w_qkv, w_out):
    count = lax.axis_size("seq")
    far = count // 2
    return pl.pallas_call(
        functools.partial(ring_kernel, count),
        out_shape=(
            jax.ShapeDtypeStruct((3, count) + w_qkv.shape[1:], w_qkv.dtype),
            jax.ShapeDtypeStruct((count,) + w_out.shape, w_out.dtype),
        ),
        in_specs=[VMEM, VMEM],
        out_specs=(VMEM, VMEM),
        scratch_shapes=[
            pltpu.SemaphoreType.DMA((far, 4, 2)),
            pltpu.SemaphoreType.DMA((far, 4, 2)),
            pltpu.SemaphoreType.DMA((4,)),
        ],
        compiler_params=pltpu.CompilerParams(collective_id=0, has_side_effects=True),
        name="ring_weights",
    )(w_qkv, w_out)


def frame_attention(query, key, value, unit_order, head_size):
    unit_count = unit_order.shape[0]
    patch_count = unit_count * 4
    ranks = jnp.sum(
        jnp.where(
            unit_order[None, :] == (jnp.arange(patch_count) // 4)[:, None],
            jnp.arange(unit_count)[None, :] // (WIN // 4),
            0,
        ),
        axis=1,
    )
    same = ranks[:, None] == ranks[None, :]
    scores = jnp.einsum(
        "qhd,khd->hqk", query, key, preferred_element_type=jnp.float32
    ) * head_size ** (-0.5)
    scores = jnp.where(same[None], scores, -jnp.inf)
    weights = jax.nn.softmax(scores, axis=-1).astype(jnp.bfloat16)
    return jnp.einsum(
        "hqk,khd->qhd", weights, value, preferred_element_type=jnp.float32
    ).astype(jnp.bfloat16)


def on_device(
    patches,
    norm_gain,
    w_qkv,
    w_out,
    window_order,
    merge_gain,
    w_kv,
    queries,
    suffix_kv,
    question_lengths,
    frame_range,
):
    head_count = lax.axis_size("head")
    seq_count = lax.axis_size("seq")
    row_count = patches.shape[0]
    frame_count = window_order.shape[0]
    columns = w_qkv.shape[2]
    head_size = VD // VH
    local_heads = columns // head_size
    source = patches.astype(jnp.float32)
    normed = rms_scale(source, norm_gain).astype(jnp.bfloat16)
    qkv_all, w_out_all = ring_weights(w_qkv.transpose(1, 0, 2), w_out)
    qkv_all = qkv_all.reshape(3, -1, columns)
    query, key, value = [
        jnp.dot(normed, qkv_all[part], preferred_element_type=jnp.float32)
        .astype(jnp.bfloat16)
        .reshape(frame_count, -1, local_heads, head_size)
        for part in range(3)
    ]
    attended = jax.vmap(
        lambda q, k, v, order: frame_attention(q, k, v, order, head_size)
    )(query, key, value, window_order).reshape(row_count, columns)
    w_full = w_out_all.transpose(1, 0, 2).reshape(columns, VD)
    share_rows = row_count // head_count
    partial = jnp.dot(attended, w_full, preferred_element_type=jnp.float32).astype(jnp.bfloat16)
    parts = exchange(partial.reshape(head_count, share_rows, VD), "head", False, 1)
    shared = jnp.sum(parts.astype(jnp.float32), axis=0)
    own_rows = lax.dynamic_slice_in_dim(source, lax.axis_index("head") * share_rows, share_rows, 0)
    merged = rms_scale(own_rows + shared, merge_gain).astype(jnp.bfloat16)
    share_tokens = share_rows // 4
    depth = w_kv.shape[0]
    merged = merged.reshape(share_tokens, seq_count, depth).transpose(1, 0, 2)
    merged = exchange(merged, "seq", False, 2)
    merged = exchange(merged, "head", True, 3)
    merged = merged.transpose(1, 0, 2, 3).reshape(-1, depth)
    kv_columns = w_kv.shape[2]
    partial = jnp.dot(
        merged, w_kv.reshape(depth, 2 * kv_columns), preferred_element_type=jnp.float32
    ).astype(jnp.bfloat16)
    parts = exchange(partial.reshape(seq_count, -1, 2 * kv_columns), "seq", False, 4)
    visual = jnp.sum(parts.astype(jnp.float32), axis=0).astype(jnp.bfloat16)
    visual = exchange(visual, "seq", True, 5).reshape(-1, 2 * kv_columns)

    token_count = visual.shape[0]
    quest_count = queries.shape[0]
    span = suffix_kv.shape[1]
    kv_local = kv_columns // HD
    asking = queries.reshape(quest_count, kv_local, -1, HD)
    frame_tokens = FPATCH // 4
    seq_index = lax.axis_index("seq")
    bounds = lax.dynamic_slice_in_dim(frame_range, seq_index * quest_count, quest_count, 0)
    frame_index = jnp.arange(token_count) // frame_tokens
    live = (frame_index[None, :] >= bounds[:, 0:1]) & (frame_index[None, :] < bounds[:, 1:2])
    suffix_live = jnp.arange(span)[None, :] < question_lengths[:, None]
    suffix = suffix_kv.reshape(quest_count, span, 2, kv_local, HD)
    answers = []
    for g in range(kv_local):
        ask = asking[:, g]
        keys = visual[:, g * HD : (g + 1) * HD]
        values = visual[:, kv_columns + g * HD : kv_columns + (g + 1) * HD]
        scores = jnp.einsum(
            "qjd,nd->qjn", ask, keys, preferred_element_type=jnp.float32
        ) * HD ** (-0.5)
        scores = jnp.where(live[:, None, :], scores, -jnp.inf)
        tail = jnp.einsum(
            "qjd,qsd->qjs", ask, suffix[:, :, 0, g], preferred_element_type=jnp.float32
        ) * HD ** (-0.5)
        tail = jnp.where(suffix_live[:, None, :], tail, -jnp.inf)
        highest = jnp.maximum(
            jnp.max(scores, axis=-1, keepdims=True), jnp.max(tail, axis=-1, keepdims=True)
        )
        weights = jnp.exp(scores - highest)
        tail_weights = jnp.exp(tail - highest)
        totals = jnp.sum(weights, axis=-1, keepdims=True) + jnp.sum(
            tail_weights, axis=-1, keepdims=True
        )
        mixed = jnp.einsum(
            "qjn,nd->qjd", weights.astype(jnp.bfloat16), values, preferred_element_type=jnp.float32
        ) + jnp.einsum(
            "qjs,qsd->qjd",
            tail_weights.astype(jnp.bfloat16),
            suffix[:, :, 1, g],
            preferred_element_type=jnp.float32,
        )
        answers.append((mixed / totals).astype(jnp.bfloat16))
    return jnp.stack(answers, axis=1).reshape(quest_count, -1)


def fused_kernel(
    seq_count,
    head_count,
    patches_in,
    norm_gain_in,
    merge_gain_in,
    wqkv_in,
    wo_in,
    order_in,
    wkv_in,
    queries_in,
    suffix_in,
    lengths_in,
    range_in,
    out_ref,
    patches_ref,
    norm_gain_ref,
    merge_gain_ref,
    wqkv_ref,
    wo_ref,
    order_ref,
    wkv_ref,
    queries_ref,
    suffix_ref,
    lengths_ref,
    range_ref,
    wide,
    wq_ref,
    kv_ref,
    asks_ref,
    rows_all,
    order_all,
    normed,
    wq_all,
    wo_packed,
    wo_all,
    wo_full,
    wkv_all,
    asks_all,
    swap_out,
    swap_in,
    core_out,
    core_in,
    side_out,
    side_in,
    merged_out,
    merged_all,
    key_out,
    key_in,
    value_out,
    value_in,
    mixed_out,
    mixed_in,
    level_out,
    level_in,
    load_sems,
    send_sems,
    recv_sems,
):
    planes = seq_count // 2
    me = lax.axis_index("seq")
    head = lax.axis_index("head")
    z, y = me // 2, lax.rem(me, 2)
    x, c = head // 2, lax.rem(head, 2)
    half = lax.rem(z, 2)
    group = 2 * c + x
    frame_rows, depth = patches_ref.shape
    group_rows = frame_rows // head_count
    share = group_rows // 4
    head_size = VD // VH
    own_width = 2 * head_size

    def at(z_to, y_to, x_to, c_to):
        return {"seq": 2 * z_to + y_to, "head": 2 * x_to + c_to}

    partner = z + 1 - 2 * half
    across = at(z, 1 - y, x, c)
    beside = at(z, y, 1 - x, c)
    twin = at(z, y, x, 1 - c)
    paired = at(partner, y, x, c)

    low = z < planes // 2
    inner = (z > 0) & (z < planes - 1)

    def ordered(outer_plane, inner_plane):
        plane = jnp.where(inner, inner_plane, outer_plane)
        return jnp.where(low, plane, planes - 1 - plane)

    def target(k):
        return ordered((3, 2, 1)[k], (2, 0, 3)[k])

    def source(j):
        return ordered((1, 3, 2)[j], (2, 3, 0)[j])

    barrier = pltpu.get_barrier_semaphore()
    peers = [
        {"seq": lax.rem(me + step, seq_count), "head": head} for step in range(1, seq_count)
    ] + [beside, twin]
    for peer in peers:
        pl.semaphore_signal(barrier, inc=1, device_id=peer, device_id_type=MESH)

    pairs = (
        (wqkv_in, wqkv_ref),
        (patches_in, patches_ref),
        (order_in, order_ref),
        (norm_gain_in, norm_gain_ref),
        (wo_in, wo_ref),
        (wkv_in, wkv_ref),
        (queries_in, queries_ref),
        (suffix_in, suffix_ref),
        (lengths_in, lengths_ref),
        (merge_gain_in, merge_gain_ref),
        (range_in, range_ref),
    )
    loads = [
        pltpu.make_async_copy(src, dst, load_sems.at[i]) for i, (src, dst) in enumerate(pairs)
    ]
    for load in loads:
        load.start()
    taken = []
    started = []
    guarded = []

    def slots(count=1):
        taken.append(count)
        return sum(taken) - count

    def copy_of(src, dst, device, send_slot, recv_slot):
        return pltpu.make_async_remote_copy(
            src_ref=src,
            dst_ref=dst,
            send_sem=send_sems.at[send_slot],
            recv_sem=recv_sems.at[recv_slot],
            device_id=device,
            device_id_type=MESH,
        )

    def send(src, dst, device, send_slot, recv_slot):
        copy = copy_of(src, dst, device, send_slot, recv_slot)
        copy.start()
        started.append(copy)
        return copy

    def send_if(inside, src, dst, device, send_slot, recv_slot):
        copy = copy_of(src, dst, device, send_slot, recv_slot)

        @pl.when(inside)
        def _():
            copy.start()

        guarded.append((inside, copy))

    def send_all(count, slot, copy_at):
        for step in range(1, count):
            src, dst, device = copy_at(step)
            copy_of(src, dst, device, slot, slot).start()

    def left(copy):
        started[:] = [kept for kept in started if kept is not copy]
        copy.wait_send()

    def arrived(ref, slot, name):
        copy_of(ref, ref, twin, slot, slot).wait_recv()

    for load in loads[:3]:
        load.wait()

    for part in range(head_count):
        row = lax.broadcasted_iota(jnp.int32, (group_rows, frame_rows), 0)
        place = lax.broadcasted_iota(jnp.int32, (group_rows, frame_rows), 1)
        picked = 4 * (share * part + lax.rem(row, share)) + row // share
        pick = jnp.where(place == picked, 1.0, 0.0).astype(jnp.bfloat16)
        rows_all[half, pl.ds(part * group_rows, group_rows), :] = jnp.dot(
            pick, patches_ref[...], preferred_element_type=jnp.float32
        ).astype(jnp.bfloat16)
    columns = wqkv_ref.shape[2]
    wq_width = wq_ref.shape[2]
    lane = lax.broadcasted_iota(jnp.int32, wq_ref.shape[1:], 1)
    packed = [jnp.zeros(wq_ref.shape[1:], jnp.float32)] * 2
    wide[...] = jnp.zeros_like(wide)
    for part in range(3):
        wide[part, :, :columns] = wqkv_ref[part].astype(jnp.float32)
        for side in range(2):
            shift = (part - side) * own_width
            moved = wide[part] if shift == 0 else pltpu.roll(wide[part], shift % wq_width, 1)
            inside = (lane >= part * own_width) & (lane < (part + 1) * own_width)
            packed[side] = jnp.where(inside, moved, packed[side])
    for side in range(2):
        wq_ref[side] = packed[side].astype(jnp.bfloat16)
    order_all[half] = order_ref[...]
    pl.semaphore_wait(barrier, len(peers))

    quarter = pl.ds(pl.multiple_of(group * group_rows, group_rows), group_rows)
    far = planes - 1
    order_slot, rows_slot, rows_x_slot, rows_c_slot, rows_xc_slot = (slots() for _ in range(5))
    wq_z, wq_y, wo_z, wo_y = (slots(planes) for _ in range(4))
    send(order_all.at[half], order_all.at[half], paired, order_slot, order_slot)

    def wq_send(k, inside=None):
        to = target(k)
        copy = (
            wq_ref.at[lax.rem(to, 2)],
            wq_all.at[me],
            at(to, y, x, c),
            wq_z + k,
            wq_z + z,
        )
        return send(*copy) if inside is None else send_if(inside, *copy)

    def over_y(ref, plane, base):
        own = ref.at[2 * plane + y]
        return send(own, own, across, base + plane, base + plane)

    def hear_y(ref, plane, base, name):
        arrived(ref.at[2 * plane + 1 - y], base + plane, name)

    def wq_hear(j):
        plane = source(j)
        arrived(wq_all.at[2 * plane + y], wq_z + plane, "wq_z")
        return over_y(wq_all, plane, wq_y)

    outer = jnp.logical_not(inner)
    wq_first = wq_send(0)
    wq_send(1, inner)
    wq_all[me] = wq_ref[half]
    send(wq_ref.at[half], wq_all.at[me], across, wq_y + z, wq_y + z)

    for load in loads[3:]:
        load.wait()
    kv_columns = wkv_ref.shape[2]
    for side in range(2):
        kv_ref[:, side * kv_columns : (side + 1) * kv_columns] = wkv_ref[:, side, :]
    early = kv_ref.shape[0] // 4
    wkv_slot = slots(2)
    wkv_parts = (pl.ds(0, early), pl.ds(early, kv_ref.shape[0] - early))

    def wkv_send(i):
        part = wkv_parts[i]
        send(kv_ref.at[part], wkv_all.at[y, part], across, wkv_slot + i, wkv_slot + i)

    wkv_send(0)
    wkv_all[y] = kv_ref[...]
    for i in range(2):
        for j in range(2):
            wo_packed[2 * i + j] = wo_ref[i * 80 : (i + 1) * 80, j * 128 : (j + 1) * 128]
    wo_packed[4] = jnp.concatenate(
        [wo_ref[:80, 256:320], wo_ref[80:, 256:320]], axis=1
    )
    wo_all[me] = wo_packed[...]
    asked = queries_ref[...].astype(jnp.float32)
    quest_count = asked.shape[0]
    kv_heads = wkv_ref.shape[2] // HD
    asking = asked.shape[1] // (kv_heads * HD)
    for g in range(kv_heads):
        asks_ref[g] = jnp.concatenate(
            [
                asked[q : q + 1, (g * asking + j) * HD : (g * asking + j + 1) * HD]
                for q in range(quest_count)
                for j in range(asking)
            ],
            axis=0,
        ).astype(jnp.bfloat16)
    asks_all[me] = asks_ref[...]

    def normalise(slot):
        for part in range(head_count):
            rows = pl.ds(part * group_rows, group_rows)
            source = rows_all[slot, rows, :].astype(jnp.float32)
            normed[slot, rows, :] = rms_scale(source, norm_gain_ref[...].reshape(1, -1)).astype(jnp.bfloat16)

    normalise(half)

    left(wq_first)
    rows_copy = send(
        rows_all.at[half, quarter], rows_all.at[half, quarter], paired, rows_slot, rows_slot
    )
    wq_send(2, inner)
    wq_send(1, outer)
    wq_hear(0)
    over_y(wo_all, z, wo_y)
    left(rows_copy)
    wq_send(2, outer)

    scale = HD ** (-0.5)
    tails = []
    for g in range(kv_heads):
        columns = slice(g * HD, (g + 1) * HD)
        mixes, levels = [], []
        for q in range(quest_count):
            ask = asks_ref[g, q * asking : (q + 1) * asking, :]
            keys = suffix_ref[q, :, 0, columns]
            values = suffix_ref[q, :, 1, columns]
            scores = (
                lax.dot_general(
                    ask, keys, (((1,), (1,)), ((), ())), preferred_element_type=jnp.float32
                )
                * scale
            )
            place = lax.broadcasted_iota(jnp.int32, scores.shape, 1)
            scores = jnp.where(place < lengths_ref[q], scores, -1e30)
            highest = jnp.max(scores, axis=1, keepdims=True)
            weights = jnp.exp(scores - highest)
            total = jnp.sum(weights, axis=1, keepdims=True)
            mix = jnp.dot(
                weights.astype(jnp.bfloat16), values, preferred_element_type=jnp.float32
            )
            mixes.append(mix / total)
            levels.append(highest + jnp.log(total))
        tails.append((jnp.concatenate(mixes, axis=0), jnp.concatenate(levels, axis=0)))

    other = 1 - half
    def wo_send(k):
        send(wo_packed, wo_all.at[me], at(target(k), y, x, c), wo_z + k, wo_z + z)

    theirs = rows_all.at[other, quarter]
    arrived(theirs, rows_slot, "rows")
    send(theirs, theirs, beside, rows_x_slot, rows_x_slot)
    send(theirs, theirs, twin, rows_c_slot, rows_c_slot)
    wq_hear(1)
    for k in range(far - 1):
        wo_send(k)
    for j in range(2, far):
        wq_hear(j)
    wo_send(far - 1)

    def unpack(slice_at):
        for i in range(2):
            for j in range(2):
                wo_full[slice_at, i * 80 : (i + 1) * 80, j * 128 : (j + 1) * 128] = wo_all[
                    slice_at, 2 * i + j
                ]
        last = wo_all[slice_at, 4]
        wo_full[slice_at, :80, 256:384] = last
        wo_full[slice_at, 80:, 256:384] = pltpu.roll(last.astype(jnp.float32), 64, 1).astype(
            jnp.bfloat16
        )

    wo_relays = {}

    def wo_hear(j, inside=None):
        plane = source(j)
        own = wo_all.at[2 * plane + y]
        if j not in wo_relays:
            wo_relays[j] = copy_of(own, own, across, wo_y + plane, wo_y + plane)
            started.append(wo_relays[j])
        copy = wo_relays[j]

        def take():
            arrived(own, wo_z + plane, "wo_z")
            copy.start()
            unpack(2 * plane + y)

        if inside is None:
            take()
        else:
            pl.when(inside)(take)

    side_quarter = pl.ds(
        pl.multiple_of((2 * c + 1 - x) * group_rows, group_rows), group_rows
    )
    beside_rows = rows_all.at[other, side_quarter]
    arrived(beside_rows, rows_x_slot, "rows_x")
    send(beside_rows, beside_rows, twin, rows_xc_slot, rows_xc_slot)
    twin_quarter = pl.ds(
        pl.multiple_of((2 * (1 - c) + x) * group_rows, group_rows), group_rows
    )
    arrived(rows_all.at[other, twin_quarter], rows_c_slot, "rows_c")
    arrived(rows_all.at[other, twin_quarter], rows_xc_slot, "rows_xc")
    arrived(order_all.at[other], order_slot, "order")
    normalise(other)
    unpack(me)
    wo_hear(0)
    for plane in range(planes):
        hear_y(wq_all, plane, wq_y, "wq_y")
        if plane == 1:
            wo_hear(1, outer)

    lane = lax.broadcasted_iota(jnp.int32, (frame_rows, 256), 1)

    def attend(slot):
        unit_count = order_ref.shape[1]
        row = lax.broadcasted_iota(jnp.int32, (frame_rows, unit_count), 0)
        unit = row // group_rows * share + lax.rem(row, share)
        place = lax.broadcasted_iota(jnp.int32, (frame_rows, unit_count), 1)
        window = jnp.sum(
            jnp.where(order_all[slot] == unit, place // (WIN // 4), 0).astype(jnp.float32),
            axis=1,
            keepdims=True,
        )
        sort = lax.broadcasted_iota(jnp.int32, (frame_rows, 128), 1).astype(jnp.float32)
        member = jnp.where(window == sort, 1.0, 0.0).astype(jnp.bfloat16)
        same = (
            lax.dot_general(
                member, member, (((1,), (1,)), ((), ())), preferred_element_type=jnp.float32
            )
            > 0.5
        )
        qkv = jnp.dot(
            normed[slot],
            wq_all[...].reshape(depth, wq_ref.shape[2]),
            preferred_element_type=jnp.float32,
        )
        width = qkv.shape[1]
        query = qkv[:, :256].astype(jnp.bfloat16)
        key = pltpu.roll(qkv, width - own_width, 1)[:, :256].astype(jnp.bfloat16)
        value = pltpu.roll(qkv, width - 2 * own_width, 1)[:, :256].astype(jnp.bfloat16)
        mixed = jnp.zeros((frame_rows, 256), jnp.float32)
        for i in range(2):
            inside = (lane >= i * head_size) & (lane < (i + 1) * head_size)
            scores = lax.dot_general(
                jnp.where(inside, query, jnp.zeros_like(query)),
                key,
                (((1,), (1,)), ((), ())),
                preferred_element_type=jnp.float32,
            ) * head_size ** (-0.5)
            scores = jnp.where(same, scores, -1e30)
            weights = jnp.exp(scores - jnp.max(scores, axis=1, keepdims=True))
            weights = weights / jnp.sum(weights, axis=1, keepdims=True)
            product = jnp.dot(
                weights.astype(jnp.bfloat16), value, preferred_element_type=jnp.float32
            )
            mixed = jnp.where(inside, product, mixed)
        shifted = pltpu.roll(mixed, own_width - 128, 1)
        return jnp.where(half == 0, mixed, shifted).astype(jnp.bfloat16)

    swap_slot, core_slot, side_slot = slots(), slots(2), slots(2)
    swap_out[...] = attend(other)
    send(swap_out, swap_in, paired, swap_slot, swap_slot)
    wo_hear(1, inner)
    for j in range(2, far):
        wo_hear(j)
    ask_slot, mix_slot, level_slot = (slots() for _ in range(3))

    def owner(step):
        to = lax.rem(me + step, seq_count)
        return to, {"seq": to, "head": head}

    send_all(seq_count, ask_slot, lambda step: (asks_ref, asks_all.at[me], owner(step)[1]))
    others = pl.ds(0, seq_count - 1)
    mine = attend(half)
    arrived(swap_in, swap_slot, "swap")
    theirs = swap_in[...]
    front = jnp.where(half == 0, mine, theirs)
    back = jnp.where(half == 0, theirs, mine)
    attended = jnp.concatenate(
        [front[:, :128], front[:, 128:] + back[:, :128], back[:, 128:]], axis=1
    )
    for plane in range(planes):
        hear_y(wo_all, plane, wo_y, "wo_y")
        unpack(2 * plane + 1 - y)
    both = 2 * group_rows
    kept = []
    for i in range(2):
        part = wo_full[i * (seq_count // 2) : (i + 1) * (seq_count // 2)]
        partial = lax.dot_general(
            attended,
            part.reshape(depth // 2, wo_full.shape[2]),
            (((1,), (1,)), ((), ())),
            preferred_element_type=jnp.float32,
        )
        top, bottom = partial[:both], partial[both:]
        core_out[i] = jnp.where(c == 0, bottom, top).astype(jnp.bfloat16)
        send(core_out.at[i], core_in.at[i], twin, core_slot + i, core_slot + i)
        kept.append(jnp.where(c == 0, top, bottom))
    for i in range(2):
        arrived(core_in.at[i], core_slot + i, "core")
        total = kept[i] + core_in[i].astype(jnp.float32)
        top, bottom = total[:group_rows], total[group_rows:]
        side_out[i] = jnp.where(x == 0, bottom, top).astype(jnp.bfloat16)
        send(side_out.at[i], side_in.at[i], beside, side_slot + i, side_slot + i)
        kept[i] = jnp.where(x == 0, top, bottom)
    wkv_send(1)
    for i in range(2):
        arrived(side_in.at[i], side_slot + i, "side")
        kept[i] = kept[i] + side_in[i].astype(jnp.float32)
    hidden = jnp.concatenate(kept, axis=1) + rows_all[half, quarter, :].astype(jnp.float32)
    merged = rms_scale(hidden, merge_gain_ref[...].reshape(1, -1)).astype(jnp.bfloat16)
    merged_out[...] = merged.reshape(planes, share, depth)

    mz, mx, mc, mxc, key_slots, value_slots = (slots(planes) for _ in range(6))
    for k in range(far):
        to = target(k)
        send(merged_out.at[to], merged_all.at[z, group], at(to, y, x, c), mz + k, mz + z)
    merged_all[z, group] = merged_out[z]
    side_group, twin_group = 2 * c + 1 - x, 2 * (1 - c) + x
    cross_group = 2 * (1 - c) + 1 - x

    def spread(plane, block):
        here = merged_all.at[plane, group]
        send(block, here, beside, mx + plane, mx + plane)
        send(block, here, twin, mc + plane, mc + plane)

    def relay(plane):
        block = merged_all.at[plane, side_group]
        arrived(block, mx + plane, "mx")
        send(block, block, twin, mxc + plane, mxc + plane)

    frame_tokens = frame_rows // 4

    def project(plane):
        arrived(merged_all.at[plane, twin_group], mc + plane, "mc")
        arrived(merged_all.at[plane, cross_group], mxc + plane, "mxc")
        block = merged_all[plane].reshape(frame_tokens, depth)
        weights = wkv_all[...].reshape(depth, kv_ref.shape[1])
        return jnp.dot(block, weights, preferred_element_type=jnp.float32)

    def project_to(plane):
        product = project(plane)
        key_out[plane] = product[:, :kv_columns]
        value_out[plane] = product[:, kv_columns:].astype(jnp.bfloat16)
        to = at(plane, y, x, c)
        send(key_out.at[plane], key_in.at[z], to, key_slots + plane, key_slots + z)
        send(value_out.at[plane], value_in.at[z], to, value_slots + plane, value_slots + z)

    planes_heard = [source(j) for j in range(far)]
    spread(z, merged_out.at[z])
    for j in range(far):
        plane = planes_heard[j]
        arrived(merged_all.at[plane, group], mz + plane, "mz")
        spread(plane, merged_all.at[plane, group])
        relay(planes_heard[j - 1] if j else z)
    for i in range(2):
        arrived(wkv_all.at[1 - y, wkv_parts[i]], wkv_slot + i, "wkv")
    for plane in planes_heard[:-1]:
        project_to(plane)
    relay(planes_heard[-1])
    project_to(planes_heard[-1])
    visual = project(z)
    keys, values = visual[:, :kv_columns], visual[:, kv_columns:]
    for plane in planes_heard:
        arrived(key_in.at[plane], key_slots + plane, "key")
        arrived(value_in.at[plane], value_slots + plane, "value")
        keys = keys + key_in[plane]
        values = values + value_in[plane].astype(jnp.float32)
    all_keys, all_values = keys.astype(jnp.bfloat16), values.astype(jnp.bfloat16)

    arrived(asks_all.at[others], ask_slot, "ask")
    all_rows = seq_count * asks_ref.shape[1]
    own_rows = asks_ref.shape[1]
    questions = range_ref.shape[1]
    seen = jnp.concatenate(
        [
            jnp.full(
                (asking, 1),
                jnp.where((range_ref[0, q] <= me) & (me < range_ref[1, q]), 0.0, -1e30),
                jnp.float32,
            )
            for q in range(questions)
        ],
        axis=0,
    )
    level_out[...] = jnp.zeros_like(level_out)
    diagonal = lax.broadcasted_iota(
        jnp.int32, (all_rows, all_rows), 0
    ) == lax.broadcasted_iota(jnp.int32, (all_rows, all_rows), 1)
    for g in range(kv_heads):
        ask = asks_all[:, g].reshape(all_rows, HD)
        keys = all_keys[:, g * HD : (g + 1) * HD]
        values = all_values[:, g * HD : (g + 1) * HD]
        scores = (
            lax.dot_general(
                ask, keys, (((1,), (1,)), ((), ())), preferred_element_type=jnp.float32
            )
            * scale
        )
        highest = jnp.max(scores, axis=1, keepdims=True)
        weights = jnp.exp(scores - highest)
        total = jnp.sum(weights, axis=1, keepdims=True)
        mix = (
            jnp.dot(weights.astype(jnp.bfloat16), values, preferred_element_type=jnp.float32)
            / total
        )
        level = highest + jnp.log(total) + seen
        mixed_out[:, g] = mix.astype(jnp.bfloat16).reshape(seq_count, own_rows, HD)
        level_out[g : g + 1, :] = jnp.sum(
            jnp.where(diagonal, level, 0.0), axis=0, keepdims=True
        )
    mixed_in[me] = mixed_out[me]
    level_in[me] = level_out[...]
    send_all(
        seq_count,
        mix_slot,
        lambda step: (mixed_out.at[owner(step)[0]], mixed_in.at[me], owner(step)[1]),
    )
    send_all(seq_count, level_slot, lambda step: (level_out, level_in.at[me], owner(step)[1]))
    arrived(mixed_in.at[others], mix_slot, "mix")
    arrived(level_in.at[others], level_slot, "level")
    row = lax.broadcasted_iota(jnp.int32, (own_rows, all_rows), 0)
    place = lax.broadcasted_iota(jnp.int32, (own_rows, all_rows), 1)
    chosen = place == row + me * own_rows
    answers = []
    for g in range(kv_heads):
        mix, level = tails[g]
        levels = [
            jnp.sum(jnp.where(chosen, level_in[s, g : g + 1, :], 0.0), axis=1, keepdims=True)
            for s in range(seq_count)
        ]
        highest = level
        for other_level in levels:
            highest = jnp.maximum(highest, other_level)
        share_of = jnp.exp(level - highest)
        total = share_of
        answer = share_of * mix
        for s in range(seq_count):
            share_of = jnp.exp(levels[s] - highest)
            total = total + share_of
            answer = answer + share_of * mixed_in[s, g].astype(jnp.float32)
        answers.append(answer / total)
    out_ref[...] = jnp.concatenate(
        [
            jnp.concatenate(
                [
                    answers[g][q * asking + j : q * asking + j + 1]
                    for g in range(kv_heads)
                    for j in range(asking)
                ],
                axis=1,
            )
            for q in range(quest_count)
        ],
        axis=0,
    ).astype(jnp.bfloat16)
    for copy in started:
        copy.wait_send()
    for block, slot in (
        (asks_all.at[others], ask_slot),
        (mixed_in.at[others], mix_slot),
        (level_in.at[others], level_slot),
    ):
        copy_of(block, block, twin, slot, slot).wait_send()
    for inside, copy in guarded:

        @pl.when(inside)
        def _(copy=copy):
            copy.wait_send()


def fused(
    patches,
    norm_gain,
    w_qkv,
    w_out,
    window_order,
    merge_gain,
    w_kv,
    queries,
    suffix_kv,
    question_lengths,
    frame_range,
):
    seq_count, head_count = lax.axis_size("seq"), lax.axis_size("head")
    planes = seq_count // 2
    frame_rows, depth = patches.shape
    rows, _, columns = w_qkv.shape
    half = columns // 2
    kv_columns = w_kv.shape[2]
    kv_heads = kv_columns // HD
    bf16 = jnp.bfloat16
    wq_width = -(-3 * half // 128) * 128
    asks_shape = (kv_heads, queries.size // (kv_heads * HD), HD)
    own_rows = asks_shape[1]
    group_rows = frame_rows // head_count
    share = group_rows // 4
    messages = 11 + 11 * (seq_count // 2)
    arguments = (
        patches,
        norm_gain,
        merge_gain,
        w_qkv.transpose(1, 0, 2),
        w_out.T,
        window_order,
        w_kv,
        queries,
        suffix_kv,
        question_lengths,
        frame_range.T,
    )
    answers = pl.pallas_call(
        functools.partial(fused_kernel, seq_count, head_count),
        out_shape=pltpu.VMEM(queries.shape, bf16),
        in_specs=[pl.BlockSpec(memory_space=pl.ANY)] * len(arguments),
        out_specs=VMEM,
        scratch_shapes=[pltpu.VMEM(array.shape, array.dtype) for array in arguments[:-2]]
        + [pltpu.SMEM(array.shape, array.dtype) for array in arguments[-2:]]
        + [
            pltpu.VMEM((3, rows, wq_width), jnp.float32),
            pltpu.VMEM((2, rows, wq_width), bf16),
            pltpu.VMEM((w_kv.shape[0], 2 * kv_columns), bf16),
            pltpu.VMEM(asks_shape, bf16),
            pltpu.VMEM((2, frame_rows, depth), bf16),
            pltpu.VMEM((2,) + window_order.shape, jnp.int32),
            pltpu.VMEM((2, frame_rows, depth), bf16),
            pltpu.VMEM((seq_count, rows, wq_width), bf16),
            pltpu.VMEM((5, 80, 128), bf16),
            pltpu.VMEM((seq_count, 5, 80, 128), bf16),
            pltpu.VMEM((seq_count, rows, 384), bf16),
            pltpu.VMEM((2, w_kv.shape[0], 2 * kv_columns), bf16),
            pltpu.VMEM((seq_count,) + asks_shape, bf16),
            pltpu.VMEM((frame_rows, 256), bf16),
            pltpu.VMEM((frame_rows, 256), bf16),
            pltpu.VMEM((2, 2 * group_rows, depth // 2), bf16),
            pltpu.VMEM((2, 2 * group_rows, depth // 2), bf16),
            pltpu.VMEM((2, group_rows, depth // 2), bf16),
            pltpu.VMEM((2, group_rows, depth // 2), bf16),
            pltpu.VMEM((planes, share, depth), bf16),
            pltpu.VMEM((planes, head_count, share, depth), bf16),
            pltpu.VMEM((planes, frame_rows // 4, kv_columns), jnp.float32),
            pltpu.VMEM((planes, frame_rows // 4, kv_columns), jnp.float32),
            pltpu.VMEM((planes, frame_rows // 4, kv_columns), bf16),
            pltpu.VMEM((planes, frame_rows // 4, kv_columns), bf16),
            pltpu.VMEM((seq_count,) + asks_shape, bf16),
            pltpu.VMEM((seq_count,) + asks_shape, bf16),
            pltpu.VMEM((8, seq_count * own_rows), jnp.float32),
            pltpu.VMEM((seq_count, 8, seq_count * own_rows), jnp.float32),
            pltpu.SemaphoreType.DMA((len(arguments),)),
            pltpu.SemaphoreType.DMA((messages,)),
            pltpu.SemaphoreType.DMA((messages,)),
        ],
        compiler_params=pltpu.CompilerParams(
            collective_id=0, has_side_effects=True, vmem_limit_bytes=60 << 20
        ),
        name="fused",
    )(*arguments)
    return answers


def device_program(*arguments):
    patches, _, w_qkv, _, window_order = arguments[:5]
    paired = lax.axis_size("seq") == 8 and lax.axis_size("head") == 4
    whole = patches.shape[0] == FPATCH and window_order.shape[0] == 1
    if paired and whole and w_qkv.shape[0] % 16 == 0:
        return fused(*arguments)
    return on_device(*arguments)


def solution(mesh):
    placed = (
        P("seq", None),
        P(),
        P("seq", None, "head"),
        P("head", "seq"),
        P("seq", None),
        P(),
        P("seq", None, "head"),
        P("seq", "head"),
        P("seq", None, None, "head"),
        P("seq"),
        P(),
    )
    return jax.shard_map(
        device_program, mesh=mesh, in_specs=placed, out_specs=P("seq", "head"), check_vma=False
    )
```

```python
import functools

import jax
import jax.numpy as jnp
from jax import lax
from jax.experimental import pallas as pl
from jax.experimental.pallas import tpu as pltpu
from jax.sharding import PartitionSpec as P

VD = 1280
VH = 16
HD = 128
FPATCH = 256
WIN = 64

MESH = pl.DeviceIdType.MESH
VMEM = pl.BlockSpec(memory_space=pltpu.VMEM)


def rms_scale(values, gain):
    return values * lax.rsqrt(jnp.mean(values * values, axis=-1, keepdims=True) + 1e-06) * gain


def exchange_kernel(axis, count, gather, x_ref, out_ref, send_sem, recv_sem, own_sem):
    me = lax.axis_index(axis)
    barrier = pltpu.get_barrier_semaphore()
    for step in range(1, count):
        pl.semaphore_signal(
            barrier, inc=1, device_id={axis: lax.rem(me + step, count)}, device_id_type=MESH
        )
    pl.semaphore_wait(barrier, count - 1)
    copies = []
    for step in range(1, count):
        peer = lax.rem(me + step, count)
        copy = pltpu.make_async_remote_copy(
            src_ref=x_ref if gather else x_ref.at[peer],
            dst_ref=out_ref.at[me],
            send_sem=send_sem.at[step],
            recv_sem=recv_sem.at[step],
            device_id={axis: peer},
            device_id_type=MESH,
        )
        copy.start()
        copies.append(copy)
    own = pltpu.make_async_copy(x_ref if gather else x_ref.at[me], out_ref.at[me], own_sem)
    own.start()
    own.wait()
    for copy in copies:
        copy.wait()


def exchange(x, axis, gather, collective_id):
    count = lax.axis_size(axis)
    shape = ((count,) + x.shape) if gather else x.shape
    return pl.pallas_call(
        functools.partial(exchange_kernel, axis, count, gather),
        out_shape=jax.ShapeDtypeStruct(shape, x.dtype),
        in_specs=[VMEM],
        out_specs=VMEM,
        scratch_shapes=[
            pltpu.SemaphoreType.DMA((count,)),
            pltpu.SemaphoreType.DMA((count,)),
            pltpu.SemaphoreType.DMA,
        ],
        compiler_params=pltpu.CompilerParams(collective_id=collective_id, has_side_effects=True),
        name=f"exchange_{collective_id}",
    )(x)


def ring_kernel(count, qkv_ref, wout_ref, qkv_out, wout_out, send_sem, recv_sem, own_sem):
    me = lax.axis_index("seq")
    odd = lax.rem(me, 2)
    place = (1 - odd) * (me // 2) + odd * (count - 1 - me // 2)

    def index_of(position):
        position = lax.rem(position + count, count)
        late = position // (count // 2)
        return (1 - late) * 2 * position + late * (2 * (count - 1 - position) + 1)

    neighbours = (index_of(place + 1), index_of(place - 1))
    barrier = pltpu.get_barrier_semaphore()
    for neighbour in neighbours:
        pl.semaphore_signal(barrier, inc=1, device_id={"seq": neighbour}, device_id_type=MESH)
    pl.semaphore_wait(barrier, 2)
    far, near = count // 2, count - 1 - count // 2
    pieces = 4

    def slot(piece, source):
        return qkv_out.at[piece, source] if piece < 3 else wout_out.at[source]

    def own(piece):
        return qkv_ref.at[piece] if piece < 3 else wout_ref

    copies = {}
    for step in range(far):
        for piece in range(pieces):
            for way in range(2):
                hops = far if (piece < 2) == (way == 0) else near
                if step >= hops:
                    continue
                source = index_of(place - step if way == 0 else place + step)
                if step > 0:
                    copies[step - 1, piece, way].wait_recv()
                copy = pltpu.make_async_remote_copy(
                    src_ref=own(piece) if step == 0 else slot(piece, source),
                    dst_ref=slot(piece, source),
                    send_sem=send_sem.at[step, piece, way],
                    recv_sem=recv_sem.at[step, piece, way],
                    device_id={"seq": neighbours[way]},
                    device_id_type=MESH,
                )
                copy.start()
                copies[step, piece, way] = copy
    kept = [pltpu.make_async_copy(own(p), slot(p, me), own_sem.at[p]) for p in range(pieces)]
    for copy in kept:
        copy.start()
    for copy in kept:
        copy.wait()
    for (step, piece, way), copy in copies.items():
        if (step + 1, piece, way) not in copies:
            copy.wait_recv()
    for copy in copies.values():
        copy.wait_send()


def ring_weights(w_qkv, w_out):
    count = lax.axis_size("seq")
    far = count // 2
    return pl.pallas_call(
        functools.partial(ring_kernel, count),
        out_shape=(
            jax.ShapeDtypeStruct((3, count) + w_qkv.shape[1:], w_qkv.dtype),
            jax.ShapeDtypeStruct((count,) + w_out.shape, w_out.dtype),
        ),
        in_specs=[VMEM, VMEM],
        out_specs=(VMEM, VMEM),
        scratch_shapes=[
            pltpu.SemaphoreType.DMA((far, 4, 2)),
            pltpu.SemaphoreType.DMA((far, 4, 2)),
            pltpu.SemaphoreType.DMA((4,)),
        ],
        compiler_params=pltpu.CompilerParams(collective_id=0, has_side_effects=True),
        name="ring_weights",
    )(w_qkv, w_out)


def frame_attention(query, key, value, unit_order, head_size):
    unit_count = unit_order.shape[0]
    patch_count = unit_count * 4
    ranks = jnp.sum(
        jnp.where(
            unit_order[None, :] == (jnp.arange(patch_count) // 4)[:, None],
            jnp.arange(unit_count)[None, :] // (WIN // 4),
            0,
        ),
        axis=1,
    )
    same = ranks[:, None] == ranks[None, :]
    scores = jnp.einsum(
        "qhd,khd->hqk", query, key, preferred_element_type=jnp.float32
    ) * head_size ** (-0.5)
    scores = jnp.where(same[None], scores, -jnp.inf)
    weights = jax.nn.softmax(scores, axis=-1).astype(jnp.bfloat16)
    return jnp.einsum(
        "hqk,khd->qhd", weights, value, preferred_element_type=jnp.float32
    ).astype(jnp.bfloat16)


def on_device(
    patches,
    norm_gain,
    w_qkv,
    w_out,
    window_order,
    merge_gain,
    w_kv,
    queries,
    suffix_kv,
    question_lengths,
    frame_range,
):
    head_count = lax.axis_size("head")
    seq_count = lax.axis_size("seq")
    row_count = patches.shape[0]
    frame_count = window_order.shape[0]
    columns = w_qkv.shape[2]
    head_size = VD // VH
    local_heads = columns // head_size
    source = patches.astype(jnp.float32)
    normed = rms_scale(source, norm_gain).astype(jnp.bfloat16)
    qkv_all, w_out_all = ring_weights(w_qkv.transpose(1, 0, 2), w_out)
    qkv_all = qkv_all.reshape(3, -1, columns)
    query, key, value = [
        jnp.dot(normed, qkv_all[part], preferred_element_type=jnp.float32)
        .astype(jnp.bfloat16)
        .reshape(frame_count, -1, local_heads, head_size)
        for part in range(3)
    ]
    attended = jax.vmap(
        lambda q, k, v, order: frame_attention(q, k, v, order, head_size)
    )(query, key, value, window_order).reshape(row_count, columns)
    w_full = w_out_all.transpose(1, 0, 2).reshape(columns, VD)
    share_rows = row_count // head_count
    partial = jnp.dot(attended, w_full, preferred_element_type=jnp.float32).astype(jnp.bfloat16)
    parts = exchange(partial.reshape(head_count, share_rows, VD), "head", False, 1)
    shared = jnp.sum(parts.astype(jnp.float32), axis=0)
    own_rows = lax.dynamic_slice_in_dim(source, lax.axis_index("head") * share_rows, share_rows, 0)
    merged = rms_scale(own_rows + shared, merge_gain).astype(jnp.bfloat16)
    share_tokens = share_rows // 4
    depth = w_kv.shape[0]
    merged = merged.reshape(share_tokens, seq_count, depth).transpose(1, 0, 2)
    merged = exchange(merged, "seq", False, 2)
    merged = exchange(merged, "head", True, 3)
    merged = merged.transpose(1, 0, 2, 3).reshape(-1, depth)
    kv_columns = w_kv.shape[2]
    partial = jnp.dot(
        merged, w_kv.reshape(depth, 2 * kv_columns), preferred_element_type=jnp.float32
    ).astype(jnp.bfloat16)
    parts = exchange(partial.reshape(seq_count, -1, 2 * kv_columns), "seq", False, 4)
    visual = jnp.sum(parts.astype(jnp.float32), axis=0).astype(jnp.bfloat16)
    visual = exchange(visual, "seq", True, 5).reshape(-1, 2 * kv_columns)

    token_count = visual.shape[0]
    quest_count = queries.shape[0]
    span = suffix_kv.shape[1]
    kv_local = kv_columns // HD
    asking = queries.reshape(quest_count, kv_local, -1, HD)
    frame_tokens = FPATCH // 4
    seq_index = lax.axis_index("seq")
    bounds = lax.dynamic_slice_in_dim(frame_range, seq_index * quest_count, quest_count, 0)
    frame_index = jnp.arange(token_count) // frame_tokens
    live = (frame_index[None, :] >= bounds[:, 0:1]) & (frame_index[None, :] < bounds[:, 1:2])
    suffix_live = jnp.arange(span)[None, :] < question_lengths[:, None]
    suffix = suffix_kv.reshape(quest_count, span, 2, kv_local, HD)
    answers = []
    for g in range(kv_local):
        ask = asking[:, g]
        keys = visual[:, g * HD : (g + 1) * HD]
        values = visual[:, kv_columns + g * HD : kv_columns + (g + 1) * HD]
        scores = jnp.einsum(
            "qjd,nd->qjn", ask, keys, preferred_element_type=jnp.float32
        ) * HD ** (-0.5)
        scores = jnp.where(live[:, None, :], scores, -jnp.inf)
        tail = jnp.einsum(
            "qjd,qsd->qjs", ask, suffix[:, :, 0, g], preferred_element_type=jnp.float32
        ) * HD ** (-0.5)
        tail = jnp.where(suffix_live[:, None, :], tail, -jnp.inf)
        highest = jnp.maximum(
            jnp.max(scores, axis=-1, keepdims=True), jnp.max(tail, axis=-1, keepdims=True)
        )
        weights = jnp.exp(scores - highest)
        tail_weights = jnp.exp(tail - highest)
        totals = jnp.sum(weights, axis=-1, keepdims=True) + jnp.sum(
            tail_weights, axis=-1, keepdims=True
        )
        mixed = jnp.einsum(
            "qjn,nd->qjd", weights.astype(jnp.bfloat16), values, preferred_element_type=jnp.float32
        ) + jnp.einsum(
            "qjs,qsd->qjd",
            tail_weights.astype(jnp.bfloat16),
            suffix[:, :, 1, g],
            preferred_element_type=jnp.float32,
        )
        answers.append((mixed / totals).astype(jnp.bfloat16))
    return jnp.stack(answers, axis=1).reshape(quest_count, -1)


def fused_kernel(
    seq_count,
    head_count,
    patches_in,
    norm_gain_in,
    merge_gain_in,
    wqkv_in,
    wo_in,
    order_in,
    wkv_in,
    queries_in,
    suffix_in,
    lengths_in,
    range_in,
    out_ref,
    patches_ref,
    norm_gain_ref,
    merge_gain_ref,
    wqkv_ref,
    wo_ref,
    order_ref,
    wkv_ref,
    queries_ref,
    suffix_ref,
    lengths_ref,
    range_ref,
    wide,
    wq_ref,
    kv_ref,
    asks_ref,
    rows_all,
    order_all,
    normed,
    wq_all,
    wo_packed,
    wo_all,
    wo_full,
    wkv_all,
    asks_all,
    swap_out,
    swap_in,
    core_out,
    core_in,
    side_out,
    side_in,
    merged_out,
    merged_all,
    key_out,
    key_in,
    value_out,
    value_in,
    mixed_out,
    mixed_in,
    level_out,
    level_in,
    load_sems,
    send_sems,
    recv_sems,
):
    planes = seq_count // 2
    me = lax.axis_index("seq")
    head = lax.axis_index("head")
    z, y = me // 2, lax.rem(me, 2)
    x, c = head // 2, lax.rem(head, 2)
    half = lax.rem(z, 2)
    group = 2 * c + x
    frame_rows, depth = patches_ref.shape
    group_rows = frame_rows // head_count
    share = group_rows // 4
    head_size = VD // VH
    own_width = 2 * head_size

    def at(z_to, y_to, x_to, c_to):
        return {"seq": 2 * z_to + y_to, "head": 2 * x_to + c_to}

    partner = z + 1 - 2 * half
    across = at(z, 1 - y, x, c)
    beside = at(z, y, 1 - x, c)
    twin = at(z, y, x, 1 - c)
    paired = at(partner, y, x, c)

    low = z < planes // 2
    inner = (z > 0) & (z < planes - 1)

    def ordered(outer_plane, inner_plane):
        plane = jnp.where(inner, inner_plane, outer_plane)
        return jnp.where(low, plane, planes - 1 - plane)

    def target(k):
        return ordered((3, 2, 1)[k], (2, 0, 3)[k])

    def source(j):
        return ordered((1, 3, 2)[j], (2, 3, 0)[j])

    barrier = pltpu.get_barrier_semaphore()
    peers = [
        {"seq": lax.rem(me + step, seq_count), "head": head} for step in range(1, seq_count)
    ] + [beside, twin]
    for peer in peers:
        pl.semaphore_signal(barrier, inc=1, device_id=peer, device_id_type=MESH)

    pairs = (
        (wqkv_in, wqkv_ref),
        (patches_in, patches_ref),
        (order_in, order_ref),
        (norm_gain_in, norm_gain_ref),
        (wo_in, wo_ref),
        (wkv_in, wkv_ref),
        (queries_in, queries_ref),
        (suffix_in, suffix_ref),
        (lengths_in, lengths_ref),
        (merge_gain_in, merge_gain_ref),
        (range_in, range_ref),
    )
    loads = [
        pltpu.make_async_copy(src, dst, load_sems.at[i]) for i, (src, dst) in enumerate(pairs)
    ]
    for load in loads:
        load.start()
    taken = []
    started = []
    guarded = []

    def slots(count=1):
        taken.append(count)
        return sum(taken) - count

    def copy_of(src, dst, device, send_slot, recv_slot):
        return pltpu.make_async_remote_copy(
            src_ref=src,
            dst_ref=dst,
            send_sem=send_sems.at[send_slot],
            recv_sem=recv_sems.at[recv_slot],
            device_id=device,
            device_id_type=MESH,
        )

    def send(src, dst, device, send_slot, recv_slot):
        copy = copy_of(src, dst, device, send_slot, recv_slot)
        copy.start()
        started.append(copy)
        return copy

    def send_if(inside, src, dst, device, send_slot, recv_slot):
        copy = copy_of(src, dst, device, send_slot, recv_slot)

        @pl.when(inside)
        def _():
            copy.start()

        guarded.append((inside, copy))

    def send_all(count, slot, copy_at):
        for step in range(1, count):
            src, dst, device = copy_at(step)
            copy_of(src, dst, device, slot, slot).start()

    def left(copy):
        started[:] = [kept for kept in started if kept is not copy]
        copy.wait_send()

    def arrived(ref, slot, name):
        copy_of(ref, ref, twin, slot, slot).wait_recv()

    for load in loads[:3]:
        load.wait()

    for part in range(head_count):
        row = lax.broadcasted_iota(jnp.int32, (group_rows, frame_rows), 0)
        place = lax.broadcasted_iota(jnp.int32, (group_rows, frame_rows), 1)
        picked = 4 * (share * part + lax.rem(row, share)) + row // share
        pick = jnp.where(place == picked, 1.0, 0.0).astype(jnp.bfloat16)
        rows_all[half, pl.ds(part * group_rows, group_rows), :] = jnp.dot(
            pick, patches_ref[...], preferred_element_type=jnp.float32
        ).astype(jnp.bfloat16)
    columns = wqkv_ref.shape[2]
    wq_width = wq_ref.shape[2]
    lane = lax.broadcasted_iota(jnp.int32, wq_ref.shape[1:], 1)
    packed = [jnp.zeros(wq_ref.shape[1:], jnp.float32)] * 2
    wide[...] = jnp.zeros_like(wide)
    for part in range(3):
        wide[part, :, :columns] = wqkv_ref[part].astype(jnp.float32)
        for side in range(2):
            shift = (part - side) * own_width
            moved = wide[part] if shift == 0 else pltpu.roll(wide[part], shift % wq_width, 1)
            inside = (lane >= part * own_width) & (lane < (part + 1) * own_width)
            packed[side] = jnp.where(inside, moved, packed[side])
    for side in range(2):
        wq_ref[side] = packed[side].astype(jnp.bfloat16)
    order_all[half] = order_ref[...]
    pl.semaphore_wait(barrier, len(peers))

    quarter = pl.ds(pl.multiple_of(group * group_rows, group_rows), group_rows)
    far = planes - 1
    order_slot, rows_slot, rows_x_slot, rows_c_slot, rows_xc_slot = (slots() for _ in range(5))
    wq_z, wq_y, wo_z, wo_y = (slots(planes) for _ in range(4))
    send(order_all.at[half], order_all.at[half], paired, order_slot, order_slot)

    def wq_send(k, inside=None):
        to = target(k)
        copy = (
            wq_ref.at[lax.rem(to, 2)],
            wq_all.at[me],
            at(to, y, x, c),
            wq_z + k,
            wq_z + z,
        )
        return send(*copy) if inside is None else send_if(inside, *copy)

    def over_y(ref, plane, base):
        own = ref.at[2 * plane + y]
        return send(own, own, across, base + plane, base + plane)

    def hear_y(ref, plane, base, name):
        arrived(ref.at[2 * plane + 1 - y], base + plane, name)

    def wq_hear(j):
        plane = source(j)
        arrived(wq_all.at[2 * plane + y], wq_z + plane, "wq_z")
        return over_y(wq_all, plane, wq_y)

    outer = jnp.logical_not(inner)
    wq_first = wq_send(0)
    wq_send(1, inner)
    wq_all[me] = wq_ref[half]
    send(wq_ref.at[half], wq_all.at[me], across, wq_y + z, wq_y + z)

    for load in loads[3:]:
        load.wait()
    kv_columns = wkv_ref.shape[2]
    for side in range(2):
        kv_ref[:, side * kv_columns : (side + 1) * kv_columns] = wkv_ref[:, side, :]
    early = kv_ref.shape[0] // 4
    wkv_slot = slots(2)
    wkv_parts = (pl.ds(0, early), pl.ds(early, kv_ref.shape[0] - early))

    def wkv_send(i):
        part = wkv_parts[i]
        send(kv_ref.at[part], wkv_all.at[y, part], across, wkv_slot + i, wkv_slot + i)

    wkv_send(0)
    wkv_all[y] = kv_ref[...]
    for i in range(2):
        for j in range(2):
            wo_packed[2 * i + j] = wo_ref[i * 80 : (i + 1) * 80, j * 128 : (j + 1) * 128]
    wo_packed[4] = jnp.concatenate(
        [wo_ref[:80, 256:320], wo_ref[80:, 256:320]], axis=1
    )
    wo_all[me] = wo_packed[...]
    asked = queries_ref[...].astype(jnp.float32)
    quest_count = asked.shape[0]
    kv_heads = wkv_ref.shape[2] // HD
    asking = asked.shape[1] // (kv_heads * HD)
    for g in range(kv_heads):
        asks_ref[g] = jnp.concatenate(
            [
                asked[q : q + 1, (g * asking + j) * HD : (g * asking + j + 1) * HD]
                for q in range(quest_count)
                for j in range(asking)
            ],
            axis=0,
        ).astype(jnp.bfloat16)
    asks_all[me] = asks_ref[...]

    def normalise(slot):
        for part in range(head_count):
            rows = pl.ds(part * group_rows, group_rows)
            source = rows_all[slot, rows, :].astype(jnp.float32)
            normed[slot, rows, :] = rms_scale(source, norm_gain_ref[...].reshape(1, -1)).astype(jnp.bfloat16)

    normalise(half)

    left(wq_first)
    rows_copy = send(
        rows_all.at[half, quarter], rows_all.at[half, quarter], paired, rows_slot, rows_slot
    )
    wq_send(2, inner)
    wq_send(1, outer)
    wq_hear(0)
    over_y(wo_all, z, wo_y)
    left(rows_copy)
    wq_send(2, outer)

    scale = HD ** (-0.5)
    tails = []
    for g in range(kv_heads):
        columns = slice(g * HD, (g + 1) * HD)
        mixes, levels = [], []
        for q in range(quest_count):
            ask = asks_ref[g, q * asking : (q + 1) * asking, :]
            keys = suffix_ref[q, :, 0, columns]
            values = suffix_ref[q, :, 1, columns]
            scores = (
                lax.dot_general(
                    ask, keys, (((1,), (1,)), ((), ())), preferred_element_type=jnp.float32
                )
                * scale
            )
            place = lax.broadcasted_iota(jnp.int32, scores.shape, 1)
            scores = jnp.where(place < lengths_ref[q], scores, -1e30)
            highest = jnp.max(scores, axis=1, keepdims=True)
            weights = jnp.exp(scores - highest)
            total = jnp.sum(weights, axis=1, keepdims=True)
            mix = jnp.dot(
                weights.astype(jnp.bfloat16), values, preferred_element_type=jnp.float32
            )
            mixes.append(mix / total)
            levels.append(highest + jnp.log(total))
        tails.append((jnp.concatenate(mixes, axis=0), jnp.concatenate(levels, axis=0)))

    other = 1 - half
    def wo_send(k):
        send(wo_packed, wo_all.at[me], at(target(k), y, x, c), wo_z + k, wo_z + z)

    theirs = rows_all.at[other, quarter]
    arrived(theirs, rows_slot, "rows")
    send(theirs, theirs, beside, rows_x_slot, rows_x_slot)
    send(theirs, theirs, twin, rows_c_slot, rows_c_slot)
    wq_hear(1)
    for k in range(far - 1):
        wo_send(k)
    for j in range(2, far):
        wq_hear(j)
    wo_send(far - 1)

    def unpack(slice_at):
        for i in range(2):
            for j in range(2):
                wo_full[slice_at, i * 80 : (i + 1) * 80, j * 128 : (j + 1) * 128] = wo_all[
                    slice_at, 2 * i + j
                ]
        last = wo_all[slice_at, 4]
        wo_full[slice_at, :80, 256:384] = last
        wo_full[slice_at, 80:, 256:384] = pltpu.roll(last.astype(jnp.float32), 64, 1).astype(
            jnp.bfloat16
        )

    wo_relays = {}

    def wo_hear(j, inside=None):
        plane = source(j)
        own = wo_all.at[2 * plane + y]
        if j not in wo_relays:
            wo_relays[j] = copy_of(own, own, across, wo_y + plane, wo_y + plane)
            started.append(wo_relays[j])
        copy = wo_relays[j]

        def take():
            arrived(own, wo_z + plane, "wo_z")
            copy.start()
            unpack(2 * plane + y)

        if inside is None:
            take()
        else:
            pl.when(inside)(take)

    side_quarter = pl.ds(
        pl.multiple_of((2 * c + 1 - x) * group_rows, group_rows), group_rows
    )
    beside_rows = rows_all.at[other, side_quarter]
    arrived(beside_rows, rows_x_slot, "rows_x")
    send(beside_rows, beside_rows, twin, rows_xc_slot, rows_xc_slot)
    twin_quarter = pl.ds(
        pl.multiple_of((2 * (1 - c) + x) * group_rows, group_rows), group_rows
    )
    arrived(rows_all.at[other, twin_quarter], rows_c_slot, "rows_c")
    arrived(rows_all.at[other, twin_quarter], rows_xc_slot, "rows_xc")
    arrived(order_all.at[other], order_slot, "order")
    normalise(other)
    unpack(me)
    wo_hear(0)
    for plane in range(planes):
        hear_y(wq_all, plane, wq_y, "wq_y")
        if plane == 1:
            wo_hear(1, outer)

    lane = lax.broadcasted_iota(jnp.int32, (frame_rows, 256), 1)

    def attend(slot):
        unit_count = order_ref.shape[1]
        row = lax.broadcasted_iota(jnp.int32, (frame_rows, unit_count), 0)
        unit = row // group_rows * share + lax.rem(row, share)
        place = lax.broadcasted_iota(jnp.int32, (frame_rows, unit_count), 1)
        window = jnp.sum(
            jnp.where(order_all[slot] == unit, place // (WIN // 4), 0).astype(jnp.float32),
            axis=1,
            keepdims=True,
        )
        sort = lax.broadcasted_iota(jnp.int32, (frame_rows, 128), 1).astype(jnp.float32)
        member = jnp.where(window == sort, 1.0, 0.0).astype(jnp.bfloat16)
        same = (
            lax.dot_general(
                member, member, (((1,), (1,)), ((), ())), preferred_element_type=jnp.float32
            )
            > 0.5
        )
        qkv = jnp.dot(
            normed[slot],
            wq_all[...].reshape(depth, wq_ref.shape[2]),
            preferred_element_type=jnp.float32,
        )
        width = qkv.shape[1]
        query = qkv[:, :256].astype(jnp.bfloat16)
        key = pltpu.roll(qkv, width - own_width, 1)[:, :256].astype(jnp.bfloat16)
        value = pltpu.roll(qkv, width - 2 * own_width, 1)[:, :256].astype(jnp.bfloat16)
        mixed = jnp.zeros((frame_rows, 256), jnp.float32)
        for i in range(2):
            inside = (lane >= i * head_size) & (lane < (i + 1) * head_size)
            scores = lax.dot_general(
                jnp.where(inside, query, jnp.zeros_like(query)),
                key,
                (((1,), (1,)), ((), ())),
                preferred_element_type=jnp.float32,
            ) * head_size ** (-0.5)
            scores = jnp.where(same, scores, -1e30)
            weights = jnp.exp(scores - jnp.max(scores, axis=1, keepdims=True))
            weights = weights / jnp.sum(weights, axis=1, keepdims=True)
            product = jnp.dot(
                weights.astype(jnp.bfloat16), value, preferred_element_type=jnp.float32
            )
            mixed = jnp.where(inside, product, mixed)
        shifted = pltpu.roll(mixed, own_width - 128, 1)
        return jnp.where(half == 0, mixed, shifted).astype(jnp.bfloat16)

    swap_slot, core_slot, side_slot = slots(), slots(2), slots(2)
    swap_out[...] = attend(other)
    send(swap_out, swap_in, paired, swap_slot, swap_slot)
    wo_hear(1, inner)
    for j in range(2, far):
        wo_hear(j)
    ask_slot, mix_slot, level_slot = (slots() for _ in range(3))

    owners = [2 * target(k) + side for k in range(far) for side in (1 - y, y)]
    owners.append(2 * z + 1 - y)

    def owner(step):
        to = owners[step - 1]
        return to, {"seq": to, "head": head}

    send_all(seq_count, ask_slot, lambda step: (asks_ref, asks_all.at[me], owner(step)[1]))
    others = pl.ds(0, seq_count - 1)
    mine = attend(half)
    arrived(swap_in, swap_slot, "swap")
    theirs = swap_in[...]
    front = jnp.where(half == 0, mine, theirs)
    back = jnp.where(half == 0, theirs, mine)
    attended = jnp.concatenate(
        [front[:, :128], front[:, 128:] + back[:, :128], back[:, 128:]], axis=1
    )
    for plane in range(planes):
        hear_y(wo_all, plane, wo_y, "wo_y")
        unpack(2 * plane + 1 - y)
    both = 2 * group_rows
    kept = []
    for i in range(2):
        part = wo_full[i * (seq_count // 2) : (i + 1) * (seq_count // 2)]
        partial = lax.dot_general(
            attended,
            part.reshape(depth // 2, wo_full.shape[2]),
            (((1,), (1,)), ((), ())),
            preferred_element_type=jnp.float32,
        )
        top, bottom = partial[:both], partial[both:]
        core_out[i] = jnp.where(c == 0, bottom, top).astype(jnp.bfloat16)
        send(core_out.at[i], core_in.at[i], twin, core_slot + i, core_slot + i)
        kept.append(jnp.where(c == 0, top, bottom))
    for i in range(2):
        arrived(core_in.at[i], core_slot + i, "core")
        total = kept[i] + core_in[i].astype(jnp.float32)
        top, bottom = total[:group_rows], total[group_rows:]
        side_out[i] = jnp.where(x == 0, bottom, top).astype(jnp.bfloat16)
        send(side_out.at[i], side_in.at[i], beside, side_slot + i, side_slot + i)
        kept[i] = jnp.where(x == 0, top, bottom)
    wkv_send(1)
    for i in range(2):
        arrived(side_in.at[i], side_slot + i, "side")
        kept[i] = kept[i] + side_in[i].astype(jnp.float32)
    hidden = jnp.concatenate(kept, axis=1) + rows_all[half, quarter, :].astype(jnp.float32)
    merged = rms_scale(hidden, merge_gain_ref[...].reshape(1, -1)).astype(jnp.bfloat16)
    merged_out[...] = merged.reshape(planes, share, depth)

    mz, mx, mc, mxc, key_slots, value_slots = (slots(planes) for _ in range(6))
    for k in range(far):
        to = target(k)
        send(merged_out.at[to], merged_all.at[z, group], at(to, y, x, c), mz + k, mz + z)
    merged_all[z, group] = merged_out[z]
    side_group, twin_group = 2 * c + 1 - x, 2 * (1 - c) + x
    cross_group = 2 * (1 - c) + 1 - x

    def spread(plane, block):
        here = merged_all.at[plane, group]
        send(block, here, beside, mx + plane, mx + plane)
        send(block, here, twin, mc + plane, mc + plane)

    def relay(plane):
        block = merged_all.at[plane, side_group]
        arrived(block, mx + plane, "mx")
        send(block, block, twin, mxc + plane, mxc + plane)

    frame_tokens = frame_rows // 4

    def project(plane):
        arrived(merged_all.at[plane, twin_group], mc + plane, "mc")
        arrived(merged_all.at[plane, cross_group], mxc + plane, "mxc")
        block = merged_all[plane].reshape(frame_tokens, depth)
        weights = wkv_all[...].reshape(depth, kv_ref.shape[1])
        return jnp.dot(block, weights, preferred_element_type=jnp.float32)

    def project_to(plane):
        product = project(plane)
        key_out[plane] = product[:, :kv_columns]
        value_out[plane] = product[:, kv_columns:].astype(jnp.bfloat16)
        to = at(plane, y, x, c)
        send(key_out.at[plane], key_in.at[z], to, key_slots + plane, key_slots + z)
        send(value_out.at[plane], value_in.at[z], to, value_slots + plane, value_slots + z)

    planes_heard = [source(j) for j in range(far)]
    spread(z, merged_out.at[z])
    for j in range(far):
        plane = planes_heard[j]
        arrived(merged_all.at[plane, group], mz + plane, "mz")
        spread(plane, merged_all.at[plane, group])
        relay(planes_heard[j - 1] if j else z)
    for i in range(2):
        arrived(wkv_all.at[1 - y, wkv_parts[i]], wkv_slot + i, "wkv")
    for plane in planes_heard[:-1]:
        project_to(plane)
    relay(planes_heard[-1])
    project_to(planes_heard[-1])
    visual = project(z)
    keys, values = visual[:, :kv_columns], visual[:, kv_columns:]
    for plane in planes_heard:
        arrived(key_in.at[plane], key_slots + plane, "key")
        arrived(value_in.at[plane], value_slots + plane, "value")
        keys = keys + key_in[plane]
        values = values + value_in[plane].astype(jnp.float32)
    all_keys, all_values = keys.astype(jnp.bfloat16), values.astype(jnp.bfloat16)

    arrived(asks_all.at[others], ask_slot, "ask")
    all_rows = seq_count * asks_ref.shape[1]
    own_rows = asks_ref.shape[1]
    questions = range_ref.shape[1]
    seen = jnp.concatenate(
        [
            jnp.full(
                (asking, 1),
                jnp.where((range_ref[0, q] <= me) & (me < range_ref[1, q]), 0.0, -1e30),
                jnp.float32,
            )
            for q in range(questions)
        ],
        axis=0,
    )
    level_out[...] = jnp.zeros_like(level_out)
    diagonal = lax.broadcasted_iota(
        jnp.int32, (all_rows, all_rows), 0
    ) == lax.broadcasted_iota(jnp.int32, (all_rows, all_rows), 1)
    for g in range(kv_heads):
        ask = asks_all[:, g].reshape(all_rows, HD)
        keys = all_keys[:, g * HD : (g + 1) * HD]
        values = all_values[:, g * HD : (g + 1) * HD]
        scores = (
            lax.dot_general(
                ask, keys, (((1,), (1,)), ((), ())), preferred_element_type=jnp.float32
            )
            * scale
        )
        highest = jnp.max(scores, axis=1, keepdims=True)
        weights = jnp.exp(scores - highest)
        total = jnp.sum(weights, axis=1, keepdims=True)
        mix = (
            jnp.dot(weights.astype(jnp.bfloat16), values, preferred_element_type=jnp.float32)
            / total
        )
        level = highest + jnp.log(total) + seen
        mixed_out[:, g] = mix.astype(jnp.bfloat16).reshape(seq_count, own_rows, HD)
        level_out[g : g + 1, :] = jnp.sum(
            jnp.where(diagonal, level, 0.0), axis=0, keepdims=True
        )
    mixed_in[me] = mixed_out[me]
    level_in[me] = level_out[...]
    for step in range(1, seq_count):
        to, device = owner(step)
        copy_of(level_out, level_in.at[me], device, level_slot, level_slot).start()
        copy_of(mixed_out.at[to], mixed_in.at[me], device, mix_slot, mix_slot).start()
    arrived(mixed_in.at[others], mix_slot, "mix")
    arrived(level_in.at[others], level_slot, "level")
    row = lax.broadcasted_iota(jnp.int32, (own_rows, all_rows), 0)
    place = lax.broadcasted_iota(jnp.int32, (own_rows, all_rows), 1)
    chosen = place == row + me * own_rows
    answers = []
    for g in range(kv_heads):
        mix, level = tails[g]
        levels = [
            jnp.sum(jnp.where(chosen, level_in[s, g : g + 1, :], 0.0), axis=1, keepdims=True)
            for s in range(seq_count)
        ]
        highest = level
        for other_level in levels:
            highest = jnp.maximum(highest, other_level)
        share_of = jnp.exp(level - highest)
        total = share_of
        answer = share_of * mix
        for s in range(seq_count):
            share_of = jnp.exp(levels[s] - highest)
            total = total + share_of
            answer = answer + share_of * mixed_in[s, g].astype(jnp.float32)
        answers.append(answer / total)
    out_ref[...] = jnp.concatenate(
        [
            jnp.concatenate(
                [
                    answers[g][q * asking + j : q * asking + j + 1]
                    for g in range(kv_heads)
                    for j in range(asking)
                ],
                axis=1,
            )
            for q in range(quest_count)
        ],
        axis=0,
    ).astype(jnp.bfloat16)
    for copy in started:
        copy.wait_send()
    for block, slot in (
        (asks_all.at[others], ask_slot),
        (mixed_in.at[others], mix_slot),
        (level_in.at[others], level_slot),
    ):
        copy_of(block, block, twin, slot, slot).wait_send()
    for inside, copy in guarded:

        @pl.when(inside)
        def _(copy=copy):
            copy.wait_send()


def fused(
    patches,
    norm_gain,
    w_qkv,
    w_out,
    window_order,
    merge_gain,
    w_kv,
    queries,
    suffix_kv,
    question_lengths,
    frame_range,
):
    seq_count, head_count = lax.axis_size("seq"), lax.axis_size("head")
    planes = seq_count // 2
    frame_rows, depth = patches.shape
    rows, _, columns = w_qkv.shape
    half = columns // 2
    kv_columns = w_kv.shape[2]
    kv_heads = kv_columns // HD
    bf16 = jnp.bfloat16
    wq_width = -(-3 * half // 128) * 128
    asks_shape = (kv_heads, queries.size // (kv_heads * HD), HD)
    own_rows = asks_shape[1]
    group_rows = frame_rows // head_count
    share = group_rows // 4
    messages = 11 + 11 * (seq_count // 2)
    arguments = (
        patches,
        norm_gain,
        merge_gain,
        w_qkv.transpose(1, 0, 2),
        w_out.T,
        window_order,
        w_kv,
        queries,
        suffix_kv,
        question_lengths,
        frame_range.T,
    )
    answers = pl.pallas_call(
        functools.partial(fused_kernel, seq_count, head_count),
        out_shape=pltpu.VMEM(queries.shape, bf16),
        in_specs=[pl.BlockSpec(memory_space=pl.ANY)] * len(arguments),
        out_specs=VMEM,
        scratch_shapes=[pltpu.VMEM(array.shape, array.dtype) for array in arguments[:-2]]
        + [pltpu.SMEM(array.shape, array.dtype) for array in arguments[-2:]]
        + [
            pltpu.VMEM((3, rows, wq_width), jnp.float32),
            pltpu.VMEM((2, rows, wq_width), bf16),
            pltpu.VMEM((w_kv.shape[0], 2 * kv_columns), bf16),
            pltpu.VMEM(asks_shape, bf16),
            pltpu.VMEM((2, frame_rows, depth), bf16),
            pltpu.VMEM((2,) + window_order.shape, jnp.int32),
            pltpu.VMEM((2, frame_rows, depth), bf16),
            pltpu.VMEM((seq_count, rows, wq_width), bf16),
            pltpu.VMEM((5, 80, 128), bf16),
            pltpu.VMEM((seq_count, 5, 80, 128), bf16),
            pltpu.VMEM((seq_count, rows, 384), bf16),
            pltpu.VMEM((2, w_kv.shape[0], 2 * kv_columns), bf16),
            pltpu.VMEM((seq_count,) + asks_shape, bf16),
            pltpu.VMEM((frame_rows, 256), bf16),
            pltpu.VMEM((frame_rows, 256), bf16),
            pltpu.VMEM((2, 2 * group_rows, depth // 2), bf16),
            pltpu.VMEM((2, 2 * group_rows, depth // 2), bf16),
            pltpu.VMEM((2, group_rows, depth // 2), bf16),
            pltpu.VMEM((2, group_rows, depth // 2), bf16),
            pltpu.VMEM((planes, share, depth), bf16),
            pltpu.VMEM((planes, head_count, share, depth), bf16),
            pltpu.VMEM((planes, frame_rows // 4, kv_columns), jnp.float32),
            pltpu.VMEM((planes, frame_rows // 4, kv_columns), jnp.float32),
            pltpu.VMEM((planes, frame_rows // 4, kv_columns), bf16),
            pltpu.VMEM((planes, frame_rows // 4, kv_columns), bf16),
            pltpu.VMEM((seq_count,) + asks_shape, bf16),
            pltpu.VMEM((seq_count,) + asks_shape, bf16),
            pltpu.VMEM((8, seq_count * own_rows), jnp.float32),
            pltpu.VMEM((seq_count, 8, seq_count * own_rows), jnp.float32),
            pltpu.SemaphoreType.DMA((len(arguments),)),
            pltpu.SemaphoreType.DMA((messages,)),
            pltpu.SemaphoreType.DMA((messages,)),
        ],
        compiler_params=pltpu.CompilerParams(
            collective_id=0, has_side_effects=True, vmem_limit_bytes=60 << 20
        ),
        name="fused",
    )(*arguments)
    return answers


def device_program(*arguments):
    patches, _, w_qkv, _, window_order = arguments[:5]
    paired = lax.axis_size("seq") == 8 and lax.axis_size("head") == 4
    whole = patches.shape[0] == FPATCH and window_order.shape[0] == 1
    if paired and whole and w_qkv.shape[0] % 16 == 0:
        return fused(*arguments)
    return on_device(*arguments)


def solution(mesh):
    placed = (
        P("seq", None),
        P(),
        P("seq", None, "head"),
        P("head", "seq"),
        P("seq", None),
        P(),
        P("seq", None, "head"),
        P("seq", "head"),
        P("seq", None, None, "head"),
        P("seq"),
        P(),
    )
    return jax.shard_map(
        device_program, mesh=mesh, in_specs=placed, out_specs=P("seq", "head"), check_vma=False
    )
```
